8 devices in a mesh: dp: 2 (over z, y), ws: 4 (over x, core).
Axes of the slice: x: 2, y: 2, z: 1, core: 2. Of those that a mesh axis runs over, the one named last changes fastest.
Arguments:
- hidden: bfloat16 [128, 768], P(('dp', 'ws')), parts along dimension 0
- self_k: bfloat16 [128, 12, 384, 64], P(('dp', 'ws')), parts along dimension 0
- self_v: bfloat16 [128, 12, 384, 64], P(('dp', 'ws')), parts along dimension 0
- cross_k: bfloat16 [128, 12, 1024, 64], P(('dp', 'ws')), parts along dimension 0
- cross_v: bfloat16 [128, 12, 1024, 64], P(('dp', 'ws')), parts along dimension 0
- positions: int32 [128], P(('dp', 'ws')), parts along dimension 0
- enc_mask: int32 [128, 1024], P(('dp', 'ws')), parts along dimension 0
- rel_bias: float32 [12, 384], replicated
- expert_idx: int32 [128], P(('dp', 'ws')), parts along dimension 0
- ln_self: float32 [768], replicated
- ln_cross: float32 [768], replicated
- ln_ffn: float32 [768], replicated
- wq_self: bfloat16 [768, 768], P(None, 'ws')
- wk_self: bfloat16 [768, 768], P(None, 'ws')
- wv_self: bfloat16 [768, 768], P(None, 'ws')
- wo_self: bfloat16 [768, 768], P(None, 'ws')
- wq_cross: bfloat16 [768, 768], P(None, 'ws')
- wo_cross: bfloat16 [768, 768], P(None, 'ws')
- w_router: float32 [768, 16], P(None, 'ws')
- w_in: bfloat16 [16, 768, 3072], P(None, None, 'ws')
- w_out: bfloat16 [16, 3072, 768], P(None, 'ws')
Outputs:
- output 1: bfloat16 [128, 768], P(('dp', 'ws')), parts along dimension 0
- output 2: bfloat16 [128, 12, 384, 64], P(('dp', 'ws')), parts along dimension 0
- output 3: bfloat16 [128, 12, 384, 64], P(('dp', 'ws')), parts along dimension 0
There are 2 independent parts. The reference program is written for one: setup_inputs(seed, part) draws one part's arguments, and reference() takes and returns one part's arrays. A program takes and returns all parts, laid end to end along the dimension named above; an argument that names none is the same for every part.
All inputs are finite; a program needn't handle non-finite values.
Results may differ from the reference program's by a relative error of at most 0.0108291.
Values are sent between devices in bfloat16 or wider.
A program may use at most 1 GiB of HBM per device.

```python
import jax
import jax.numpy as jnp
from jax import lax

D_MODEL = 768
NUM_HEADS = 12
HEAD_DIM = 64
D_FF = 3072
EXPERTS = 16
CACHE_LEN = 384
SRC_LEN = 1024
GROUP_ROWS = 64

ATTN_WIDTH = NUM_HEADS * HEAD_DIM
CAPACITY = (2 * GROUP_ROWS + EXPERTS - 1) // EXPERTS
EPSILON = 1e-6
NEG_BIG = -1e30


def scaled_normal(key, shape, scale):
    return (jax.random.normal(key, shape, jnp.float32) * scale).astype(jnp.bfloat16)


def setup_inputs(seed: int = 0, part: int = 0) -> dict:
    base_key = jax.random.key(seed)
    shared = jax.random.split(base_key, 13)
    part_keys = jax.random.split(jax.random.fold_in(base_key, part), 12)
    row_ids = jnp.arange(GROUP_ROWS)
    cache_shape = (GROUP_ROWS, NUM_HEADS, CACHE_LEN, HEAD_DIM)
    src_shape = (GROUP_ROWS, NUM_HEADS, SRC_LEN, HEAD_DIM)
    hidden = scaled_normal(part_keys[0], (GROUP_ROWS, D_MODEL), 1.0)
    self_k = scaled_normal(part_keys[1], cache_shape, 1.0)
    self_v = scaled_normal(part_keys[2], cache_shape, 1.0)
    cross_k = scaled_normal(part_keys[3], src_shape, 1.0)
    cross_v = scaled_normal(part_keys[4], src_shape, 1.0)
    positions = jax.random.randint(part_keys[5], (GROUP_ROWS,), 0, CACHE_LEN)
    last_row = jax.random.randint(part_keys[6], (), 0, GROUP_ROWS)
    positions = jnp.where(row_ids == last_row, CACHE_LEN - 1, positions).astype(jnp.int32)
    src_lens = jax.random.randint(part_keys[7], (GROUP_ROWS,), 1, SRC_LEN + 1)
    full_row = jax.random.randint(part_keys[8], (), 0, GROUP_ROWS)
    src_lens = jnp.where(row_ids == full_row, SRC_LEN, src_lens)
    enc_mask = (jnp.arange(SRC_LEN)[None, :] < src_lens[:, None]).astype(jnp.int32)
    hot_expert = jax.random.randint(part_keys[9], (), 0, EXPERTS)
    free_pick = jax.random.randint(part_keys[10], (GROUP_ROWS,), 0, EXPERTS)
    row_order = jax.random.permutation(part_keys[11], GROUP_ROWS)
    hot_rows = jnp.zeros((GROUP_ROWS,), jnp.int32).at[row_order[:CAPACITY + 1]].set(1)
    expert_idx = jnp.where(hot_rows == 1, hot_expert, free_pick).astype(jnp.int32)
    return {
        'hidden': hidden,
        'self_k': self_k,
        'self_v': self_v,
        'cross_k': cross_k,
        'cross_v': cross_v,
        'positions': positions,
        'enc_mask': enc_mask,
        'rel_bias': jax.random.normal(shared[0], (NUM_HEADS, CACHE_LEN), jnp.float32),
        'expert_idx': expert_idx,
        'ln_self': jax.random.uniform(shared[1], (D_MODEL,), jnp.float32, 0.5, 1.5),
        'ln_cross': jax.random.uniform(shared[2], (D_MODEL,), jnp.float32, 0.5, 1.5),
        'ln_ffn': jax.random.uniform(shared[3], (D_MODEL,), jnp.float32, 0.5, 1.5),
        'wq_self': scaled_normal(shared[4], (D_MODEL, ATTN_WIDTH), 1.5 * (D_MODEL * HEAD_DIM) ** -0.5),
        'wk_self': scaled_normal(shared[5], (D_MODEL, ATTN_WIDTH), D_MODEL ** -0.5),
        'wv_self': scaled_normal(shared[6], (D_MODEL, ATTN_WIDTH), D_MODEL ** -0.5),
        'wo_self': scaled_normal(shared[7], (ATTN_WIDTH, D_MODEL), ATTN_WIDTH ** -0.5),
        'wq_cross': scaled_normal(shared[8], (D_MODEL, ATTN_WIDTH), 1.5 * (D_MODEL * HEAD_DIM) ** -0.5),
        'wo_cross': scaled_normal(shared[9], (ATTN_WIDTH, D_MODEL), ATTN_WIDTH ** -0.5),
        'w_router': jax.random.normal(shared[10], (D_MODEL, EXPERTS), jnp.float32) * D_MODEL ** -0.5,
        'w_in': scaled_normal(shared[11], (EXPERTS, D_MODEL, D_FF), D_MODEL ** -0.5),
        'w_out': scaled_normal(shared[12], (EXPERTS, D_FF, D_MODEL), (EXPERTS / D_FF) ** 0.5),
    }


def rms_norm(hidden, scale):
    hid_f32 = hidden.astype(jnp.float32)
    inv_rms = lax.rsqrt(jnp.mean(hid_f32 * hid_f32, axis=-1, keepdims=True) + EPSILON)
    return (hid_f32 * inv_rms * scale).astype(jnp.bfloat16)


def attend_row(row_args):
    queries, cache_keys, cache_vals, score_bias = row_args
    scores = jnp.einsum('hd,hld->hl', queries.astype(jnp.float32), cache_keys.astype(jnp.float32)) + score_bias
    attn_probs = jax.nn.softmax(scores, axis=-1).astype(jnp.bfloat16)
    context = jnp.einsum('hl,hld->hd', attn_probs.astype(jnp.float32), cache_vals.astype(jnp.float32))
    return context.astype(jnp.bfloat16)


def project(x_norm, weight):
    return jnp.dot(x_norm, weight, preferred_element_type=jnp.float32).astype(jnp.bfloat16)


def reference(hidden, self_k, self_v, cross_k, cross_v, positions, enc_mask, rel_bias, expert_idx,
              ln_self, ln_cross, ln_ffn, wq_self, wk_self, wv_self, wo_self, wq_cross, wo_cross,
              w_router, w_in, w_out):
    head_shape = (GROUP_ROWS, NUM_HEADS, HEAD_DIM)
    x_norm = rms_norm(hidden, ln_self)
    queries = project(x_norm, wq_self).reshape(head_shape)
    k_new = project(x_norm, wk_self).reshape(head_shape)
    v_new = project(x_norm, wv_self).reshape(head_shape)
    distance = positions[:, None] - jnp.arange(CACHE_LEN)[None, :]
    write_mask = (distance == 0)[:, None, :, None]
    new_self_k = jnp.where(write_mask, k_new[:, :, None, :], self_k)
    new_self_v = jnp.where(write_mask, v_new[:, :, None, :], self_v)
    pos_bias = jnp.take(rel_bias, jnp.clip(distance, 0, CACHE_LEN - 1), axis=1)
    pos_bias = jnp.where(distance[None] >= 0, pos_bias, NEG_BIG).transpose(1, 0, 2)
    context = lax.map(attend_row, (queries, new_self_k, new_self_v, pos_bias))
    attn_out = jnp.dot(context.reshape(GROUP_ROWS, ATTN_WIDTH), wo_self, preferred_element_type=jnp.float32)
    after_self = (hidden.astype(jnp.float32) + attn_out).astype(jnp.bfloat16)

    x_norm = rms_norm(after_self, ln_cross)
    queries = project(x_norm, wq_cross).reshape(head_shape)
    mask_bias = jnp.where(enc_mask == 1, 0.0, NEG_BIG)[:, None, :]
    context = lax.map(attend_row, (queries, cross_k, cross_v, mask_bias))
    attn_out = jnp.dot(context.reshape(GROUP_ROWS, ATTN_WIDTH), wo_cross, preferred_element_type=jnp.float32)
    after_cross = (after_self.astype(jnp.float32) + attn_out).astype(jnp.bfloat16)

    x_norm = rms_norm(after_cross, ln_ffn)
    logits = jnp.dot(x_norm.astype(jnp.float32), w_router, precision=lax.Precision.HIGHEST,
                     preferred_element_type=jnp.float32)
    router_probs = jax.nn.softmax(logits, axis=-1)
    chosen = jnp.arange(EXPERTS)[None, :] == expert_idx[:, None]
    gate_val = jnp.sum(jnp.where(chosen, router_probs, 0.0), axis=-1)
    row_ids = jnp.arange(GROUP_ROWS)
    earlier = (expert_idx[None, :] == expert_idx[:, None]) & (row_ids[None, :] < row_ids[:, None])
    slot_idx = jnp.sum(earlier.astype(jnp.int32), axis=1)
    keep_gate = jnp.where(slot_idx < CAPACITY, gate_val, 0.0)

    def expert_row(row_args):
        x_row, expert = row_args
        ffn_hidden = jnp.dot(x_row[None, :], w_in[expert], preferred_element_type=jnp.float32)
        ffn_hidden = jax.nn.relu(ffn_hidden).astype(jnp.bfloat16)
        ffn_out = jnp.dot(ffn_hidden, w_out[expert], preferred_element_type=jnp.float32)
        return ffn_out.astype(jnp.bfloat16)[0]

    expert_out = lax.map(expert_row, (x_norm, expert_idx))
    hidden_out = (after_cross.astype(jnp.float32) + expert_out.astype(jnp.float32) * keep_gate[:, None]).astype(jnp.bfloat16)
    return (hidden_out, new_self_k, new_self_v)
```

```python
import functools
import jax
import jax.numpy as jnp
from jax import lax
from jax.experimental import pallas as pl
from jax.experimental.pallas import tpu as pltpu
from jax.sharding import PartitionSpec as P

EPSILON = 1e-6
NEG_BIG = -1e30
F32 = jnp.float32
BF16 = jnp.bfloat16
MESH = pl.DeviceIdType.MESH
VMEM_SPEC = pl.BlockSpec(memory_space=pltpu.VMEM)
SMEM_SPEC = pl.BlockSpec(memory_space=pltpu.SMEM)
ANY_SPEC = pl.BlockSpec(memory_space=pl.ANY)
VMEM_MAX = 67_000_000
HEAD_PAD = 16


def rms_norm(hidden, scale):
    hid = hidden.astype(F32)
    inv = lax.rsqrt(jnp.mean(hid * hid, axis=-1, keepdims=True) + EPSILON)
    return (hid * inv * scale).astype(BF16)


def dot_nn(a, b):
    return lax.dot_general(a, b, (((1,), (0,)), ((), ())), preferred_element_type=F32)


def dot_nt(a, b):
    return lax.dot_general(a, b, (((1,), (1,)), ((), ())), preferred_element_type=F32)


def entry_barrier(me, n):
    sem = pltpu.get_barrier_semaphore()
    for k in range(1, n):
        pl.semaphore_signal(sem, inc=1, device_id={"ws": lax.rem(me + k, n)}, device_id_type=MESH)
    pl.semaphore_wait(sem, n - 1)


def start_exchange(me, n, src_of, dst, send_sem, recv_sem):
    copies = []
    for k in range(1, n):
        peer = lax.rem(me + k, n)
        copy = pltpu.make_async_remote_copy(
            src_ref=src_of(peer), dst_ref=dst, send_sem=send_sem.at[k - 1], recv_sem=recv_sem.at[k - 1],
            device_id={"ws": peer}, device_id_type=MESH)
        copy.start()
        copies.append(copy)
    return copies


def wait_all(copies):
    for copy in copies:
        copy.wait()


def my_columns(full, me, n, width):
    picked = full[:, 0:width]
    for j in range(1, n):
        picked = jnp.where(me == j, full[:, j * width:(j + 1) * width], picked)
    return picked


def qkv_kernel(n, h_ref, ln_ref, wq_ref, wk_ref, wv_ref, bias_ref, mask_ref,
               q_ref, k_ref, v_ref, hall_ref, brev_ref, lens_ref,
               hbuf, sendbuf, recvbuf, s1, r1, s2, r2):
    me = lax.axis_index("ws")
    rows, width = h_ref.shape
    cols = wq_ref.shape[0]
    entry_barrier(me, n)
    copies = start_exchange(me, n, lambda p: h_ref, hbuf.at[me], s1, r1)
    hbuf[me] = h_ref[...]
    lens_ref[...] = jnp.broadcast_to(jnp.sum(mask_ref[...], axis=1, keepdims=True), lens_ref.shape)
    length = bias_ref.shape[1]
    flip = (lax.broadcasted_iota(jnp.int32, (length, length), 0)
            + lax.broadcasted_iota(jnp.int32, (length, length), 1) == length - 1).astype(F32)
    brev_ref[...] = lax.dot_general(bias_ref[...], flip, (((1,), (0,)), ((), ())),
                                    precision=lax.Precision.HIGHEST, preferred_element_type=F32)
    wait_all(copies)
    hidden = hbuf[...].reshape(n * rows, width)
    hall_ref[...] = hidden
    x = rms_norm(hidden, ln_ref[...])
    for i, w in enumerate((wq_ref, wk_ref, wv_ref)):
        sendbuf[:, i] = dot_nt(x, w[...]).astype(BF16).reshape(n, rows, cols)
    copies = start_exchange(me, n, lambda p: sendbuf.at[p], recvbuf.at[me], s2, r2)
    recvbuf[me] = sendbuf[me]
    wait_all(copies)
    for i, o in enumerate((q_ref, k_ref, v_ref)):
        o[...] = jnp.concatenate([recvbuf[j, i] for j in range(n)], axis=1)


def block_rows(row, head_dim):
    width = row.shape[1]
    head = lax.broadcasted_iota(jnp.int32, (HEAD_PAD, width), 0)
    lane = lax.broadcasted_iota(jnp.int32, (HEAD_PAD, width), 1)
    return jnp.where(lane // head_dim == head, jnp.broadcast_to(row, (HEAD_PAD, width)), 0.0)


def softmax_rows(scores):
    top = jnp.max(scores, axis=-1, keepdims=True)
    e = jnp.exp(scores - top)
    return (e / jnp.sum(e, axis=-1, keepdims=True)).astype(BF16)


def self_kernel(heads, pos_ref, q_ref, k_ref, v_ref, brev_ref, sk_ref, sv_ref,
                ctx_ref, nk_ref, nv_ref,
                kbuf, vbuf, kt, vt, sbuf, pbuf, qf, cf, in_sem, out_sem):
    rows, width, length = kbuf.shape
    head_dim = width // heads

    def load(r, i):
        src, buf = ((sk_ref, kbuf), (sv_ref, vbuf))[i]
        return pltpu.make_async_copy(src.at[r], buf.at[r], in_sem.at[i, r])

    def save(r, i):
        buf, dst = ((kbuf, nk_ref), (vbuf, nv_ref))[i]
        return pltpu.make_async_copy(buf.at[r], dst.at[r], out_sem.at[i, r])

    for i in range(2):
        @pl.loop(0, rows)
        def _(r, i=i):
            load(r, i).start()

    pad = jnp.zeros((128 - rows, width), F32)
    kt[...] = jnp.transpose(jnp.concatenate([k_ref[...].astype(F32), pad], axis=0)).astype(BF16)
    vt[...] = jnp.transpose(jnp.concatenate([v_ref[...].astype(F32), pad], axis=0)).astype(BF16)
    qf[...] = q_ref[...].astype(F32)

    def insert(r, buf, cols):
        pos = pos_ref[0, r]
        tile = pos // 128
        at = pos - tile * 128
        row_i = lax.broadcasted_iota(jnp.int32, (128, 128), 0)
        lane_i = lax.broadcasted_iota(jnp.int32, (128, 128), 1)
        pick = jnp.where((row_i == r) & (lane_i == at), 1.0, 0.0).astype(BF16)
        new = dot_nn(cols[...], pick)
        view = buf.at[r, :, pl.ds(pl.multiple_of(tile * 128, 128), 128)]
        hit = lax.broadcasted_iota(jnp.int32, (width, 128), 1) == at
        view[...] = jnp.where(hit, new, view[...].astype(F32)).astype(BF16)

    @pl.loop(0, rows)
    def _(r):
        load(r, 0).wait()
        insert(r, kbuf, kt)
        q_blk = block_rows(qf[pl.ds(r, 1), :], head_dim).astype(BF16)
        sbuf[r] = dot_nn(q_blk, kbuf[r])
        save(r, 0).start()

    @pl.loop(0, rows)
    def _(r):
        pos = pos_ref[0, r]
        bias = pltpu.roll(brev_ref[...], lax.rem(pos + 1, length), 1)
        lane = lax.broadcasted_iota(jnp.int32, (HEAD_PAD, length), 1)
        pbuf[r] = softmax_rows(jnp.where(lane <= pos, sbuf[r] + bias, NEG_BIG))

    @pl.loop(0, rows)
    def _(r):
        load(r, 1).wait()
        insert(r, vbuf, vt)
        out = dot_nt(pbuf[r], vbuf[r])
        head = lax.broadcasted_iota(jnp.int32, (HEAD_PAD, width), 0)
        lane = lax.broadcasted_iota(jnp.int32, (HEAD_PAD, width), 1)
        cf[pl.ds(r, 1), :] = jnp.sum(jnp.where(lane // head_dim == head, out, 0.0), axis=0, keepdims=True)
        save(r, 1).start()

    ctx_ref[...] = cf[...].astype(BF16)
    for i in range(2):
        @pl.loop(0, rows)
        def _(r, i=i):
            save(r, i).wait()


def mid_kernel(n, ctx_ref, hall_ref, wo_ref, ln_ref, wq_ref,
               q_ref, h1_ref, cbuf, hpart, sendbuf, recvbuf, s1, r1, s2, r2, s3, r3):
    me = lax.axis_index("ws")
    rows, width = ctx_ref.shape
    cols = wo_ref.shape[0]
    entry_barrier(me, n)
    copies = start_exchange(me, n, lambda p: ctx_ref, cbuf.at[me], s1, r1)
    cbuf[me] = ctx_ref[...]
    mine = my_columns(hall_ref[...].astype(F32), me, n, cols)
    wait_all(copies)
    attn = dot_nt(cbuf[...].reshape(n * rows, width), wo_ref[...])
    hpart[me] = (mine + attn).astype(BF16)
    copies = start_exchange(me, n, lambda p: hpart.at[me], hpart.at[me], s2, r2)
    wait_all(copies)
    h1 = jnp.concatenate([hpart[j] for j in range(n)], axis=1)
    h1_ref[...] = h1
    x = rms_norm(h1, ln_ref[...])
    sendbuf[...] = dot_nt(x, wq_ref[...]).astype(BF16).reshape(n, rows, cols)
    copies = start_exchange(me, n, lambda p: sendbuf.at[p], recvbuf.at[me], s3, r3)
    recvbuf[me] = sendbuf[me]
    wait_all(copies)
    q_ref[...] = jnp.concatenate([recvbuf[j] for j in range(n)], axis=1)


def cross_kernel(heads, lens_ref, q_ref, mask_ref, ck_ref, cv_ref,
                 ctx_ref, kbuf, vbuf, sbuf, pbuf, qf, cf, in_sem):
    rows, width, length = kbuf.shape
    head_dim = width // heads
    tiles = length // 128

    def per_size(r, body):
        count = (lens_ref[r, 0] + 127) // 128
        for t in range(1, tiles + 1):
            @pl.when(count == t)
            def _(t=t):
                body(t * 128)

    def load(r, i, size):
        src, buf = ((ck_ref, kbuf), (cv_ref, vbuf))[i]
        return pltpu.make_async_copy(src.at[r, :, 0:size], buf.at[r, :, 0:size], in_sem.at[i, r])

    for i in range(2):
        @pl.loop(0, rows)
        def _(r, i=i):
            per_size(r, lambda size: load(r, i, size).start())

    qf[...] = q_ref[...].astype(F32)

    @pl.loop(0, rows)
    def _(r):
        q_blk = block_rows(qf[pl.ds(r, 1), :], head_dim).astype(BF16)

        def body(size):
            load(r, 0, size).wait()
            sbuf[r, :, 0:size] = dot_nn(q_blk, kbuf[r, :, 0:size])
        per_size(r, body)

    @pl.loop(0, rows)
    def _(r):
        keep = jnp.broadcast_to(mask_ref[pl.ds(r, 1), :], (HEAD_PAD, length)) == 1
        pbuf[r] = softmax_rows(jnp.where(keep, sbuf[r], NEG_BIG))

    @pl.loop(0, rows)
    def _(r):
        head = lax.broadcasted_iota(jnp.int32, (HEAD_PAD, width), 0)
        lane = lax.broadcasted_iota(jnp.int32, (HEAD_PAD, width), 1)

        def body(size):
            load(r, 1, size).wait()
            out = dot_nt(pbuf[r, :, 0:size], vbuf[r, :, 0:size])
            cf[pl.ds(r, 1), :] = jnp.sum(jnp.where(lane // head_dim == head, out, 0.0), axis=0, keepdims=True)
        per_size(r, body)

    ctx_ref[...] = cf[...].astype(BF16)


def ffn_kernel(n, ctx_ref, h1_ref, wo_ref, ln_ref, wr_ref, idx_ref, win_ref, wout_ref,
               out_ref, cbuf, hpart, rbuf, ibuf, xbuf, mbuf, wi, wo, acc, part, own, ybuf,
               s1, r1, s2, r2, s3, r3, s4, r4, s5, r5, wi_sem, wo_sem):
    me = lax.axis_index("ws")
    rows, width = ctx_ref.shape
    cols = wo_ref.shape[0]
    experts = win_ref.shape[0]
    total = n * rows
    capacity = (2 * total + experts - 1) // experts

    def load(e, i):
        src, buf, sem = ((win_ref, wi, wi_sem), (wout_ref, wo, wo_sem))[i]
        return pltpu.make_async_copy(src.at[e], buf.at[e], sem.at[e])

    @pl.loop(0, experts)
    def _(e):
        load(e, 0).start()
        load(e, 1).start()

    entry_barrier(me, n)
    first = (start_exchange(me, n, lambda p: ctx_ref, cbuf.at[me], s1, r1)
             + start_exchange(me, n, lambda p: idx_ref, ibuf.at[me], s2, r2)
             + start_exchange(me, n, lambda p: wr_ref, rbuf.at[me], s3, r3))
    cbuf[me] = ctx_ref[...]
    ibuf[me] = idx_ref[...]
    rbuf[me] = wr_ref[...]
    mine = my_columns(h1_ref[...].astype(F32), me, n, cols)
    wait_all(first)
    attn = dot_nt(cbuf[...].reshape(total, width), wo_ref[...])
    hpart[me] = (mine + attn).astype(BF16)
    copies = start_exchange(me, n, lambda p: hpart.at[me], hpart.at[me], s4, r4)

    idx_row = jnp.concatenate([ibuf[j] for j in range(n)], axis=1)
    grid_i = lax.broadcasted_iota(jnp.int32, (total, total), 0)
    grid_j = lax.broadcasted_iota(jnp.int32, (total, total), 1)
    row_b = jnp.broadcast_to(idx_row, (total, total))
    idx_col = jnp.sum(jnp.where(grid_i == grid_j, row_b, 0), axis=1, keepdims=True)
    earlier = (row_b == idx_col) & (grid_j < grid_i)
    slot = jnp.sum(earlier.astype(jnp.int32), axis=1, keepdims=True)
    target = jnp.where(slot < capacity, idx_col, -1)
    mbuf[...] = jnp.broadcast_to(target, mbuf.shape)

    wait_all(copies)
    h2 = jnp.concatenate([hpart[j] for j in range(n)], axis=1)
    x = rms_norm(h2, ln_ref[...])
    xbuf[...] = x
    own[...] = h2.reshape(n, rows, width)
    acc[...] = jnp.zeros_like(acc)

    @pl.loop(0, experts)
    def _(e):
        load(e, 0).wait()
        u = jnp.maximum(dot_nn(xbuf[...], wi[e]), 0.0)
        hit = jnp.broadcast_to(mbuf[:, 0:1], u.shape) == e
        u = jnp.where(hit, u, 0.0).astype(BF16)
        load(e, 1).wait()
        acc[...] += dot_nn(u, wo[e])

    part[...] = acc[...].reshape(n, rows, width)
    copies = start_exchange(me, n, lambda p: part.at[p], ybuf.at[me], s5, r5)
    ybuf[me] = part[me]

    my_rows = pl.ds(pl.multiple_of(me * rows, rows), rows)
    router = jnp.concatenate([rbuf[j] for j in range(n)], axis=0)
    logits = lax.dot_general(xbuf[my_rows, :].astype(F32), router, (((1,), (1,)), ((), ())),
                             precision=lax.Precision.HIGHEST, preferred_element_type=F32)
    probs = jnp.exp(logits - jnp.max(logits, axis=-1, keepdims=True))
    probs = probs / jnp.sum(probs, axis=-1, keepdims=True)
    chosen = lax.broadcasted_iota(jnp.int32, (rows, experts), 1) == mbuf[my_rows, :][:, 0:experts]
    gate = jnp.sum(jnp.where(chosen, probs, 0.0), axis=-1, keepdims=True)
    wait_all(copies)
    y = ybuf[0]
    for j in range(1, n):
        y = y + ybuf[j]
    out_ref[...] = (own[me].astype(F32) + y.astype(BF16).astype(F32) * gate).astype(BF16)


def call(body, out_shape, in_specs, out_specs, scratch, collective=None, flops=1_000_000, moved=1_000_000, vmem=VMEM_MAX):
    params = dict(vmem_limit_bytes=vmem)
    if collective is not None:
        params.update(collective_id=collective, has_side_effects=True)
    return pl.pallas_call(
        body, out_shape=out_shape, in_specs=in_specs, out_specs=out_specs, scratch_shapes=scratch,
        compiler_params=pltpu.CompilerParams(**params),
        cost_estimate=pl.CostEstimate(flops=flops, bytes_accessed=moved, transcendentals=0))


def solution(mesh):
    n = mesh.shape['ws']
    row_axes = ('dp', 'ws')
    row_vec = P(row_axes)
    row_mat = P(row_axes, None)
    cache_spec = P(row_axes, None, None, None)
    col_split = P(None, 'ws')
    in_specs = (row_mat, cache_spec, cache_spec, cache_spec, cache_spec, row_vec, row_mat, P(None, None), row_vec,
                P(None), P(None), P(None), col_split, col_split, col_split, col_split, col_split, col_split,
                col_split, P(None, None, 'ws'), P(None, 'ws', None))
    out_specs = (row_mat, cache_spec, cache_spec)
    dma = pltpu.SemaphoreType.DMA

    def decoder_block(hidden, self_k, self_v, cross_k, cross_v, positions, enc_mask, rel_bias, expert_idx,
                      ln_self, ln_cross, ln_ffn, wq_self, wk_self, wv_self, wo_self, wq_cross, wo_cross,
                      w_router, w_in, w_out):
        rows, width = hidden.shape
        heads, length = rel_bias.shape
        head_dim = width // heads
        source = enc_mask.shape[1]
        cols = wq_self.shape[1]
        experts, _, units = w_in.shape
        total = n * rows
        sds = jax.ShapeDtypeStruct

        def flat(cache):
            return jnp.swapaxes(cache, 2, 3).reshape(rows, width, cache.shape[2])

        bias16 = jnp.pad(rel_bias, ((0, HEAD_PAD - heads), (0, 0)))
        sems = [dma((n - 1,))]
        q, k, v, hall, brev, lens = call(
            functools.partial(qkv_kernel, n),
            [sds((rows, width), BF16)] * 3 + [sds((total, width), BF16), sds((HEAD_PAD, length), F32), sds((rows, 128), jnp.int32)],
            [VMEM_SPEC] * 7, [VMEM_SPEC] * 6,
            [pltpu.VMEM((n, rows, width), BF16), pltpu.VMEM((n, 3, rows, cols), BF16), pltpu.VMEM((n, 3, rows, cols), BF16)] + sems * 4,
            collective=0, vmem=16_000_000,
        )(hidden, ln_self[None, :], wq_self.T, wk_self.T, wv_self.T, bias16, enc_mask)

        ctx, new_k, new_v = call(
            functools.partial(self_kernel, heads),
            [sds((rows, width), BF16)] + [sds((rows, width, length), BF16)] * 2,
            [SMEM_SPEC] + [VMEM_SPEC] * 4 + [ANY_SPEC] * 2, [VMEM_SPEC] + [ANY_SPEC] * 2,
            [pltpu.VMEM((rows, width, length), BF16)] * 2 + [pltpu.VMEM((width, 128), BF16)] * 2
            + [pltpu.VMEM((rows, HEAD_PAD, length), F32), pltpu.VMEM((rows, HEAD_PAD, length), BF16),
               pltpu.VMEM((rows, width), F32), pltpu.VMEM((rows, width), F32), dma((2, rows)), dma((2, rows))],
        )(positions[None, :], q, k, v, brev, flat(self_k), flat(self_v))

        qc, h1 = call(
            functools.partial(mid_kernel, n),
            [sds((rows, width), BF16), sds((total, width), BF16)],
            [VMEM_SPEC] * 5, [VMEM_SPEC] * 2,
            [pltpu.VMEM((n, rows, width), BF16), pltpu.VMEM((n, total, cols), BF16),
             pltpu.VMEM((n, rows, cols), BF16), pltpu.VMEM((n, rows, cols), BF16)] + sems * 6,
            collective=1, vmem=16_000_000,
        )(ctx, hall, wo_self.T, ln_cross[None, :], wq_cross.T)

        ctx2 = call(
            functools.partial(cross_kernel, heads),
            sds((rows, width), BF16),
            [SMEM_SPEC] + [VMEM_SPEC] * 2 + [ANY_SPEC] * 2, VMEM_SPEC,
            [pltpu.VMEM((rows, width, source), BF16)] * 2
            + [pltpu.VMEM((rows, HEAD_PAD, source), F32), pltpu.VMEM((rows, HEAD_PAD, source), BF16),
               pltpu.VMEM((rows, width), F32), pltpu.VMEM((rows, width), F32), dma((2, rows))],
        )(lens, qc, enc_mask, flat(cross_k), flat(cross_v))

        out = call(
            functools.partial(ffn_kernel, n),
            sds((rows, width), BF16),
            [VMEM_SPEC] * 6 + [ANY_SPEC] * 2, VMEM_SPEC,
            [pltpu.VMEM((n, rows, width), BF16), pltpu.VMEM((n, total, cols), BF16),
             pltpu.VMEM((n, experts // n, width), F32), pltpu.VMEM((n, 1, rows), jnp.int32),
             pltpu.VMEM((total, width), BF16), pltpu.VMEM((total, 128), jnp.int32),
             pltpu.VMEM((experts, width, units), BF16), pltpu.VMEM((experts, units, width), BF16),
             pltpu.VMEM((total, width), F32), pltpu.VMEM((n, rows, width), F32), pltpu.VMEM((n, rows, width), BF16),
             pltpu.VMEM((n, rows, width), F32)]
            + sems * 10 + [dma((experts,)), dma((experts,))],
            collective=2,
        )(ctx2, h1, wo_cross.T, ln_ffn[None, :], w_router.T, expert_idx[None, :], w_in, w_out)

        def unflat(cache):
            return jnp.swapaxes(cache.reshape(rows, heads, head_dim, length), 2, 3)

        return out, unflat(new_k), unflat(new_v)

    return jax.shard_map(decoder_block, mesh=mesh, in_specs=in_specs, out_specs=out_specs, check_vma=False)
```

```python
import functools
import jax
import jax.numpy as jnp
from jax import lax
from jax.experimental import pallas as pl
from jax.experimental.pallas import tpu as pltpu
from jax.sharding import PartitionSpec as P

EPSILON = 1e-6
NEG_BIG = -1e30
F32 = jnp.float32
BF16 = jnp.bfloat16
MESH = pl.DeviceIdType.MESH
VMEM_SPEC = pl.BlockSpec(memory_space=pltpu.VMEM)
SMEM_SPEC = pl.BlockSpec(memory_space=pltpu.SMEM)
HBM_SPEC = pl.BlockSpec(memory_space=pltpu.HBM)
VMEM_MAX = 67_000_000
HEAD_PAD = 16


def rms_norm(hidden, scale):
    hid = hidden.astype(F32)
    inv = lax.rsqrt(jnp.mean(hid * hid, axis=-1, keepdims=True) + EPSILON)
    return (hid * inv * scale).astype(BF16)


def dot_nn(a, b):
    return lax.dot_general(a, b, (((1,), (0,)), ((), ())), preferred_element_type=F32)


def dot_nt(a, b):
    return lax.dot_general(a, b, (((1,), (1,)), ((), ())), preferred_element_type=F32)


def entry_barrier(me, n):
    sem = pltpu.get_barrier_semaphore()
    for k in range(1, n):
        pl.semaphore_signal(sem, inc=1, device_id={"ws": lax.rem(me + k, n)}, device_id_type=MESH)
    pl.semaphore_wait(sem, n - 1)


def start_exchange(me, n, src_of, dst, send_sem, recv_sem):
    copies = []
    for k in range(1, n):
        peer = lax.rem(me + k, n)
        copy = pltpu.make_async_remote_copy(
            src_ref=src_of(peer), dst_ref=dst, send_sem=send_sem.at[k - 1], recv_sem=recv_sem.at[k - 1],
            device_id={"ws": peer}, device_id_type=MESH)
        copy.start()
        copies.append(copy)
    return copies


def wait_all(copies):
    for copy in copies:
        copy.wait()


def my_columns(full, me, n, width):
    picked = full[:, 0:width]
    for j in range(1, n):
        picked = jnp.where(me == j, full[:, j * width:(j + 1) * width], picked)
    return picked


def fetch(pairs, sem):
    copies = [pltpu.make_async_copy(src, dst, sem.at[i]) for i, (src, dst) in enumerate(pairs)]
    for copy in copies:
        copy.start()
    return copies


def qkv_kernel(n, h_hbm, ln_hbm, wq_hbm, wk_hbm, wv_hbm, bias_hbm, mask_hbm,
               q_ref, k_ref, v_ref, hall_ref, brev_ref, lens_ref,
               h_ref, ln_ref, w_ref, bias_ref, mask_ref, hbuf, sendbuf, recvbuf, s1, r1, s2, r2, in_sem):
    me = lax.axis_index("ws")
    rows, width = h_ref.shape
    cols = w_ref.shape[1]
    loads = fetch([(h_hbm, h_ref), (ln_hbm, ln_ref), (bias_hbm, bias_ref), (mask_hbm, mask_ref)]
                  + [(w, w_ref.at[i]) for i, w in enumerate((wq_hbm, wk_hbm, wv_hbm))], in_sem)
    entry_barrier(me, n)
    loads[0].wait()
    copies = start_exchange(me, n, lambda p: h_ref, hbuf.at[me], s1, r1)
    hbuf[me] = h_ref[...]
    for load in loads[1:]:
        load.wait()
    lens_ref[...] = jnp.broadcast_to(jnp.sum(mask_ref[...], axis=1, keepdims=True), lens_ref.shape)
    heads, length = bias_ref.shape
    flip = (lax.broadcasted_iota(jnp.int32, (length, length), 0)
            + lax.broadcasted_iota(jnp.int32, (length, length), 1) == length - 1).astype(F32)
    brev_ref[...] = jnp.zeros_like(brev_ref)
    brev_ref[0:heads, :] = lax.dot_general(bias_ref[...], flip, (((1,), (0,)), ((), ())),
                                           precision=lax.Precision.HIGHEST, preferred_element_type=F32)
    wait_all(copies)
    hidden = hbuf[...].reshape(n * rows, width)
    hall_ref[...] = hidden
    x = rms_norm(hidden, ln_ref[...].reshape(1, width))
    for i in range(3):
        sendbuf[:, i] = dot_nt(x, w_ref[i]).astype(BF16).reshape(n, rows, cols)
    copies = start_exchange(me, n, lambda p: sendbuf.at[p], recvbuf.at[me], s2, r2)
    recvbuf[me] = sendbuf[me]
    wait_all(copies)
    for i, o in enumerate((q_ref, k_ref, v_ref)):
        o[...] = jnp.concatenate([recvbuf[j, i] for j in range(n)], axis=1)


def head_mask(shape, head_dim):
    head = lax.broadcasted_iota(jnp.int32, shape, 0)
    return lax.broadcasted_iota(jnp.int32, shape, 1) // head_dim == head


def spread_heads(q_ref, qblk, head_dim):
    rows, width = q_ref.shape
    q = q_ref[...].astype(F32)
    keep = head_mask((HEAD_PAD, width), head_dim)
    for r in range(rows):
        qblk[r] = jnp.where(keep, jnp.broadcast_to(q[r:r + 1], (HEAD_PAD, width)), 0.0).astype(BF16)


def softmax_rows(scores):
    top = jnp.max(scores, axis=-1, keepdims=True)
    e = jnp.exp(scores - top)
    return (e / jnp.sum(e, axis=-1, keepdims=True)).astype(BF16).astype(F32)


def weighted_values(prob, value, heads, head_dim, length):
    parts = []
    for h in range(heads):
        total = None
        for t in range(length // 128):
            lanes = slice(t * 128, (t + 1) * 128)
            term = value[h * head_dim:(h + 1) * head_dim, lanes].astype(F32) * prob[h:h + 1, lanes]
            total = term if total is None else total + term
        parts.append(total)
    return jnp.sum(jnp.transpose(jnp.concatenate(parts, axis=0)), axis=0, keepdims=True)


def self_kernel(heads, pos_hbm, q_ref, k_ref, v_ref, brev_ref, sk_ref, sv_ref,
                ctx_ref, nk_ref, nv_ref,
                kbuf, vbuf, kt, vt, s0, s1, p0, p1, qblk, cf, in_sem, out_sem, pos_ref, pos_sem):
    rows, width, length = kbuf.shape
    head_dim = width // heads
    scalars = pltpu.make_async_copy(pos_hbm, pos_ref, pos_sem)
    scalars.start()

    def load(r, i):
        src, buf = ((sk_ref, kbuf), (sv_ref, vbuf))[i]
        return pltpu.make_async_copy(src.at[r], buf.at[r], in_sem.at[i, r])

    def save(r, i):
        buf, dst = ((kbuf, nk_ref), (vbuf, nv_ref))[i]
        return pltpu.make_async_copy(buf.at[r], dst.at[r], out_sem.at[i, r])

    for r in range(rows):
        load(r, 0).start()
        load(r, 1).start()

    pad = jnp.zeros((128 - rows, width), F32)
    kt[...] = jnp.transpose(jnp.concatenate([k_ref[...].astype(F32), pad], axis=0))
    vt[...] = jnp.transpose(jnp.concatenate([v_ref[...].astype(F32), pad], axis=0))
    spread_heads(q_ref, qblk, head_dim)
    sbufs, pbufs = (s0, s1), (p0, p1)
    scalars.wait()

    def insert(r, buf, cols):
        pos = pos_ref[r]
        tile = pos // 128
        at = pos - tile * 128
        new = jnp.broadcast_to(cols[:, r:r + 1], (width, 128))
        view = buf.at[r, :, pl.ds(pl.multiple_of(tile * 128, 128), 128)]
        hit = lax.broadcasted_iota(jnp.int32, (width, 128), 1) == at
        view[...] = jnp.where(hit, new, view[...].astype(F32)).astype(BF16)

    def softmax(r):
        pos = pos_ref[r]
        bias = pltpu.roll(brev_ref[...], lax.rem(pos + 1, length), 1)
        lane = lax.broadcasted_iota(jnp.int32, (HEAD_PAD, length), 1)
        pbufs[r % 2][...] = softmax_rows(jnp.where(lane <= pos, sbufs[r % 2][...] + bias, NEG_BIG))

    for step in range(rows + 3):
        r = step
        if r < rows:
            load(r, 0).wait()
            load(r, 1).wait()
        if step >= 3:
            done = step - 3
            cf[done:done + 1, :] = weighted_values(pbufs[done % 2], vbuf.at[done], heads, head_dim, length)
        if 2 <= step < rows + 2:
            softmax(step - 2)
        if 1 <= step < rows + 1:
            sbufs[(step - 1) % 2][...] = dot_nn(qblk[step - 1], kbuf[step - 1])
        if r < rows:
            insert(r, kbuf, kt)
            insert(r, vbuf, vt)
        if 1 <= step < rows + 1:
            save(step - 1, 0).start()
            save(step - 1, 1).start()

    ctx_ref[...] = cf[...].astype(BF16)
    for r in range(rows):
        save(r, 0).wait()
        save(r, 1).wait()


def mid_kernel(n, ctx_ref, hall_ref, wo_hbm, ln_hbm, wq_hbm,
               q_ref, h1_ref, wo_ref, ln_ref, wq_ref, in_sem, cbuf, hpart, sendbuf, recvbuf, s1, r1, s2, r2, s3, r3):
    me = lax.axis_index("ws")
    rows, width = ctx_ref.shape
    cols = wo_ref.shape[0]
    loads = fetch([(wo_hbm, wo_ref), (ln_hbm, ln_ref), (wq_hbm, wq_ref)], in_sem)
    entry_barrier(me, n)
    copies = start_exchange(me, n, lambda p: ctx_ref, cbuf.at[me], s1, r1)
    cbuf[me] = ctx_ref[...]
    mine = my_columns(hall_ref[...].astype(F32), me, n, cols)
    wait_all(loads)
    wait_all(copies)
    attn = dot_nt(cbuf[...].reshape(n * rows, width), wo_ref[...])
    hpart[me] = (mine + attn).astype(BF16)
    copies = start_exchange(me, n, lambda p: hpart.at[me], hpart.at[me], s2, r2)
    wait_all(copies)
    h1 = jnp.concatenate([hpart[j] for j in range(n)], axis=1)
    h1_ref[...] = h1
    x = rms_norm(h1, ln_ref[...].reshape(1, width))
    sendbuf[...] = dot_nt(x, wq_ref[...]).astype(BF16).reshape(n, rows, cols)
    copies = start_exchange(me, n, lambda p: sendbuf.at[p], recvbuf.at[me], s3, r3)
    recvbuf[me] = sendbuf[me]
    wait_all(copies)
    q_ref[...] = jnp.concatenate([recvbuf[j] for j in range(n)], axis=1)


def cross_kernel(heads, lens_ref, q_ref, mask_ref, ck_ref, cv_ref,
                 ctx_ref, kbuf, vbuf, s0, s1, p0, p1, qblk, cf, in_sem):
    rows, width, length = kbuf.shape
    head_dim = width // heads
    tiles = length // 128

    def tile_count(r):
        return (lens_ref[r, 0] + 127) // 128

    def per_size(r, body):
        count = tile_count(r)
        for t in range(1, tiles + 1):
            @pl.when(count == t)
            def _(t=t):
                body(t * 128)

    def load(r, i, size):
        src, buf = ((ck_ref, kbuf), (cv_ref, vbuf))[i]
        return pltpu.make_async_copy(src.at[r, :, 0:size], buf.at[r, :, 0:size], in_sem.at[i, r])

    @pl.loop(0, rows)
    def _(r):
        per_size(r, lambda size: load(r, 0, size).start())
        per_size(r, lambda size: load(r, 1, size).start())

    spread_heads(q_ref, qblk, head_dim)

    @pl.loop(0, rows)
    def _(r):
        @pl.loop(tile_count(r), tiles)
        def _(t):
            vbuf[r, :, pl.ds(pl.multiple_of(t * 128, 128), 128)] = jnp.zeros((width, 128), BF16)

    sbufs, pbufs = (s0, s1), (p0, p1)

    for step in range(rows + 2):
        if step < rows:
            per_size(step, lambda size: load(step, 0, size).wait())
        if step >= 2:
            per_size(step - 2, lambda size: load(step - 2, 1, size).wait())
            done = step - 2
            cf[done:done + 1, :] = weighted_values(pbufs[done % 2], vbuf.at[done], heads, head_dim, length)
        if 1 <= step < rows + 1:
            r = step - 1
            keep = jnp.broadcast_to(mask_ref[r:r + 1, :], (HEAD_PAD, length)) == 1
            pbufs[r % 2][...] = softmax_rows(jnp.where(keep, sbufs[r % 2][...], NEG_BIG))
        if step < rows:
            sbufs[step % 2][...] = dot_nn(qblk[step], kbuf[step])

    ctx_ref[...] = cf[...].astype(BF16)


def ffn_kernel(n, ctx_ref, h1_ref, wo_hbm, ln_hbm, wr_hbm, idx_hbm, win_ref, wout_ref,
               out_ref, cbuf, hpart, rbuf, ibuf, xbuf, mbuf, wi, wo, u0, u1, part, own, ybuf,
               s1, r1, s2, r2, s3, r3, s4, r4, s5, r5, wi_sem, wo_sem,
               wo_ref, ln_ref, wr_ref, idx_ref, in_sem):
    me = lax.axis_index("ws")
    rows, width = ctx_ref.shape
    cols = wo_ref.shape[0]
    experts = win_ref.shape[0]
    total = n * rows
    capacity = (2 * total + experts - 1) // experts

    def load(e, i):
        src, buf, sem = ((win_ref, wi, wi_sem), (wout_ref, wo, wo_sem))[i]
        return pltpu.make_async_copy(src.at[e], buf.at[e], sem.at[e])

    loads = fetch([(idx_hbm, idx_ref), (wr_hbm, wr_ref), (wo_hbm, wo_ref), (ln_hbm, ln_ref)], in_sem)

    @pl.loop(0, experts)
    def _(e):
        load(e, 0).start()
        load(e, 1).start()

    entry_barrier(me, n)
    wait_all(loads)
    first = (start_exchange(me, n, lambda p: ctx_ref, cbuf.at[me], s1, r1)
             + start_exchange(me, n, lambda p: idx_ref, ibuf.at[me], s2, r2)
             + start_exchange(me, n, lambda p: wr_ref, rbuf.at[me], s3, r3))
    cbuf[me] = ctx_ref[...]
    ibuf[me] = idx_ref[...]
    rbuf[me] = wr_ref[...]
    mine = my_columns(h1_ref[...].astype(F32), me, n, cols)
    wait_all(first)
    attn = dot_nt(cbuf[...].reshape(total, width), wo_ref[...])
    hpart[me] = (mine + attn).astype(BF16)
    copies = start_exchange(me, n, lambda p: hpart.at[me], hpart.at[me], s4, r4)

    idx_row = jnp.concatenate([ibuf[j] for j in range(n)], axis=1)
    grid_i = lax.broadcasted_iota(jnp.int32, (total, total), 0)
    grid_j = lax.broadcasted_iota(jnp.int32, (total, total), 1)
    row_b = jnp.broadcast_to(idx_row, (total, total))
    idx_col = jnp.sum(jnp.where(grid_i == grid_j, row_b, 0), axis=1, keepdims=True)
    earlier = (row_b == idx_col) & (grid_j < grid_i)
    slot = jnp.sum(earlier.astype(jnp.int32), axis=1, keepdims=True)
    target = jnp.where(slot < capacity, idx_col, -1)
    mbuf[...] = jnp.broadcast_to(target, mbuf.shape)

    wait_all(copies)
    h2 = jnp.concatenate([hpart[j] for j in range(n)], axis=1)
    x = rms_norm(h2, ln_ref[...].reshape(1, width))
    xbuf[...] = x
    own[...] = h2.reshape(n, rows, width)
    def hidden_units(e, buf):
        load(e, 0).wait()
        u = jnp.maximum(dot_nn(xbuf[...], wi[e]), 0.0)
        hit = jnp.broadcast_to(mbuf[:, 0:1], u.shape) == e
        buf[...] = jnp.where(hit, u, 0.0).astype(BF16)

    def add_output(e, buf):
        part[...] += dot_nn(buf[...], wo[e]).reshape(part.shape)

    part[...] = jnp.zeros_like(part)
    hidden_units(0, u0)

    @pl.loop(0, experts // 2)
    def _(i):
        e = i * 2
        load(e, 1).wait()
        hidden_units(e + 1, u1)
        add_output(e, u0)
        load(e + 1, 1).wait()

        @pl.when(e + 2 < experts)
        def _():
            hidden_units(e + 2, u0)
            add_output(e + 1, u1)

        @pl.when(e + 2 >= experts)
        def _():
            add_output(e + 1, u1)

    copies = start_exchange(me, n, lambda p: part.at[p], ybuf.at[me], s5, r5)
    ybuf[me] = part[me]

    my_rows = pl.ds(pl.multiple_of(me * rows, rows), rows)
    router = jnp.concatenate([rbuf[j] for j in range(n)], axis=0)
    logits = lax.dot_general(xbuf[my_rows, :].astype(F32), router, (((1,), (1,)), ((), ())),
                             precision=lax.Precision.HIGHEST, preferred_element_type=F32)
    probs = jnp.exp(logits - jnp.max(logits, axis=-1, keepdims=True))
    probs = probs / jnp.sum(probs, axis=-1, keepdims=True)
    chosen = lax.broadcasted_iota(jnp.int32, (rows, experts), 1) == mbuf[my_rows, :][:, 0:experts]
    gate = jnp.sum(jnp.where(chosen, probs, 0.0), axis=-1, keepdims=True)
    wait_all(copies)
    y = ybuf[0]
    for j in range(1, n):
        y = y + ybuf[j]
    out_ref[...] = (own[me].astype(F32) + y.astype(BF16).astype(F32) * gate).astype(BF16)


def call(body, out_shape, in_specs, out_specs, scratch, collective=None, flops=1_000_000, moved=1_000_000, vmem=VMEM_MAX):
    params = dict(vmem_limit_bytes=vmem)
    if collective is not None:
        params.update(collective_id=collective, has_side_effects=True)
    kernel = pl.pallas_call(
        body, out_shape=out_shape, in_specs=in_specs, out_specs=out_specs, scratch_shapes=scratch,
        compiler_params=pltpu.CompilerParams(**params),
        cost_estimate=pl.CostEstimate(flops=flops, bytes_accessed=moved, transcendentals=0))

    def run(*operands):
        return kernel(*[pltpu.with_memory_space_constraint(x, pltpu.HBM) if spec is HBM_SPEC else x
                        for x, spec in zip(operands, in_specs)])
    return run


def solution(mesh):
    n = mesh.shape['ws']
    row_axes = ('dp', 'ws')
    row_vec = P(row_axes)
    row_mat = P(row_axes, None)
    cache_spec = P(row_axes, None, None, None)
    col_split = P(None, 'ws')
    in_specs = (row_mat, cache_spec, cache_spec, cache_spec, cache_spec, row_vec, row_mat, P(None, None), row_vec,
                P(None), P(None), P(None), col_split, col_split, col_split, col_split, col_split, col_split,
                col_split, P(None, None, 'ws'), P(None, 'ws', None))
    out_specs = (row_mat, cache_spec, cache_spec)
    dma = pltpu.SemaphoreType.DMA

    def decoder_block(hidden, self_k, self_v, cross_k, cross_v, positions, enc_mask, rel_bias, expert_idx,
                      ln_self, ln_cross, ln_ffn, wq_self, wk_self, wv_self, wo_self, wq_cross, wo_cross,
                      w_router, w_in, w_out):
        rows, width = hidden.shape
        heads, length = rel_bias.shape
        head_dim = width // heads
        source = enc_mask.shape[1]
        cols = wq_self.shape[1]
        experts, _, units = w_in.shape
        total = n * rows
        sds = jax.ShapeDtypeStruct

        def flat(cache):
            return jnp.swapaxes(cache, 2, 3).reshape(rows, width, cache.shape[2])

        sems = [dma((n - 1,))]
        w_tile = pltpu.VMEM((cols, width), BF16)
        ln_tile = pltpu.VMEM((width,), F32)
        q, k, v, hall, brev, lens = call(
            functools.partial(qkv_kernel, n),
            [sds((rows, width), BF16)] * 3 + [sds((total, width), BF16), sds((HEAD_PAD, length), F32), sds((rows, 128), jnp.int32)],
            [HBM_SPEC] * 7, [VMEM_SPEC] * 6,
            [pltpu.VMEM((rows, width), BF16), ln_tile, pltpu.VMEM((3, cols, width), BF16), pltpu.VMEM((heads, length), F32),
             pltpu.VMEM((rows, source), jnp.int32),
             pltpu.VMEM((n, rows, width), BF16), pltpu.VMEM((n, 3, rows, cols), BF16), pltpu.VMEM((n, 3, rows, cols), BF16)]
            + sems * 4 + [dma((7,))],
            collective=0, vmem=8 << 20,
        )(hidden, ln_self, wq_self.T, wk_self.T, wv_self.T, rel_bias, enc_mask)

        def attention_scratch(size):
            return ([pltpu.VMEM((HEAD_PAD, size), F32)] * 4
                    + [pltpu.VMEM((rows, HEAD_PAD, width), BF16), pltpu.VMEM((rows, width), F32)])

        ctx, new_k, new_v = call(
            functools.partial(self_kernel, heads),
            [sds((rows, width), BF16)] + [sds((rows, width, length), BF16)] * 2,
            [HBM_SPEC] + [VMEM_SPEC] * 4 + [HBM_SPEC] * 2, [VMEM_SPEC] + [HBM_SPEC] * 2,
            [pltpu.VMEM((rows, width, length), BF16)] * 2 + [pltpu.VMEM((width, 128), F32)] * 2
            + attention_scratch(length) + [dma((2, rows)), dma((2, rows)), pltpu.SMEM((rows,), jnp.int32), dma],
            vmem=22 << 20,
        )(positions, q, k, v, brev, flat(self_k), flat(self_v))

        qc, h1 = call(
            functools.partial(mid_kernel, n),
            [sds((rows, width), BF16), sds((total, width), BF16)],
            [VMEM_SPEC] * 2 + [HBM_SPEC] * 3, [VMEM_SPEC] * 2,
            [w_tile, ln_tile, w_tile, dma((3,)), pltpu.VMEM((n, rows, width), BF16), pltpu.VMEM((n, total, cols), BF16),
             pltpu.VMEM((n, rows, cols), BF16), pltpu.VMEM((n, rows, cols), BF16)] + sems * 6,
            collective=1, vmem=8 << 20,
        )(ctx, hall, wo_self.T, ln_cross, wq_cross.T)

        ctx2 = call(
            functools.partial(cross_kernel, heads),
            sds((rows, width), BF16),
            [SMEM_SPEC] + [VMEM_SPEC] * 2 + [HBM_SPEC] * 2, VMEM_SPEC,
            [pltpu.VMEM((rows, width, source), BF16)] * 2 + attention_scratch(source) + [dma((2, rows))],
            vmem=52 << 20,
        )(lens, qc, enc_mask, flat(cross_k), flat(cross_v))

        out = call(
            functools.partial(ffn_kernel, n),
            sds((rows, width), BF16),
            [VMEM_SPEC] * 2 + [HBM_SPEC] * 6, VMEM_SPEC,
            [pltpu.VMEM((n, rows, width), BF16), pltpu.VMEM((n, total, cols), BF16),
             pltpu.VMEM((n, experts // n, width), F32), pltpu.VMEM((n, 1, rows), jnp.int32),
             pltpu.VMEM((total, width), BF16), pltpu.VMEM((total, 128), jnp.int32),
             pltpu.VMEM((experts, width, units), BF16), pltpu.VMEM((experts, units, width), BF16),
             pltpu.VMEM((total, units), BF16), pltpu.VMEM((total, units), BF16),
             pltpu.VMEM((n, rows, width), F32), pltpu.VMEM((n, rows, width), BF16),
             pltpu.VMEM((n, rows, width), F32)]
            + sems * 10 + [dma((experts,)), dma((experts,))]
            + [w_tile, ln_tile, pltpu.VMEM((experts // n, width), F32), pltpu.VMEM((1, rows), jnp.int32), dma((4,))],
            collective=2, vmem=41 << 20,
        )(ctx2, h1, wo_cross.T, ln_ffn, w_router.T, expert_idx[None, :], w_in, w_out)

        def unflat(cache):
            return jnp.swapaxes(cache.reshape(rows, heads, head_dim, length), 2, 3)

        return out, unflat(new_k), unflat(new_v)

    return jax.shard_map(decoder_block, mesh=mesh, in_specs=in_specs, out_specs=out_specs, check_vma=False)
```

```python
import functools
import jax
import jax.numpy as jnp
from jax import lax
from jax.experimental import pallas as pl
from jax.experimental.pallas import tpu as pltpu
from jax.sharding import PartitionSpec as P

EPSILON = 1e-6
NEG_BIG = -1e30
F32 = jnp.float32
BF16 = jnp.bfloat16
MESH = pl.DeviceIdType.MESH
VMEM_SPEC = pl.BlockSpec(memory_space=pltpu.VMEM)
SMEM_SPEC = pl.BlockSpec(memory_space=pltpu.SMEM)
HBM_SPEC = pl.BlockSpec(memory_space=pltpu.HBM)
VMEM_MAX = 67_000_000
HEAD_PAD = 16


def rms_norm(hidden, scale):
    hid = hidden.astype(F32)
    inv = lax.rsqrt(jnp.mean(hid * hid, axis=-1, keepdims=True) + EPSILON)
    return (hid * inv * scale).astype(BF16)


def dot_nn(a, b):
    return lax.dot_general(a, b, (((1,), (0,)), ((), ())), preferred_element_type=F32)


def dot_nt(a, b):
    return lax.dot_general(a, b, (((1,), (1,)), ((), ())), preferred_element_type=F32)


def entry_barrier(me, n):
    sem = pltpu.get_barrier_semaphore()
    for k in range(1, n):
        pl.semaphore_signal(sem, inc=1, device_id={"ws": lax.rem(me + k, n)}, device_id_type=MESH)
    pl.semaphore_wait(sem, n - 1)


def start_exchange(me, n, src_of, dst, send_sem, recv_sem):
    copies = []
    for k in range(1, n):
        peer = lax.rem(me + k, n)
        copy = pltpu.make_async_remote_copy(
            src_ref=src_of(peer), dst_ref=dst, send_sem=send_sem.at[k - 1], recv_sem=recv_sem.at[k - 1],
            device_id={"ws": peer}, device_id_type=MESH)
        copy.start()
        copies.append(copy)
    return copies


def wait_all(copies):
    for copy in copies:
        copy.wait()


def my_columns(full, me, n, width):
    picked = full[:, 0:width]
    for j in range(1, n):
        picked = jnp.where(me == j, full[:, j * width:(j + 1) * width], picked)
    return picked


def fetch(pairs, sem):
    copies = [pltpu.make_async_copy(src, dst, sem.at[i]) for i, (src, dst) in enumerate(pairs)]
    for copy in copies:
        copy.start()
    return copies


def read_rows(pairs, sem):
    def copy(i, r):
        return pltpu.make_async_copy(pairs[i][0].at[r], pairs[i][1].at[r], sem.at[i, r])
    rows = pairs[0][1].shape[0]

    def start():
        @pl.loop(0, rows)
        def _(r):
            for i in range(len(pairs)):
                copy(i, r).start()

    def wait():
        @pl.loop(0, rows)
        def _(r):
            for i in range(len(pairs)):
                copy(i, r).wait()
    return start, wait


def qkv_kernel(n, h_hbm, ln_hbm, wq_hbm, wk_hbm, wv_hbm, bias_hbm, mask_hbm, sk_hbm, sv_hbm,
               q_ref, k_ref, v_ref, hall_ref, brev_ref, lens_ref, sk_ref, sv_ref,
               h_ref, ln_ref, w_ref, bias_ref, mask_ref, hbuf, sendbuf, recvbuf, s1, r1, s2, r2, in_sem, row_sem):
    me = lax.axis_index("ws")
    rows, width = h_ref.shape
    cols = w_ref.shape[1]
    loads = fetch([(h_hbm, h_ref), (ln_hbm, ln_ref), (bias_hbm, bias_ref), (mask_hbm, mask_ref)]
                  + [(w, w_ref.at[i]) for i, w in enumerate((wq_hbm, wk_hbm, wv_hbm))], in_sem)
    start_rows, wait_rows = read_rows([(sk_hbm, sk_ref), (sv_hbm, sv_ref)], row_sem)
    start_rows()
    entry_barrier(me, n)
    loads[0].wait()
    copies = start_exchange(me, n, lambda p: h_ref, hbuf.at[me], s1, r1)
    hbuf[me] = h_ref[...]
    for load in loads[1:]:
        load.wait()
    lens_ref[...] = jnp.broadcast_to(jnp.sum(mask_ref[...], axis=1, keepdims=True), lens_ref.shape)
    heads, length = bias_ref.shape
    flip = (lax.broadcasted_iota(jnp.int32, (length, length), 0)
            + lax.broadcasted_iota(jnp.int32, (length, length), 1) == length - 1).astype(F32)
    brev_ref[...] = jnp.zeros_like(brev_ref)
    brev_ref[0:heads, :] = lax.dot_general(bias_ref[...], flip, (((1,), (0,)), ((), ())),
                                           precision=lax.Precision.HIGHEST, preferred_element_type=F32)
    wait_all(copies)
    hidden = hbuf[...].reshape(n * rows, width)
    hall_ref[...] = hidden
    x = rms_norm(hidden, ln_ref[...].reshape(1, width))
    for i in range(3):
        sendbuf[:, i] = dot_nt(x, w_ref[i]).astype(BF16).reshape(n, rows, cols)
    copies = start_exchange(me, n, lambda p: sendbuf.at[p], recvbuf.at[me], s2, r2)
    recvbuf[me] = sendbuf[me]
    wait_all(copies)
    for i, o in enumerate((q_ref, k_ref, v_ref)):
        o[...] = jnp.concatenate([recvbuf[j, i] for j in range(n)], axis=1)
    wait_rows()


def head_mask(shape, head_dim):
    head = lax.broadcasted_iota(jnp.int32, shape, 0)
    return lax.broadcasted_iota(jnp.int32, shape, 1) // head_dim == head


def spread_heads(q_ref, qblk, head_dim):
    rows, width = q_ref.shape
    q = q_ref[...].astype(F32)
    keep = head_mask((HEAD_PAD, width), head_dim)
    for r in range(rows):
        qblk[r] = jnp.where(keep, jnp.broadcast_to(q[r:r + 1], (HEAD_PAD, width)), 0.0).astype(BF16)


def softmax_rows(scores):
    top = jnp.max(scores, axis=-1, keepdims=True)
    e = jnp.exp(scores - top)
    return (e / jnp.sum(e, axis=-1, keepdims=True)).astype(BF16).astype(F32)


def weighted_values(prob, value, heads, head_dim, length):
    parts = []
    for h in range(heads):
        total = None
        for t in range(length // 128):
            lanes = slice(t * 128, (t + 1) * 128)
            term = value(slice(h * head_dim, (h + 1) * head_dim), t).astype(F32) * prob[h:h + 1, lanes]
            total = term if total is None else total + term
        parts.append(total)
    return jnp.sum(jnp.transpose(jnp.concatenate(parts, axis=0)), axis=0, keepdims=True)


def self_kernel(heads, pos_hbm, q_ref, k_ref, v_ref, brev_ref, sk_ref, sv_ref,
                ctx_ref, nk_ref, nv_ref,
                ktile, vtile, kt, vt, s0, s1, p0, p1, qblk, cf, xf, snew, out_sem, pos_ref, pos_sem):
    rows, width, length = sk_ref.shape
    head_dim = width // heads
    tiles = length // 128
    scalars = pltpu.make_async_copy(pos_hbm, pos_ref, pos_sem)
    scalars.start()

    pad = jnp.zeros((128 - rows, width), F32)
    kt[...] = jnp.transpose(jnp.concatenate([k_ref[...].astype(F32), pad], axis=0))
    vt[...] = jnp.transpose(jnp.concatenate([v_ref[...].astype(F32), pad], axis=0))
    spread_heads(q_ref, qblk, head_dim)
    snew[...] = dot_nn(qblk[...].reshape(rows * HEAD_PAD, width), kt[...].astype(BF16)).reshape(snew.shape)
    sbufs, pbufs = (s0, s1), (p0, p1)
    scalars.wait()

    def insert(r, cache, tile_buf, cols):
        pos = pos_ref[r]
        tile = pos // 128
        at = pos - tile * 128
        new = jnp.broadcast_to(cols[:, r:r + 1], (width, 128))
        old = cache[r, :, pl.ds(pl.multiple_of(tile * 128, 128), 128)]
        hit = lax.broadcasted_iota(jnp.int32, (width, 128), 1) == at
        tile_buf[r] = jnp.where(hit, new, old.astype(F32)).astype(BF16)

    def save(r):
        tile = pos_ref[r] // 128
        for i, (cache, tile_buf, dst) in enumerate(((sk_ref, ktile, nk_ref), (sv_ref, vtile, nv_ref))):
            for t in range(tiles):
                lanes = slice(t * 128, (t + 1) * 128)

                @pl.when(tile == t)
                def _():
                    pltpu.make_async_copy(tile_buf.at[r], dst.at[r, :, lanes], out_sem.at[i, r]).start()

                @pl.when(tile != t)
                def _():
                    pltpu.make_async_copy(cache.at[r, :, lanes], dst.at[r, :, lanes], out_sem.at[i, r]).start()

    def softmax(r):
        pos = pos_ref[r]
        bias = pltpu.roll(brev_ref[...], lax.rem(pos + 1, length), 1)
        lane = lax.broadcasted_iota(jnp.int32, (HEAD_PAD, length), 1)
        pick = lax.broadcasted_iota(jnp.int32, (HEAD_PAD, 128), 1) == r
        fresh = jnp.sum(jnp.where(pick, snew[r], 0.0), axis=-1, keepdims=True)
        scores = jnp.where(lane == pos, fresh, sbufs[r % 2][...]) + bias
        prob = softmax_rows(jnp.where(lane <= pos, scores, NEG_BIG))
        pbufs[r % 2][...] = jnp.where(lane == pos, 0.0, prob)
        at_pos = jnp.sum(jnp.where(lane == pos, prob, 0.0), axis=-1, keepdims=True)
        spread = jnp.where(head_mask((HEAD_PAD, width), head_dim), jnp.broadcast_to(at_pos, (HEAD_PAD, width)), 0.0)
        xf[r:r + 1, :] = jnp.sum(spread, axis=0, keepdims=True) * v_ref[r:r + 1, :].astype(F32)

    for step in range(rows + 2):
        if step >= 2:
            done = step - 2
            cf[done:done + 1, :] = xf[done:done + 1, :] + weighted_values(
                pbufs[done % 2], lambda d, t: sv_ref[done, d, t * 128:(t + 1) * 128], heads, head_dim, length)
        if 1 <= step < rows + 1:
            softmax(step - 1)
            save(step - 1)
        if step < rows:
            sbufs[step % 2][...] = dot_nn(qblk[step], sk_ref[step])
            insert(step, sk_ref, ktile, kt)
            insert(step, sv_ref, vtile, vt)

    ctx_ref[...] = cf[...].astype(BF16)
    for r in range(rows):
        pltpu.make_async_copy(sk_ref.at[r], nk_ref.at[r], out_sem.at[0, r]).wait()
        pltpu.make_async_copy(sv_ref.at[r], nv_ref.at[r], out_sem.at[1, r]).wait()


def mid_kernel(n, ctx_ref, hall_ref, wo_hbm, ln_hbm, wq_hbm, ck_hbm, cv_hbm,
               q_ref, h1_ref, ck_ref, cv_ref, wo_ref, ln_ref, wq_ref, in_sem, row_sem, cbuf, hpart, sendbuf, recvbuf, s1, r1, s2, r2, s3, r3):
    me = lax.axis_index("ws")
    rows, width = ctx_ref.shape
    cols = wo_ref.shape[0]
    loads = fetch([(wo_hbm, wo_ref), (ln_hbm, ln_ref), (wq_hbm, wq_ref)], in_sem)
    near = ck_ref.shape[2]
    start_rows, wait_rows = read_rows([(ck_hbm.at[:, :, 0:near], ck_ref), (cv_hbm.at[:, :, 0:near], cv_ref)], row_sem)
    start_rows()
    entry_barrier(me, n)
    copies = start_exchange(me, n, lambda p: ctx_ref, cbuf.at[me], s1, r1)
    cbuf[me] = ctx_ref[...]
    mine = my_columns(hall_ref[...].astype(F32), me, n, cols)
    wait_all(loads)
    wait_all(copies)
    attn = dot_nt(cbuf[...].reshape(n * rows, width), wo_ref[...])
    hpart[me] = (mine + attn).astype(BF16)
    copies = start_exchange(me, n, lambda p: hpart.at[me], hpart.at[me], s2, r2)
    wait_all(copies)
    h1 = jnp.concatenate([hpart[j] for j in range(n)], axis=1)
    h1_ref[...] = h1
    x = rms_norm(h1, ln_ref[...].reshape(1, width))
    sendbuf[...] = dot_nt(x, wq_ref[...]).astype(BF16).reshape(n, rows, cols)
    copies = start_exchange(me, n, lambda p: sendbuf.at[p], recvbuf.at[me], s3, r3)
    recvbuf[me] = sendbuf[me]
    wait_all(copies)
    q_ref[...] = jnp.concatenate([recvbuf[j] for j in range(n)], axis=1)
    wait_rows()


def cross_kernel(heads, lens_ref, q_ref, mask_ref, kn_ref, vn_ref, ck_ref, cv_ref,
                 ctx_ref, kbuf, vbuf, s0, s1, p0, p1, qblk, cf, in_sem):
    rows, width, near = kn_ref.shape
    length = near + kbuf.shape[2]
    head_dim = width // heads
    block = 256
    tiles, near_tiles = length // 128, near // 128

    def tile_count(r):
        return (lens_ref[r, 0] + 127) // 128

    def far_copies(r, body):
        count = tile_count(r)
        for t in range(near_tiles + 1, tiles + 1):
            @pl.when(count == t)
            def _(size=(t - near_tiles) * 128):
                body(lambda i: pltpu.make_async_copy(
                    (ck_ref, cv_ref)[i].at[r, :, near:near + size], (kbuf, vbuf)[i].at[r, :, 0:size], in_sem.at[i, r]))

    def per_block(r, body):
        blocks = (lens_ref[r, 0] + block - 1) // block
        for t in range(1, length // block + 1):
            @pl.when(blocks == t)
            def _(size=t * block):
                body(size)

    @pl.loop(0, rows)
    def _(r):
        far_copies(r, lambda copy: (copy(0).start(), copy(1).start()))

    spread_heads(q_ref, qblk, head_dim)

    @pl.loop(0, rows)
    def _(r):
        for t in range(near_tiles + 1, tiles, 2):
            @pl.when(tile_count(r) == t)
            def _(at=(t - near_tiles) * 128):
                vbuf[r, :, at:at + 128] = jnp.zeros((width, 128), BF16)

    def scores(r, size, out):
        first = min(size, near)
        out[:, 0:first] = dot_nn(qblk[r], kn_ref[r, :, 0:first])
        if size > near:
            out[:, near:size] = dot_nn(qblk[r], kbuf[r, :, 0:size - near])

    def softmax(r, src, out):
        keep = jnp.broadcast_to(mask_ref[pl.ds(r, 1), :], (HEAD_PAD, length)) == 1
        out[...] = softmax_rows(jnp.where(keep, src[...], NEG_BIG))

    def values(r, size, prob):
        def tile(d, t):
            if t < near_tiles:
                return vn_ref[r, d, t * 128:(t + 1) * 128]
            return vbuf[r, d, (t - near_tiles) * 128:(t - near_tiles + 1) * 128]
        cf[pl.ds(r, 1), :] = weighted_values(prob, tile, heads, head_dim, size)

    def arrived(r, i):
        far_copies(r, lambda copy: copy(i).wait())

    arrived(0, 0)
    per_block(0, lambda size: scores(0, size, s0))
    arrived(1, 0)

    def second(size):
        softmax(0, s0, p0)
        scores(1, size, s1)
    per_block(1, second)

    def step(r, sa, sb, pa, pb):
        arrived(r, 1)
        arrived(r + 2, 0)

        def outer(size_v):
            def inner(size_s):
                values(r, size_v, pa)
                softmax(r + 1, sb, pb)
                scores(r + 2, size_s, sa)
            per_block(r + 2, inner)
        per_block(r, outer)

    @pl.loop(0, (rows - 2) // 2)
    def _(i):
        step(2 * i, s0, s1, p0, p1)
        step(2 * i + 1, s1, s0, p1, p0)

    def last_but_one(size):
        values(rows - 2, size, p0)
        softmax(rows - 1, s1, p1)
    arrived(rows - 2, 1)
    per_block(rows - 2, last_but_one)
    arrived(rows - 1, 1)
    per_block(rows - 1, lambda size: values(rows - 1, size, p1))
    ctx_ref[...] = cf[...].astype(BF16)


def ffn_kernel(n, ctx_ref, h1_ref, wo_hbm, ln_hbm, wr_hbm, idx_hbm, win_ref, wout_ref,
               out_ref, cbuf, hpart, rbuf, ibuf, xbuf, mbuf, wi, wo, u0, u1, part, own, ybuf,
               s1, r1, s2, r2, s3, r3, s4, r4, s5, r5, wi_sem, wo_sem,
               wo_ref, ln_ref, wr_ref, idx_ref, in_sem):
    me = lax.axis_index("ws")
    rows, width = ctx_ref.shape
    cols = wo_ref.shape[0]
    experts = win_ref.shape[0]
    total = n * rows
    capacity = (2 * total + experts - 1) // experts

    def load(e, i):
        src, buf, sem = ((win_ref, wi, wi_sem), (wout_ref, wo, wo_sem))[i]
        return pltpu.make_async_copy(src.at[e], buf.at[e], sem.at[e])

    loads = fetch([(idx_hbm, idx_ref), (wr_hbm, wr_ref), (wo_hbm, wo_ref), (ln_hbm, ln_ref)], in_sem)

    @pl.loop(0, experts)
    def _(e):
        load(e, 0).start()
        load(e, 1).start()

    entry_barrier(me, n)
    wait_all(loads)
    first = (start_exchange(me, n, lambda p: ctx_ref, cbuf.at[me], s1, r1)
             + start_exchange(me, n, lambda p: idx_ref, ibuf.at[me], s2, r2)
             + start_exchange(me, n, lambda p: wr_ref, rbuf.at[me], s3, r3))
    cbuf[me] = ctx_ref[...]
    ibuf[me] = idx_ref[...]
    rbuf[me] = wr_ref[...]
    mine = my_columns(h1_ref[...].astype(F32), me, n, cols)
    wait_all(first)
    attn = dot_nt(cbuf[...].reshape(total, width), wo_ref[...])
    hpart[me] = (mine + attn).astype(BF16)
    copies = start_exchange(me, n, lambda p: hpart.at[me], hpart.at[me], s4, r4)

    idx_row = jnp.concatenate([ibuf[j] for j in range(n)], axis=1)
    grid_i = lax.broadcasted_iota(jnp.int32, (total, total), 0)
    grid_j = lax.broadcasted_iota(jnp.int32, (total, total), 1)
    row_b = jnp.broadcast_to(idx_row, (total, total))
    idx_col = jnp.sum(jnp.where(grid_i == grid_j, row_b, 0), axis=1, keepdims=True)
    earlier = (row_b == idx_col) & (grid_j < grid_i)
    slot = jnp.sum(earlier.astype(jnp.int32), axis=1, keepdims=True)
    target = jnp.where(slot < capacity, idx_col, -1)
    mbuf[...] = jnp.broadcast_to(target, mbuf.shape)

    wait_all(copies)
    h2 = jnp.concatenate([hpart[j] for j in range(n)], axis=1)
    x = rms_norm(h2, ln_ref[...].reshape(1, width))
    xbuf[...] = x
    own[...] = h2.reshape(n, rows, width)
    def hidden_units(e, buf):
        load(e, 0).wait()
        u = jnp.maximum(dot_nn(xbuf[...], wi[e]), 0.0)
        hit = jnp.broadcast_to(mbuf[:, 0:1], u.shape) == e
        buf[...] = jnp.where(hit, u, 0.0).astype(BF16)

    def add_output(e, buf):
        part[...] += dot_nn(buf[...], wo[e]).reshape(part.shape)

    part[...] = jnp.zeros_like(part)
    hidden_units(0, u0)

    @pl.loop(0, experts // 2)
    def _(i):
        e = i * 2
        load(e, 1).wait()
        hidden_units(e + 1, u1)
        add_output(e, u0)
        load(e + 1, 1).wait()

        @pl.when(e + 2 < experts)
        def _():
            hidden_units(e + 2, u0)
            add_output(e + 1, u1)

        @pl.when(e + 2 >= experts)
        def _():
            add_output(e + 1, u1)

    copies = start_exchange(me, n, lambda p: part.at[p], ybuf.at[me], s5, r5)
    ybuf[me] = part[me]

    my_rows = pl.ds(pl.multiple_of(me * rows, rows), rows)
    router = jnp.concatenate([rbuf[j] for j in range(n)], axis=0)
    logits = lax.dot_general(xbuf[my_rows, :].astype(F32), router, (((1,), (1,)), ((), ())),
                             precision=lax.Precision.HIGHEST, preferred_element_type=F32)
    probs = jnp.exp(logits - jnp.max(logits, axis=-1, keepdims=True))
    probs = probs / jnp.sum(probs, axis=-1, keepdims=True)
    chosen = lax.broadcasted_iota(jnp.int32, (rows, experts), 1) == mbuf[my_rows, :][:, 0:experts]
    gate = jnp.sum(jnp.where(chosen, probs, 0.0), axis=-1, keepdims=True)
    wait_all(copies)
    y = ybuf[0]
    for j in range(1, n):
        y = y + ybuf[j]
    out_ref[...] = (own[me].astype(F32) + y.astype(BF16).astype(F32) * gate).astype(BF16)


def call(body, out_shape, in_specs, out_specs, scratch, collective=None, flops=1_000_000, moved=1_000_000, vmem=VMEM_MAX):
    params = dict(vmem_limit_bytes=vmem)
    if collective is not None:
        params.update(collective_id=collective, has_side_effects=True)
    kernel = pl.pallas_call(
        body, out_shape=out_shape, in_specs=in_specs, out_specs=out_specs, scratch_shapes=scratch,
        compiler_params=pltpu.CompilerParams(**params),
        cost_estimate=pl.CostEstimate(flops=flops, bytes_accessed=moved, transcendentals=0))

    def run(*operands):
        return kernel(*[pltpu.with_memory_space_constraint(x, pltpu.HBM) if spec is HBM_SPEC else x
                        for x, spec in zip(operands, in_specs)])
    return run


def solution(mesh):
    n = mesh.shape['ws']
    row_axes = ('dp', 'ws')
    row_vec = P(row_axes)
    row_mat = P(row_axes, None)
    cache_spec = P(row_axes, None, None, None)
    col_split = P(None, 'ws')
    in_specs = (row_mat, cache_spec, cache_spec, cache_spec, cache_spec, row_vec, row_mat, P(None, None), row_vec,
                P(None), P(None), P(None), col_split, col_split, col_split, col_split, col_split, col_split,
                col_split, P(None, None, 'ws'), P(None, 'ws', None))
    out_specs = (row_mat, cache_spec, cache_spec)
    dma = pltpu.SemaphoreType.DMA

    def decoder_block(hidden, self_k, self_v, cross_k, cross_v, positions, enc_mask, rel_bias, expert_idx,
                      ln_self, ln_cross, ln_ffn, wq_self, wk_self, wv_self, wo_self, wq_cross, wo_cross,
                      w_router, w_in, w_out):
        rows, width = hidden.shape
        heads, length = rel_bias.shape
        head_dim = width // heads
        source = enc_mask.shape[1]
        cols = wq_self.shape[1]
        experts, _, units = w_in.shape
        total = n * rows
        sds = jax.ShapeDtypeStruct

        def flat(cache):
            return jnp.swapaxes(cache, 2, 3).reshape(rows, width, cache.shape[2])

        sems = [dma((n - 1,))]
        w_tile = pltpu.VMEM((cols, width), BF16)
        ln_tile = pltpu.VMEM((width,), F32)
        near = source // 2
        q, k, v, hall, brev, lens, near_sk, near_sv = call(
            functools.partial(qkv_kernel, n),
            [sds((rows, width), BF16)] * 3 + [sds((total, width), BF16), sds((HEAD_PAD, length), F32), sds((rows, 128), jnp.int32)]
            + [sds((rows, width, length), BF16)] * 2,
            [HBM_SPEC] * 9, [VMEM_SPEC] * 8,
            [pltpu.VMEM((rows, width), BF16), ln_tile, pltpu.VMEM((3, cols, width), BF16), pltpu.VMEM((heads, length), F32),
             pltpu.VMEM((rows, source), jnp.int32),
             pltpu.VMEM((n, rows, width), BF16), pltpu.VMEM((n, 3, rows, cols), BF16), pltpu.VMEM((n, 3, rows, cols), BF16)]
            + sems * 4 + [dma((7,)), dma((2, rows))],
            collective=0, vmem=8 << 20,
        )(hidden, ln_self, wq_self.T, wk_self.T, wv_self.T, rel_bias, enc_mask, flat(self_k), flat(self_v))

        def attention_scratch(size):
            return ([pltpu.VMEM((HEAD_PAD, size), F32)] * 4
                    + [pltpu.VMEM((rows, HEAD_PAD, width), BF16), pltpu.VMEM((rows, width), F32)])

        ctx, new_k, new_v = call(
            functools.partial(self_kernel, heads),
            [sds((rows, width), BF16)] + [sds((rows, width, length), BF16)] * 2,
            [HBM_SPEC] + [VMEM_SPEC] * 6, [VMEM_SPEC] + [HBM_SPEC] * 2,
            [pltpu.VMEM((rows, width, 128), BF16)] * 2 + [pltpu.VMEM((width, 128), F32)] * 2 + attention_scratch(length)
            + [pltpu.VMEM((rows, width), F32), pltpu.VMEM((rows, HEAD_PAD, 128), F32),
               dma((2, rows)), pltpu.SMEM((rows,), jnp.int32), dma],
            vmem=12 << 20,
        )(positions, q, k, v, brev, near_sk, near_sv)

        qc, h1, near_ck, near_cv = call(
            functools.partial(mid_kernel, n),
            [sds((rows, width), BF16), sds((total, width), BF16)] + [sds((rows, width, near), BF16)] * 2,
            [VMEM_SPEC] * 2 + [HBM_SPEC] * 5, [VMEM_SPEC] * 4,
            [w_tile, ln_tile, w_tile, dma((3,)), dma((2, rows)), pltpu.VMEM((n, rows, width), BF16), pltpu.VMEM((n, total, cols), BF16),
             pltpu.VMEM((n, rows, cols), BF16), pltpu.VMEM((n, rows, cols), BF16)] + sems * 6,
            collective=1, vmem=8 << 20,
        )(ctx, hall, wo_self.T, ln_cross, wq_cross.T, flat(cross_k), flat(cross_v))

        ctx2 = call(
            functools.partial(cross_kernel, heads),
            sds((rows, width), BF16),
            [SMEM_SPEC] + [VMEM_SPEC] * 4 + [HBM_SPEC] * 2, VMEM_SPEC,
            [pltpu.VMEM((rows, width, source - near), BF16)] * 2 + attention_scratch(source) + [dma((2, rows))],
            vmem=26 << 20,
        )(lens, qc, enc_mask, near_ck, near_cv, flat(cross_k), flat(cross_v))

        out = call(
            functools.partial(ffn_kernel, n),
            sds((rows, width), BF16),
            [VMEM_SPEC] * 2 + [HBM_SPEC] * 6, VMEM_SPEC,
            [pltpu.VMEM((n, rows, width), BF16), pltpu.VMEM((n, total, cols), BF16),
             pltpu.VMEM((n, experts // n, width), F32), pltpu.VMEM((n, 1, rows), jnp.int32),
             pltpu.VMEM((total, width), BF16), pltpu.VMEM((total, 128), jnp.int32),
             pltpu.VMEM((experts, width, units), BF16), pltpu.VMEM((experts, units, width), BF16),
             pltpu.VMEM((total, units), BF16), pltpu.VMEM((total, units), BF16),
             pltpu.VMEM((n, rows, width), F32), pltpu.VMEM((n, rows, width), BF16),
             pltpu.VMEM((n, rows, width), F32)]
            + sems * 10 + [dma((experts,)), dma((experts,))]
            + [w_tile, ln_tile, pltpu.VMEM((experts // n, width), F32), pltpu.VMEM((1, rows), jnp.int32), dma((4,))],
            collective=2, vmem=41 << 20,
        )(ctx2, h1, wo_cross.T, ln_ffn, w_router.T, expert_idx[None, :], w_in, w_out)

        def unflat(cache):
            return jnp.swapaxes(cache.reshape(rows, heads, head_dim, length), 2, 3)

        return out, unflat(new_k), unflat(new_v)

    return jax.shard_map(decoder_block, mesh=mesh, in_specs=in_specs, out_specs=out_specs, check_vma=False)
```

```python
import functools
import jax
import jax.numpy as jnp
from jax import lax
from jax.experimental import pallas as pl
from jax.experimental.pallas import tpu as pltpu
from jax.sharding import PartitionSpec as P

EPSILON = 1e-6
NEG_BIG = -1e30
F32 = jnp.float32
BF16 = jnp.bfloat16
MESH = pl.DeviceIdType.MESH
VMEM_SPEC = pl.BlockSpec(memory_space=pltpu.VMEM)
SMEM_SPEC = pl.BlockSpec(memory_space=pltpu.SMEM)
HBM_SPEC = pl.BlockSpec(memory_space=pltpu.HBM)
VMEM_MAX = 67_000_000
HEAD_PAD = 16
NEAR, SLOTS, EARLY = 512, 8, 4
VM3, VM4, VM5 = 8, 14, 39


def rms_norm(hidden, scale):
    hid = hidden.astype(F32)
    inv = lax.rsqrt(jnp.mean(hid * hid, axis=-1, keepdims=True) + EPSILON)
    return (hid * inv * scale).astype(BF16)


def dot_nn(a, b):
    return lax.dot_general(a, b, (((1,), (0,)), ((), ())), preferred_element_type=F32)


def dot_nt(a, b):
    return lax.dot_general(a, b, (((1,), (1,)), ((), ())), preferred_element_type=F32)


def entry_barrier(me, n, across=None):
    sem = pltpu.get_barrier_semaphore()
    for k in range(1, n):
        pl.semaphore_signal(sem, inc=1, device_id={"ws": lax.rem(me + k, n)}, device_id_type=MESH)
    if across is not None:
        pl.semaphore_signal(sem, inc=1, device_id=across, device_id_type=MESH)
    pl.semaphore_wait(sem, n - 1 if across is None else n)


def send(src, dst, send_sem, recv_sem, device):
    copy = pltpu.make_async_remote_copy(src_ref=src, dst_ref=dst, send_sem=send_sem, recv_sem=recv_sem,
                                        device_id=device, device_id_type=MESH)
    copy.start()
    return copy


def start_exchange(me, n, src_of, dst, send_sem, recv_sem):
    copies = []
    for k in range(1, n):
        peer = lax.rem(me + k, n)
        copy = pltpu.make_async_remote_copy(
            src_ref=src_of(peer), dst_ref=dst, send_sem=send_sem.at[k - 1], recv_sem=recv_sem.at[k - 1],
            device_id={"ws": peer}, device_id_type=MESH)
        copy.start()
        copies.append(copy)
    return copies


def wait_all(copies):
    for copy in copies:
        copy.wait()


def my_columns(full, me, n, width):
    picked = full[:, 0:width]
    for j in range(1, n):
        picked = jnp.where(me == j, full[:, j * width:(j + 1) * width], picked)
    return picked


def fetch(pairs, sem):
    copies = [pltpu.make_async_copy(src, dst, sem.at[i]) for i, (src, dst) in enumerate(pairs)]
    for copy in copies:
        copy.start()
    return copies


def read_rows(pairs, sem):
    def copy(i, r):
        return pltpu.make_async_copy(pairs[i][0].at[r], pairs[i][1].at[r], sem.at[i, r])
    rows = pairs[0][1].shape[0]

    def start():
        @pl.loop(0, rows)
        def _(r):
            for i in range(len(pairs)):
                copy(i, r).start()

    def wait():
        @pl.loop(0, rows)
        def _(r):
            for i in range(len(pairs)):
                copy(i, r).wait()
    return start, wait


def qkv_kernel(n, h_hbm, ln_hbm, wq_hbm, wk_hbm, wv_hbm, bias_hbm, mask_hbm, wc_hbm, sk_hbm, sv_hbm,
               q_ref, k_ref, v_ref, hall_ref, brev_ref, lens_ref, wc_half, sk_ref, sv_ref,
               h_ref, ln_ref, w_ref, bias_ref, mask_ref, hbuf, sendbuf, recvbuf, s1, r1, s2, r2, in_sem, row_sem,
               wc_own, swc, rwc):
    me = lax.axis_index("ws")
    rows, width = h_ref.shape
    cols = w_ref.shape[1]
    half = cols // 2
    start = pl.multiple_of(lax.axis_index("dp") * half, 16)
    loads = fetch([(h_hbm, h_ref), (wc_hbm.at[pl.ds(start, half)], wc_own), (ln_hbm, ln_ref), (bias_hbm, bias_ref), (mask_hbm, mask_ref)]
                  + [(w, w_ref.at[i]) for i, w in enumerate((wq_hbm, wk_hbm, wv_hbm))], in_sem)
    start_rows, wait_rows = read_rows([(sk_hbm, sk_ref), (sv_hbm, sv_ref)], row_sem)
    start_rows()
    entry_barrier(me, n)
    loads[0].wait()
    copies = start_exchange(me, n, lambda p: h_ref, hbuf.at[me], s1, r1)
    hbuf[me] = h_ref[...]
    other = {"ws": lax.rem(me + n // 2, n)}
    loads[1].wait()
    cut = 80
    bulk = [send(wc_own.at[0:cut], wc_half.at[0:cut], swc.at[0], rwc.at[0], other)]
    for load in loads[2:]:
        load.wait()
    lens_ref[...] = jnp.broadcast_to(jnp.sum(mask_ref[...], axis=1, keepdims=True), lens_ref.shape)
    heads, length = bias_ref.shape
    flip = (lax.broadcasted_iota(jnp.int32, (length, length), 0)
            + lax.broadcasted_iota(jnp.int32, (length, length), 1) == length - 1).astype(F32)
    brev_ref[...] = jnp.zeros_like(brev_ref)
    brev_ref[0:heads, :] = lax.dot_general(bias_ref[...], flip, (((1,), (0,)), ((), ())),
                                           precision=lax.Precision.HIGHEST, preferred_element_type=F32)
    wait_all(copies)
    hidden = hbuf[...].reshape(n * rows, width)
    hall_ref[...] = hidden
    x = rms_norm(hidden, ln_ref[...].reshape(1, width))
    for i in range(3):
        sendbuf[:, i] = dot_nt(x, w_ref[i]).astype(BF16).reshape(n, rows, cols)
    copies = start_exchange(me, n, lambda p: sendbuf.at[p], recvbuf.at[me], s2, r2)
    bulk.append(send(wc_own.at[cut:half], wc_half.at[cut:half], swc.at[1], rwc.at[1], other))
    recvbuf[me] = sendbuf[me]
    wait_all(copies)
    for i, o in enumerate((q_ref, k_ref, v_ref)):
        o[...] = jnp.concatenate([recvbuf[j, i] for j in range(n)], axis=1)
    wait_all(bulk)
    wait_rows()


def head_mask(shape, head_dim):
    head = lax.broadcasted_iota(jnp.int32, shape, 0)
    return lax.broadcasted_iota(jnp.int32, shape, 1) // head_dim == head


def spread_heads(q_ref, qblk, head_dim):
    rows, width = q_ref.shape
    q = q_ref[...].astype(F32)
    keep = head_mask((HEAD_PAD, width), head_dim)
    for r in range(rows):
        qblk[r] = jnp.where(keep, jnp.broadcast_to(q[r:r + 1], (HEAD_PAD, width)), 0.0).astype(BF16)


def softmax_rows(scores):
    top = jnp.max(scores, axis=-1, keepdims=True)
    e = jnp.exp(scores - top)
    return (e / jnp.sum(e, axis=-1, keepdims=True)).astype(BF16).astype(F32)


def weighted_values(prob, value, heads, head_dim, length):
    parts = []
    for h in range(heads):
        total = None
        for t in range(length // 128):
            lanes = slice(t * 128, (t + 1) * 128)
            term = value(slice(h * head_dim, (h + 1) * head_dim), t).astype(F32) * prob[h:h + 1, lanes]
            total = term if total is None else total + term
        parts.append(total)
    return jnp.sum(jnp.transpose(jnp.concatenate(parts, axis=0)), axis=0, keepdims=True)


def self_kernel(heads, pos_hbm, q_ref, k_ref, v_ref, brev_ref, sk_ref, sv_ref,
                ctx_ref, nk_ref, nv_ref,
                ktile, vtile, kt, vt, s0, s1, p0, p1, qblk, cf, xf, snew, out_sem, pos_ref, pos_sem):
    rows, width, length = sk_ref.shape
    head_dim = width // heads
    tiles = length // 128
    scalars = pltpu.make_async_copy(pos_hbm, pos_ref, pos_sem)
    scalars.start()

    pad = jnp.zeros((128 - rows, width), F32)
    kt[...] = jnp.transpose(jnp.concatenate([k_ref[...].astype(F32), pad], axis=0))
    vt[...] = jnp.transpose(jnp.concatenate([v_ref[...].astype(F32), pad], axis=0))
    spread_heads(q_ref, qblk, head_dim)
    snew[...] = dot_nn(qblk[...].reshape(rows * HEAD_PAD, width), kt[...].astype(BF16)).reshape(snew.shape)
    sbufs, pbufs = (s0, s1), (p0, p1)
    scalars.wait()

    def insert(r, cache, tile_buf, cols):
        pos = pos_ref[r]
        tile = pos // 128
        at = pos - tile * 128
        new = jnp.broadcast_to(cols[:, r:r + 1], (width, 128))
        old = cache[r, :, pl.ds(pl.multiple_of(tile * 128, 128), 128)]
        hit = lax.broadcasted_iota(jnp.int32, (width, 128), 1) == at
        tile_buf[r] = jnp.where(hit, new, old.astype(F32)).astype(BF16)

    def save(r):
        tile = pos_ref[r] // 128
        for i, (cache, tile_buf, dst) in enumerate(((sk_ref, ktile, nk_ref), (sv_ref, vtile, nv_ref))):
            for t in range(tiles):
                lanes = slice(t * 128, (t + 1) * 128)

                @pl.when(tile == t)
                def _():
                    pltpu.make_async_copy(tile_buf.at[r], dst.at[r, :, lanes], out_sem.at[i, r]).start()

                @pl.when(tile != t)
                def _():
                    pltpu.make_async_copy(cache.at[r, :, lanes], dst.at[r, :, lanes], out_sem.at[i, r]).start()

    def softmax(r):
        pos = pos_ref[r]
        bias = pltpu.roll(brev_ref[...], lax.rem(pos + 1, length), 1)
        lane = lax.broadcasted_iota(jnp.int32, (HEAD_PAD, length), 1)
        pick = lax.broadcasted_iota(jnp.int32, (HEAD_PAD, 128), 1) == r
        fresh = jnp.sum(jnp.where(pick, snew[r], 0.0), axis=-1, keepdims=True)
        scores = jnp.where(lane == pos, fresh, sbufs[r % 2][...]) + bias
        prob = softmax_rows(jnp.where(lane <= pos, scores, NEG_BIG))
        pbufs[r % 2][...] = jnp.where(lane == pos, 0.0, prob)
        at_pos = jnp.sum(jnp.where(lane == pos, prob, 0.0), axis=-1, keepdims=True)
        spread = jnp.where(head_mask((HEAD_PAD, width), head_dim), jnp.broadcast_to(at_pos, (HEAD_PAD, width)), 0.0)
        xf[r:r + 1, :] = jnp.sum(spread, axis=0, keepdims=True) * v_ref[r:r + 1, :].astype(F32)

    for step in range(rows + 2):
        if step >= 2:
            done = step - 2
            cf[done:done + 1, :] = xf[done:done + 1, :] + weighted_values(
                pbufs[done % 2], lambda d, t: sv_ref[done, d, t * 128:(t + 1) * 128], heads, head_dim, length)
        if 1 <= step < rows + 1:
            softmax(step - 1)
            save(step - 1)
        if step < rows:
            sbufs[step % 2][...] = dot_nn(qblk[step], sk_ref[step])
            insert(step, sk_ref, ktile, kt)
            insert(step, sv_ref, vtile, vt)

    ctx_ref[...] = cf[...].astype(BF16)
    for r in range(rows):
        pltpu.make_async_copy(sk_ref.at[r], nk_ref.at[r], out_sem.at[0, r]).wait()
        pltpu.make_async_copy(sv_ref.at[r], nv_ref.at[r], out_sem.at[1, r]).wait()


def mid_kernel(n, ctx_ref, hall_ref, wo_hbm, ln_hbm, wq_hbm, wr_hbm, idx_hbm, wc_half, wc_hbm, ck_hbm, cv_hbm, win_hbm,
               q_ref, h1_ref, wr_ref, idx_ref, wc_ref, ck_ref, cv_ref, win_ref, wr_own, idx_own, sr, rr, si, ri, wc_own, sw, rw, wo_ref, ln_ref, wq_ref, in_sem, row_sem, win_sem, cbuf, hpart, sendbuf, recvbuf, s1, r1, s2, r2, s3, r3):
    me = lax.axis_index("ws")
    rows, width = ctx_ref.shape
    cols = wo_ref.shape[0]
    loads = fetch([(wo_hbm, wo_ref), (ln_hbm, ln_ref), (wq_hbm, wq_ref), (wr_hbm, wr_own), (idx_hbm, idx_own), (wc_hbm, wc_own)], in_sem)
    near = ck_ref.shape[2]
    start_rows, wait_rows = read_rows([(ck_hbm.at[:, :, 0:near], ck_ref), (cv_hbm.at[:, :, 0:near], cv_ref)], row_sem)
    start_win, wait_win = read_rows([(win_hbm, win_ref)], win_sem)
    start_rows()
    start_win()
    group = lax.axis_index("dp")
    facing, sibling = lax.rem(me + n // 2, n), me + 1 - 2 * lax.rem(me, 2)
    half = cols // 2
    mine_half = pl.ds(pl.multiple_of(group * half, 16), half)
    its_half = pl.ds(pl.multiple_of((1 - group) * half, 16), half)
    across = {"dp": 1 - group, "ws": me}
    entry_barrier(me, n, across)
    copies = start_exchange(me, n, lambda p: ctx_ref, cbuf.at[me], s1, r1)
    swap = send(wc_half, wc_ref.at[facing, mine_half], sw.at[0], rw.at[0], across)
    bulk = [send(wc_half, wc_ref.at[facing, mine_half], sw.at[1], rw.at[1], {"ws": sibling})]
    cbuf[me] = ctx_ref[...]
    mine = my_columns(hall_ref[...].astype(F32), me, n, cols)
    wait_all(loads)
    bulk.append(send(wc_own, wc_ref.at[me], sw.at[2], rw.at[2], {"ws": sibling}))
    wc_ref[me] = wc_own[...]
    wc_ref[facing, mine_half] = wc_half[...]
    wait_all(copies)
    attn = dot_nt(cbuf[...].reshape(n * rows, width), wo_ref[...])
    hpart[me] = (mine + attn).astype(BF16)
    copies = start_exchange(me, n, lambda p: hpart.at[me], hpart.at[me], s2, r2)
    wait_all(copies)
    h1 = jnp.concatenate([hpart[j] for j in range(n)], axis=1)
    h1_ref[...] = h1
    x = rms_norm(h1, ln_ref[...].reshape(1, width))
    sendbuf[...] = dot_nt(x, wq_ref[...]).astype(BF16).reshape(n, rows, cols)
    copies = (start_exchange(me, n, lambda p: sendbuf.at[p], recvbuf.at[me], s3, r3)
              + start_exchange(me, n, lambda p: wr_own, wr_ref.at[me], sr, rr)
              + start_exchange(me, n, lambda p: idx_own, idx_ref.at[me], si, ri))
    recvbuf[me] = sendbuf[me]
    wr_ref[me] = wr_own[...]
    idx_ref[me] = idx_own[...]
    swap.wait()
    bulk.append(send(wc_ref.at[facing, its_half], wc_ref.at[facing, its_half], sw.at[3], rw.at[3], {"ws": sibling}))
    wait_all(copies)
    q_ref[...] = jnp.concatenate([recvbuf[j] for j in range(n)], axis=1)
    wait_all(bulk)
    wait_rows()
    wait_win()


def cross_kernel(heads, lens_ref, q_ref, mask_ref, kn_ref, vn_ref, ck_ref, cv_ref,
                 ctx_ref, kbuf, vbuf, s0, s1, p0, p1, qblk, cf, in_sem):
    rows, width, near = kn_ref.shape
    slots = kbuf.shape[0]
    length = near + kbuf.shape[2]
    head_dim = width // heads
    block = 256
    tiles, near_tiles = length // 128, near // 128

    def slot(r):
        return lax.rem(r, slots)

    def tile_count(r):
        return (lens_ref[r, 0] + 127) // 128

    def far_copies(r, body):
        count = tile_count(r)
        for t in range(near_tiles + 1, tiles + 1):
            @pl.when(count == t)
            def _(size=(t - near_tiles) * 128):
                body(lambda i: pltpu.make_async_copy(
                    (ck_ref, cv_ref)[i].at[r, :, near:near + size], (kbuf, vbuf)[i].at[slot(r), :, 0:size],
                    in_sem.at[i, slot(r)]))

    def far_start(r):
        far_copies(r, lambda copy: (copy(0).start(), copy(1).start()))
        for t in [t for t in range(1, tiles, 2) if t >= near_tiles]:
            @pl.when(tile_count(r) == t)
            def _(at=(t - near_tiles) * 128):
                vbuf[slot(r), :, at:at + 128] = jnp.zeros((width, 128), BF16)

    def per_block(r, body):
        blocks = (lens_ref[r, 0] + block - 1) // block
        for t in range(1, length // block + 1):
            @pl.when(blocks == t)
            def _(size=t * block):
                body(size)

    @pl.loop(0, slots)
    def _(r):
        far_start(r)

    spread_heads(q_ref, qblk, head_dim)

    def scores(r, size, out):
        first = min(size, near)
        out[:, 0:first] = dot_nn(qblk[r], kn_ref[r, :, 0:first])
        if size > near:
            out[:, near:size] = dot_nn(qblk[r], kbuf[slot(r), :, 0:size - near])

    def softmax(r, src, out):
        keep = jnp.broadcast_to(mask_ref[pl.ds(r, 1), :], (HEAD_PAD, length)) == 1
        out[...] = softmax_rows(jnp.where(keep, src[...], NEG_BIG))

    def values(r, size, prob):
        def tile(d, t):
            if t < near_tiles:
                return vn_ref[r, d, t * 128:(t + 1) * 128]
            return vbuf[slot(r), d, (t - near_tiles) * 128:(t - near_tiles + 1) * 128]
        cf[pl.ds(r, 1), :] = weighted_values(prob, tile, heads, head_dim, size)

    def arrived(r, i):
        far_copies(r, lambda copy: copy(i).wait())

    arrived(0, 0)
    per_block(0, lambda size: scores(0, size, s0))
    arrived(1, 0)

    def second(size):
        softmax(0, s0, p0)
        scores(1, size, s1)
    per_block(1, second)

    def step(r, sa, sb, pa, pb):
        arrived(r, 1)
        arrived(r + 2, 0)

        def outer(size_v):
            def inner(size_s):
                values(r, size_v, pa)
                softmax(r + 1, sb, pb)
                scores(r + 2, size_s, sa)
            per_block(r + 2, inner)
        per_block(r, outer)

        @pl.when(r + slots < rows)
        def _():
            far_start(r + slots)

    @pl.loop(0, (rows - 2) // 2)
    def _(i):
        step(2 * i, s0, s1, p0, p1)
        step(2 * i + 1, s1, s0, p1, p0)

    def last_but_one(size):
        values(rows - 2, size, p0)
        softmax(rows - 1, s1, p1)
    arrived(rows - 2, 1)
    per_block(rows - 2, last_but_one)
    arrived(rows - 1, 1)
    per_block(rows - 1, lambda size: values(rows - 1, size, p1))
    ctx_ref[...] = cf[...].astype(BF16)


def ffn_kernel(n, ctx_ref, h1_ref, wo_ref, ln_hbm, rbuf, ibuf, early_ref, win_ref, wout_ref,
               out_ref, cbuf, xbuf, mbuf, wi, wo, ubuf, part, own, ybuf,
               s1, r1, s5, r5, wi_sem, wo_sem, ln_ref, in_sem):
    me = lax.axis_index("ws")
    rows, width = ctx_ref.shape
    experts = win_ref.shape[0]
    total = n * rows
    capacity = (2 * total + experts - 1) // experts

    early = early_ref.shape[0]

    def load(e, i):
        if i == 0:
            return pltpu.make_async_copy(win_ref.at[e + early], wi.at[e], wi_sem.at[e])
        return pltpu.make_async_copy(wout_ref.at[e], wo.at[e], wo_sem.at[e])

    loads = fetch([(ln_hbm, ln_ref)], in_sem)

    for i in range(2):
        @pl.loop(0, experts - early if i == 0 else experts)
        def _(e, i=i):
            load(e, i).start()

    entry_barrier(me, n)
    copies = start_exchange(me, n, lambda p: ctx_ref, cbuf.at[me], s1, r1)
    cbuf[me] = ctx_ref[...]

    idx_row = jnp.concatenate([ibuf[j] for j in range(n)], axis=1)
    grid_i = lax.broadcasted_iota(jnp.int32, (total, total), 0)
    grid_j = lax.broadcasted_iota(jnp.int32, (total, total), 1)
    row_b = jnp.broadcast_to(idx_row, (total, total))
    idx_col = jnp.sum(jnp.where(grid_i == grid_j, row_b, 0), axis=1, keepdims=True)
    earlier = (row_b == idx_col) & (grid_j < grid_i)
    slot = jnp.sum(earlier.astype(jnp.int32), axis=1, keepdims=True)
    target = jnp.where(slot < capacity, idx_col, -1)
    mbuf[...] = jnp.broadcast_to(target, mbuf.shape)

    wait_all(loads)
    wait_all(copies)
    attn = dot_nt(cbuf[...].reshape(total, width), wo_ref[...].reshape(width, width))
    h2 = (h1_ref[...].astype(F32) + attn).astype(BF16)
    x = rms_norm(h2, ln_ref[...].reshape(1, width))
    xbuf[...] = x
    own[...] = h2.reshape(n, rows, width)
    def hidden_units(e, weight):
        u = jnp.maximum(dot_nn(xbuf[...], weight), 0.0)
        hit = jnp.broadcast_to(mbuf[:, 0:1], u.shape) == e
        ubuf[e] = jnp.where(hit, u, 0.0).astype(BF16)

    @pl.loop(0, early // 2)
    def _(i):
        for k in range(2):
            hidden_units(i * 2 + k, early_ref[i * 2 + k])

    @pl.loop(0, (experts - early) // 2)
    def _(i):
        for k in range(2):
            load(i * 2 + k, 0).wait()
        for k in range(2):
            hidden_units(early + i * 2 + k, wi[i * 2 + k])

    sends = []
    block = part.shape[-1]
    for c in range(width // block):
        lanes = slice(c * block, (c + 1) * block)

        def add_output(i, total, c=c, lanes=lanes):
            if c == 0:
                for k in range(4):
                    load(i * 4 + k, 1).wait()
            for k in range(4):
                total = total + dot_nn(ubuf[i * 4 + k], wo[i * 4 + k, :, lanes])
            return total
        sums = lax.fori_loop(0, experts // 4, add_output, jnp.zeros((total, block), F32))
        part[c] = sums.reshape(n, rows, block)
        sends += start_exchange(me, n, lambda p: part.at[c, p], ybuf.at[c, me], s5.at[c], r5.at[c])
        ybuf[c, me] = part[c, me]
    copies = sends

    my_rows = pl.ds(pl.multiple_of(me * rows, rows), rows)
    router = jnp.concatenate([rbuf[j] for j in range(n)], axis=0)
    logits = lax.dot_general(xbuf[my_rows, :].astype(F32), router, (((1,), (1,)), ((), ())),
                             precision=lax.Precision.HIGHEST, preferred_element_type=F32)
    probs = jnp.exp(logits - jnp.max(logits, axis=-1, keepdims=True))
    probs = probs / jnp.sum(probs, axis=-1, keepdims=True)
    chosen = lax.broadcasted_iota(jnp.int32, (rows, experts), 1) == mbuf[my_rows, :][:, 0:experts]
    gate = jnp.sum(jnp.where(chosen, probs, 0.0), axis=-1, keepdims=True)
    wait_all(copies)
    y = jnp.concatenate([sum(ybuf[c, j] for j in range(1, n)) + ybuf[c, 0] for c in range(width // block)], axis=1)
    out_ref[...] = (own[me].astype(F32) + y.astype(BF16).astype(F32) * gate).astype(BF16)


def call(body, out_shape, in_specs, out_specs, scratch, collective=None, flops=1_000_000, moved=1_000_000, vmem=VMEM_MAX):
    params = dict(vmem_limit_bytes=vmem)
    if collective is not None:
        params.update(collective_id=collective, has_side_effects=True)
    kernel = pl.pallas_call(
        body, out_shape=out_shape, in_specs=in_specs, out_specs=out_specs, scratch_shapes=scratch,
        compiler_params=pltpu.CompilerParams(**params),
        cost_estimate=pl.CostEstimate(flops=flops, bytes_accessed=moved, transcendentals=0))

    def run(*operands):
        return kernel(*[pltpu.with_memory_space_constraint(x, pltpu.HBM) if spec is HBM_SPEC else x
                        for x, spec in zip(operands, in_specs)])
    return run


def solution(mesh):
    n = mesh.shape['ws']
    row_axes = ('dp', 'ws')
    row_vec = P(row_axes)
    row_mat = P(row_axes, None)
    cache_spec = P(row_axes, None, None, None)
    col_split = P(None, 'ws')
    in_specs = (row_mat, cache_spec, cache_spec, cache_spec, cache_spec, row_vec, row_mat, P(None, None), row_vec,
                P(None), P(None), P(None), col_split, col_split, col_split, col_split, col_split, col_split,
                col_split, P(None, None, 'ws'), P(None, 'ws', None))
    out_specs = (row_mat, cache_spec, cache_spec)
    dma = pltpu.SemaphoreType.DMA

    def decoder_block(hidden, self_k, self_v, cross_k, cross_v, positions, enc_mask, rel_bias, expert_idx,
                      ln_self, ln_cross, ln_ffn, wq_self, wk_self, wv_self, wo_self, wq_cross, wo_cross,
                      w_router, w_in, w_out):
        rows, width = hidden.shape
        heads, length = rel_bias.shape
        head_dim = width // heads
        source = enc_mask.shape[1]
        cols = wq_self.shape[1]
        experts, _, units = w_in.shape
        total = n * rows
        sds = jax.ShapeDtypeStruct

        def flat(cache):
            return jnp.swapaxes(cache, 2, 3).reshape(rows, width, cache.shape[2])

        sems = [dma((n - 1,))]
        w_tile = pltpu.VMEM((cols, width), BF16)
        ln_tile = pltpu.VMEM((width,), F32)
        near, slots, early = NEAR, SLOTS, EARLY
        q, k, v, hall, brev, lens, wc_half, near_sk, near_sv = call(
            functools.partial(qkv_kernel, n),
            [sds((rows, width), BF16)] * 3 + [sds((total, width), BF16), sds((HEAD_PAD, length), F32), sds((rows, 128), jnp.int32),
               sds((cols // 2, width), BF16)]
            + [sds((rows, width, length), BF16)] * 2,
            [HBM_SPEC] * 10, [VMEM_SPEC] * 9,
            [pltpu.VMEM((rows, width), BF16), ln_tile, pltpu.VMEM((3, cols, width), BF16), pltpu.VMEM((heads, length), F32),
             pltpu.VMEM((rows, source), jnp.int32),
             pltpu.VMEM((n, rows, width), BF16), pltpu.VMEM((n, 3, rows, cols), BF16), pltpu.VMEM((n, 3, rows, cols), BF16)]
            + sems * 4 + [dma((8,)), dma((2, rows)), pltpu.VMEM((cols // 2, width), BF16), dma((2,)), dma((2,))],
            collective=0, vmem=8 << 20,
        )(hidden, ln_self, wq_self.T, wk_self.T, wv_self.T, rel_bias, enc_mask, wo_cross.T, flat(self_k), flat(self_v))

        def attention_scratch(size):
            return ([pltpu.VMEM((HEAD_PAD, size), F32)] * 4
                    + [pltpu.VMEM((rows, HEAD_PAD, width), BF16), pltpu.VMEM((rows, width), F32)])

        ctx, new_k, new_v = call(
            functools.partial(self_kernel, heads),
            [sds((rows, width), BF16)] + [sds((rows, width, length), BF16)] * 2,
            [HBM_SPEC] + [VMEM_SPEC] * 6, [VMEM_SPEC] + [HBM_SPEC] * 2,
            [pltpu.VMEM((rows, width, 128), BF16)] * 2 + [pltpu.VMEM((width, 128), F32)] * 2 + attention_scratch(length)
            + [pltpu.VMEM((rows, width), F32), pltpu.VMEM((rows, HEAD_PAD, 128), F32),
               dma((2, rows)), pltpu.SMEM((rows,), jnp.int32), dma],
            vmem=12 << 20,
        )(positions, q, k, v, brev, near_sk, near_sv)

        qc, h1, router, chosen, wc_full, near_ck, near_cv, early_w = call(
            functools.partial(mid_kernel, n),
            [sds((rows, width), BF16), sds((total, width), BF16), sds((n, experts // n, width), F32), sds((n, 1, rows), jnp.int32),
               sds((n, cols, width), BF16)]
            + [sds((rows, width, near), BF16)] * 2
            + [sds((early, width, units), BF16)],
            [VMEM_SPEC] * 2 + [HBM_SPEC] * 5 + [VMEM_SPEC] + [HBM_SPEC] * 4, [VMEM_SPEC] * 8,
            [pltpu.VMEM((experts // n, width), F32), pltpu.VMEM((1, rows), jnp.int32)] + sems * 4
            + [w_tile, dma((4,)), dma((4,)), w_tile, ln_tile, w_tile, dma((6,)), dma((2, rows)), dma((1, early)), pltpu.VMEM((n, rows, width), BF16), pltpu.VMEM((n, total, cols), BF16),
             pltpu.VMEM((n, rows, cols), BF16), pltpu.VMEM((n, rows, cols), BF16)] + sems * 6,
            collective=1, vmem=VM3 << 20,
        )(ctx, hall, wo_self.T, ln_cross, wq_cross.T, w_router.T, expert_idx[None, :], wc_half, wo_cross.T, flat(cross_k), flat(cross_v), w_in)

        ctx2 = call(
            functools.partial(cross_kernel, heads),
            sds((rows, width), BF16),
            [SMEM_SPEC] + [VMEM_SPEC] * 4 + [HBM_SPEC] * 2, VMEM_SPEC,
            [pltpu.VMEM((slots, width, source - near), BF16)] * 2 + attention_scratch(source) + [dma((2, slots))],
            vmem=VM4 << 20,
        )(lens, qc, enc_mask, near_ck, near_cv, flat(cross_k), flat(cross_v))

        parts = 3
        out = call(
            functools.partial(ffn_kernel, n),
            sds((rows, width), BF16),
            [VMEM_SPEC] * 3 + [HBM_SPEC] + [VMEM_SPEC] * 3 + [HBM_SPEC] * 2, VMEM_SPEC,
            [pltpu.VMEM((n, rows, width), BF16),
             pltpu.VMEM((total, width), BF16), pltpu.VMEM((total, 128), jnp.int32),
             pltpu.VMEM((experts - early, width, units), BF16), pltpu.VMEM((experts, units, width), BF16),
             pltpu.VMEM((experts, total, units), BF16),
             pltpu.VMEM((parts, n, rows, width // parts), F32), pltpu.VMEM((n, rows, width), BF16),
             pltpu.VMEM((parts, n, rows, width // parts), F32)]
            + sems * 2 + [dma((parts, n - 1))] * 2 + [dma((experts,)), dma((experts,))]
            + [ln_tile, dma((1,))],
            collective=2, vmem=VM5 << 20,
        )(ctx2, h1, wc_full, ln_ffn, router, chosen, early_w, w_in, w_out)

        def unflat(cache):
            return jnp.swapaxes(cache.reshape(rows, heads, head_dim, length), 2, 3)

        return out, unflat(new_k), unflat(new_v)

    return jax.shard_map(decoder_block, mesh=mesh, in_specs=in_specs, out_specs=out_specs, check_vma=False)
```

```python
import functools
import jax
import jax.numpy as jnp
from jax import lax
from jax.experimental import pallas as pl
from jax.experimental.pallas import tpu as pltpu
from jax.sharding import PartitionSpec as P

EPSILON = 1e-6
NEG_BIG = -1e30
F32 = jnp.float32
BF16 = jnp.bfloat16
MESH = pl.DeviceIdType.MESH
VMEM_SPEC = pl.BlockSpec(memory_space=pltpu.VMEM)
SMEM_SPEC = pl.BlockSpec(memory_space=pltpu.SMEM)
HBM_SPEC = pl.BlockSpec(memory_space=pltpu.HBM)
VMEM_MAX = 67_000_000
HEAD_PAD = 16
NEAR, SLOTS, EARLY = 512, 8, 4
VM3, VM4, VM5 = 8, 14, 39


def rms_norm(hidden, scale):
    hid = hidden.astype(F32)
    inv = lax.rsqrt(jnp.mean(hid * hid, axis=-1, keepdims=True) + EPSILON)
    return (hid * inv * scale).astype(BF16)


def dot_nn(a, b):
    return lax.dot_general(a, b, (((1,), (0,)), ((), ())), preferred_element_type=F32)


def dot_nt(a, b):
    return lax.dot_general(a, b, (((1,), (1,)), ((), ())), preferred_element_type=F32)


def entry_barrier(me, n, across=None):
    sem = pltpu.get_barrier_semaphore()
    for k in range(1, n):
        pl.semaphore_signal(sem, inc=1, device_id={"ws": lax.rem(me + k, n)}, device_id_type=MESH)
    if across is not None:
        pl.semaphore_signal(sem, inc=1, device_id=across, device_id_type=MESH)
    pl.semaphore_wait(sem, n - 1 if across is None else n)


def send(src, dst, send_sem, recv_sem, device):
    copy = pltpu.make_async_remote_copy(src_ref=src, dst_ref=dst, send_sem=send_sem, recv_sem=recv_sem,
                                        device_id=device, device_id_type=MESH)
    copy.start()
    return copy


def start_exchange(me, n, src_of, dst, send_sem, recv_sem):
    copies = []
    for k in range(1, n):
        peer = lax.rem(me + k, n)
        copy = pltpu.make_async_remote_copy(
            src_ref=src_of(peer), dst_ref=dst, send_sem=send_sem.at[k - 1], recv_sem=recv_sem.at[k - 1],
            device_id={"ws": peer}, device_id_type=MESH)
        copy.start()
        copies.append(copy)
    return copies


def wait_all(copies):
    for copy in copies:
        copy.wait()


def my_columns(full, me, n, width):
    picked = full[:, 0:width]
    for j in range(1, n):
        picked = jnp.where(me == j, full[:, j * width:(j + 1) * width], picked)
    return picked


def fetch(pairs, sem):
    copies = [pltpu.make_async_copy(src, dst, sem.at[i]) for i, (src, dst) in enumerate(pairs)]
    for copy in copies:
        copy.start()
    return copies


def read_rows(pairs, sem):
    def copy(i, r):
        return pltpu.make_async_copy(pairs[i][0].at[r], pairs[i][1].at[r], sem.at[i, r])
    rows = pairs[0][1].shape[0]

    def start():
        @pl.loop(0, rows)
        def _(r):
            for i in range(len(pairs)):
                copy(i, r).start()

    def wait():
        @pl.loop(0, rows)
        def _(r):
            for i in range(len(pairs)):
                copy(i, r).wait()
    return start, wait


def qkv_kernel(n, h_hbm, ln_hbm, wq_hbm, wk_hbm, wv_hbm, bias_hbm, mask_hbm, wc_hbm, sk_hbm, sv_hbm,
               q_ref, k_ref, v_ref, hall_ref, brev_ref, lens_ref, wc_half, sk_ref, sv_ref,
               h_ref, ln_ref, w_ref, bias_ref, mask_ref, hbuf, sendbuf, recvbuf, s1, r1, s2, r2, in_sem, row_sem,
               wc_own, swc, rwc):
    me = lax.axis_index("ws")
    rows, width = h_ref.shape
    cols = w_ref.shape[1]
    half = cols // 2
    start = pl.multiple_of(lax.axis_index("dp") * half, 16)
    loads = fetch([(h_hbm, h_ref), (wc_hbm.at[pl.ds(start, half)], wc_own), (ln_hbm, ln_ref), (bias_hbm, bias_ref), (mask_hbm, mask_ref)]
                  + [(w, w_ref.at[i]) for i, w in enumerate((wq_hbm, wk_hbm, wv_hbm))], in_sem)
    start_rows, wait_rows = read_rows([(sk_hbm, sk_ref), (sv_hbm, sv_ref)], row_sem)
    start_rows()
    entry_barrier(me, n)
    loads[0].wait()
    copies = start_exchange(me, n, lambda p: h_ref, hbuf.at[me], s1, r1)
    hbuf[me] = h_ref[...]
    other = {"ws": lax.rem(me + n // 2, n)}
    loads[1].wait()
    bulk = [send(wc_own, wc_half, swc, rwc, other)]
    for load in loads[2:]:
        load.wait()
    lens_ref[...] = jnp.broadcast_to(jnp.sum(mask_ref[...], axis=1, keepdims=True), lens_ref.shape)
    heads, length = bias_ref.shape
    flip = (lax.broadcasted_iota(jnp.int32, (length, length), 0)
            + lax.broadcasted_iota(jnp.int32, (length, length), 1) == length - 1).astype(F32)
    brev_ref[...] = jnp.zeros_like(brev_ref)
    brev_ref[0:heads, :] = lax.dot_general(bias_ref[...], flip, (((1,), (0,)), ((), ())),
                                           precision=lax.Precision.HIGHEST, preferred_element_type=F32)
    wait_all(copies)
    hidden = hbuf[...].reshape(n * rows, width)
    hall_ref[...] = hidden
    x = rms_norm(hidden, ln_ref[...].reshape(1, width))
    for i in range(3):
        sendbuf[:, i] = dot_nt(x, w_ref[i]).astype(BF16).reshape(n, rows, cols)
    copies = start_exchange(me, n, lambda p: sendbuf.at[p], recvbuf.at[me], s2, r2)
    recvbuf[me] = sendbuf[me]
    wait_all(copies)
    for i, o in enumerate((q_ref, k_ref, v_ref)):
        o[...] = jnp.concatenate([recvbuf[j, i] for j in range(n)], axis=1)
    wait_rows()
    wait_all(bulk)


def head_mask(shape, head_dim):
    head = lax.broadcasted_iota(jnp.int32, shape, 0)
    return lax.broadcasted_iota(jnp.int32, shape, 1) // head_dim == head


def spread_heads(q_ref, qblk, head_dim):
    rows, width = q_ref.shape
    q = q_ref[...].astype(F32)
    keep = head_mask((HEAD_PAD, width), head_dim)
    for r in range(rows):
        qblk[r] = jnp.where(keep, jnp.broadcast_to(q[r:r + 1], (HEAD_PAD, width)), 0.0).astype(BF16)


def softmax_rows(scores):
    top = jnp.max(scores, axis=-1, keepdims=True)
    e = jnp.exp(scores - top)
    return (e / jnp.sum(e, axis=-1, keepdims=True)).astype(BF16).astype(F32)


def weighted_values(prob, value, heads, head_dim, length):
    parts = []
    for h in range(heads):
        total = None
        for t in range(length // 128):
            lanes = slice(t * 128, (t + 1) * 128)
            term = value(slice(h * head_dim, (h + 1) * head_dim), t).astype(F32) * prob[h:h + 1, lanes]
            total = term if total is None else total + term
        parts.append(total)
    return jnp.sum(jnp.transpose(jnp.concatenate(parts, axis=0)), axis=0, keepdims=True)


def self_kernel(heads, pos_hbm, q_ref, k_ref, v_ref, brev_ref, sk_ref, sv_ref,
                ctx_ref, nk_ref, nv_ref,
                ktile, vtile, kt, vt, s0, s1, p0, p1, qblk, cf, xf, snew, out_sem, pos_ref, pos_sem):
    rows, width, length = sk_ref.shape
    head_dim = width // heads
    tiles = length // 128
    scalars = pltpu.make_async_copy(pos_hbm, pos_ref, pos_sem)
    scalars.start()

    pad = jnp.zeros((128 - rows, width), F32)
    kt[...] = jnp.transpose(jnp.concatenate([k_ref[...].astype(F32), pad], axis=0))
    vt[...] = jnp.transpose(jnp.concatenate([v_ref[...].astype(F32), pad], axis=0))
    spread_heads(q_ref, qblk, head_dim)
    snew[...] = dot_nn(qblk[...].reshape(rows * HEAD_PAD, width), kt[...].astype(BF16)).reshape(snew.shape)
    sbufs, pbufs = (s0, s1), (p0, p1)
    scalars.wait()

    def insert(r, cache, tile_buf, cols):
        pos = pos_ref[r]
        tile = pos // 128
        at = pos - tile * 128
        new = jnp.broadcast_to(cols[:, r:r + 1], (width, 128))
        old = cache[r, :, pl.ds(pl.multiple_of(tile * 128, 128), 128)]
        hit = lax.broadcasted_iota(jnp.int32, (width, 128), 1) == at
        tile_buf[r] = jnp.where(hit, new, old.astype(F32)).astype(BF16)

    def save(r):
        tile = pos_ref[r] // 128
        for i, (cache, tile_buf, dst) in enumerate(((sk_ref, ktile, nk_ref), (sv_ref, vtile, nv_ref))):
            for t in range(tiles):
                lanes = slice(t * 128, (t + 1) * 128)

                @pl.when(tile == t)
                def _():
                    pltpu.make_async_copy(tile_buf.at[r], dst.at[r, :, lanes], out_sem.at[i, r]).start()

                @pl.when(tile != t)
                def _():
                    pltpu.make_async_copy(cache.at[r, :, lanes], dst.at[r, :, lanes], out_sem.at[i, r]).start()

    def softmax(r):
        pos = pos_ref[r]
        bias = pltpu.roll(brev_ref[...], lax.rem(pos + 1, length), 1)
        lane = lax.broadcasted_iota(jnp.int32, (HEAD_PAD, length), 1)
        pick = lax.broadcasted_iota(jnp.int32, (HEAD_PAD, 128), 1) == r
        fresh = jnp.sum(jnp.where(pick, snew[r], 0.0), axis=-1, keepdims=True)
        scores = jnp.where(lane == pos, fresh, sbufs[r % 2][...]) + bias
        prob = softmax_rows(jnp.where(lane <= pos, scores, NEG_BIG))
        pbufs[r % 2][...] = jnp.where(lane == pos, 0.0, prob)
        at_pos = jnp.sum(jnp.where(lane == pos, prob, 0.0), axis=-1, keepdims=True)
        spread = jnp.where(head_mask((HEAD_PAD, width), head_dim), jnp.broadcast_to(at_pos, (HEAD_PAD, width)), 0.0)
        xf[r:r + 1, :] = jnp.sum(spread, axis=0, keepdims=True) * v_ref[r:r + 1, :].astype(F32)

    for step in range(rows + 2):
        if step >= 2:
            done = step - 2
            cf[done:done + 1, :] = xf[done:done + 1, :] + weighted_values(
                pbufs[done % 2], lambda d, t: sv_ref[done, d, t * 128:(t + 1) * 128], heads, head_dim, length)
        if 1 <= step < rows + 1:
            softmax(step - 1)
            save(step - 1)
        if step < rows:
            sbufs[step % 2][...] = dot_nn(qblk[step], sk_ref[step])
            insert(step, sk_ref, ktile, kt)
            insert(step, sv_ref, vtile, vt)

    ctx_ref[...] = cf[...].astype(BF16)
    for r in range(rows):
        pltpu.make_async_copy(sk_ref.at[r], nk_ref.at[r], out_sem.at[0, r]).wait()
        pltpu.make_async_copy(sv_ref.at[r], nv_ref.at[r], out_sem.at[1, r]).wait()


def mid_kernel(n, ctx_ref, hall_ref, wo_hbm, ln_hbm, wq_hbm, wr_hbm, idx_hbm, wc_half, wc_hbm, ck_hbm, cv_hbm, win_hbm,
               q_ref, h1_ref, wr_ref, idx_ref, wc_ref, ck_ref, cv_ref, win_ref, wr_own, idx_own, sr, rr, si, ri, wc_own, sw, rw, wo_ref, ln_ref, wq_ref, in_sem, row_sem, win_sem, cbuf, hpart, sendbuf, recvbuf, s1, r1, s2, r2, s3, r3):
    me = lax.axis_index("ws")
    rows, width = ctx_ref.shape
    cols = wo_ref.shape[0]
    loads = fetch([(wo_hbm, wo_ref), (ln_hbm, ln_ref), (wq_hbm, wq_ref), (wr_hbm, wr_own), (idx_hbm, idx_own), (wc_hbm, wc_own)], in_sem)
    near = ck_ref.shape[2]
    start_rows, wait_rows = read_rows([(ck_hbm.at[:, :, 0:near], ck_ref), (cv_hbm.at[:, :, 0:near], cv_ref)], row_sem)
    start_win, wait_win = read_rows([(win_hbm, win_ref)], win_sem)
    start_rows()
    start_win()
    group = lax.axis_index("dp")
    facing, sibling = lax.rem(me + n // 2, n), me + 1 - 2 * lax.rem(me, 2)
    half = cols // 2
    mine_half = pl.ds(pl.multiple_of(group * half, 16), half)
    its_half = pl.ds(pl.multiple_of((1 - group) * half, 16), half)
    across = {"dp": 1 - group, "ws": me}
    entry_barrier(me, n, across)
    copies = start_exchange(me, n, lambda p: ctx_ref, cbuf.at[me], s1, r1)
    swap = send(wc_half, wc_ref.at[facing, mine_half], sw.at[0], rw.at[0], across)
    bulk = [send(wc_half, wc_ref.at[facing, mine_half], sw.at[1], rw.at[1], {"ws": sibling})]
    cbuf[me] = ctx_ref[...]
    mine = my_columns(hall_ref[...].astype(F32), me, n, cols)
    wait_all(loads)
    bulk += start_exchange(me, n, lambda p: wr_own, wr_ref.at[me], sr, rr)
    bulk += start_exchange(me, n, lambda p: idx_own, idx_ref.at[me], si, ri)
    bulk.append(send(wc_own, wc_ref.at[me], sw.at[2], rw.at[2], {"ws": sibling}))
    wc_ref[me] = wc_own[...]
    wc_ref[facing, mine_half] = wc_half[...]
    wait_all(copies)
    attn = dot_nt(cbuf[...].reshape(n * rows, width), wo_ref[...])
    hpart[me] = (mine + attn).astype(BF16)
    copies = start_exchange(me, n, lambda p: hpart.at[me], hpart.at[me], s2, r2)
    wait_all(copies)
    h1 = jnp.concatenate([hpart[j] for j in range(n)], axis=1)
    h1_ref[...] = h1
    x = rms_norm(h1, ln_ref[...].reshape(1, width))
    sendbuf[...] = dot_nt(x, wq_ref[...]).astype(BF16).reshape(n, rows, cols)
    copies = start_exchange(me, n, lambda p: sendbuf.at[p], recvbuf.at[me], s3, r3)
    recvbuf[me] = sendbuf[me]
    wr_ref[me] = wr_own[...]
    idx_ref[me] = idx_own[...]
    swap.wait()
    bulk.append(send(wc_ref.at[facing, its_half], wc_ref.at[facing, its_half], sw.at[3], rw.at[3], {"ws": sibling}))
    wait_all(copies)
    q_ref[...] = jnp.concatenate([recvbuf[j] for j in range(n)], axis=1)
    wait_rows()
    wait_all(bulk)
    wait_win()


def cross_kernel(heads, lens_ref, q_ref, mask_ref, kn_ref, vn_ref, ck_ref, cv_ref,
                 ctx_ref, kbuf, vbuf, s0, s1, p0, p1, qblk, cf, in_sem):
    rows, width, near = kn_ref.shape
    slots = kbuf.shape[0]
    length = near + kbuf.shape[2]
    head_dim = width // heads
    block = 256
    tiles, near_tiles = length // 128, near // 128

    def slot(r):
        return lax.rem(r, slots)

    def tile_count(r):
        return (lens_ref[r, 0] + 127) // 128

    def far_copies(r, body):
        count = tile_count(r)
        for t in range(near_tiles + 1, tiles + 1):
            @pl.when(count == t)
            def _(size=(t - near_tiles) * 128):
                body(lambda i: pltpu.make_async_copy(
                    (ck_ref, cv_ref)[i].at[r, :, near:near + size], (kbuf, vbuf)[i].at[slot(r), :, 0:size],
                    in_sem.at[i, slot(r)]))

    def far_start(r):
        far_copies(r, lambda copy: (copy(0).start(), copy(1).start()))
        for t in [t for t in range(1, tiles, 2) if t >= near_tiles]:
            @pl.when(tile_count(r) == t)
            def _(at=(t - near_tiles) * 128):
                vbuf[slot(r), :, at:at + 128] = jnp.zeros((width, 128), BF16)

    def per_block(r, body):
        blocks = (lens_ref[r, 0] + block - 1) // block
        for t in range(1, length // block + 1):
            @pl.when(blocks == t)
            def _(size=t * block):
                body(size)

    @pl.loop(0, slots)
    def _(r):
        far_start(r)

    spread_heads(q_ref, qblk, head_dim)

    def scores(r, size, out):
        first = min(size, near)
        out[:, 0:first] = dot_nn(qblk[r], kn_ref[r, :, 0:first])
        if size > near:
            out[:, near:size] = dot_nn(qblk[r], kbuf[slot(r), :, 0:size - near])

    def softmax(r, src, out):
        keep = jnp.broadcast_to(mask_ref[pl.ds(r, 1), :], (HEAD_PAD, length)) == 1
        out[...] = softmax_rows(jnp.where(keep, src[...], NEG_BIG))

    def values(r, size, prob):
        def tile(d, t):
            if t < near_tiles:
                return vn_ref[r, d, t * 128:(t + 1) * 128]
            return vbuf[slot(r), d, (t - near_tiles) * 128:(t - near_tiles + 1) * 128]
        cf[pl.ds(r, 1), :] = weighted_values(prob, tile, heads, head_dim, size)

    def arrived(r, i):
        far_copies(r, lambda copy: copy(i).wait())

    arrived(0, 0)
    per_block(0, lambda size: scores(0, size, s0))
    arrived(1, 0)

    def second(size):
        softmax(0, s0, p0)
        scores(1, size, s1)
    per_block(1, second)

    def step(r, sa, sb, pa, pb):
        arrived(r, 1)
        arrived(r + 2, 0)

        def outer(size_v):
            def inner(size_s):
                values(r, size_v, pa)
                softmax(r + 1, sb, pb)
                scores(r + 2, size_s, sa)
            per_block(r + 2, inner)
        per_block(r, outer)

        @pl.when(r + slots < rows)
        def _():
            far_start(r + slots)

    @pl.loop(0, (rows - 2) // 2)
    def _(i):
        step(2 * i, s0, s1, p0, p1)
        step(2 * i + 1, s1, s0, p1, p0)

    def last_but_one(size):
        values(rows - 2, size, p0)
        softmax(rows - 1, s1, p1)
    arrived(rows - 2, 1)
    per_block(rows - 2, last_but_one)
    arrived(rows - 1, 1)
    per_block(rows - 1, lambda size: values(rows - 1, size, p1))
    ctx_ref[...] = cf[...].astype(BF16)


def ffn_kernel(n, ctx_ref, h1_ref, wo_ref, ln_hbm, rbuf, ibuf, early_ref, win_ref, wout_ref,
               out_ref, cbuf, xbuf, mbuf, wi, wo, ubuf, part, own, ybuf,
               s1, r1, s5, r5, wi_sem, wo_sem, ln_ref, in_sem):
    me = lax.axis_index("ws")
    rows, width = ctx_ref.shape
    experts = win_ref.shape[0]
    total = n * rows
    capacity = (2 * total + experts - 1) // experts

    early = early_ref.shape[0]

    def load(e, i):
        if i == 0:
            return pltpu.make_async_copy(win_ref.at[e + early], wi.at[e], wi_sem.at[e])
        return pltpu.make_async_copy(wout_ref.at[e], wo.at[e], wo_sem.at[e])

    loads = fetch([(ln_hbm, ln_ref)], in_sem)

    for i in range(2):
        @pl.loop(0, experts - early if i == 0 else experts)
        def _(e, i=i):
            load(e, i).start()

    entry_barrier(me, n)
    copies = start_exchange(me, n, lambda p: ctx_ref, cbuf.at[me], s1, r1)
    cbuf[me] = ctx_ref[...]

    idx_row = jnp.concatenate([ibuf[j] for j in range(n)], axis=1)
    grid_i = lax.broadcasted_iota(jnp.int32, (total, total), 0)
    grid_j = lax.broadcasted_iota(jnp.int32, (total, total), 1)
    row_b = jnp.broadcast_to(idx_row, (total, total))
    idx_col = jnp.sum(jnp.where(grid_i == grid_j, row_b, 0), axis=1, keepdims=True)
    earlier = (row_b == idx_col) & (grid_j < grid_i)
    slot = jnp.sum(earlier.astype(jnp.int32), axis=1, keepdims=True)
    target = jnp.where(slot < capacity, idx_col, -1)
    mbuf[...] = jnp.broadcast_to(target, mbuf.shape)

    wait_all(loads)
    wait_all(copies)
    attn = dot_nt(cbuf[...].reshape(total, width), wo_ref[...].reshape(width, width))
    h2 = (h1_ref[...].astype(F32) + attn).astype(BF16)
    x = rms_norm(h2, ln_ref[...].reshape(1, width))
    xbuf[...] = x
    own[...] = h2.reshape(n, rows, width)
    def hidden_units(e, weight):
        u = jnp.maximum(dot_nn(xbuf[...], weight), 0.0)
        hit = jnp.broadcast_to(mbuf[:, 0:1], u.shape) == e
        ubuf[e] = jnp.where(hit, u, 0.0).astype(BF16)

    @pl.loop(0, early // 2)
    def _(i):
        for k in range(2):
            hidden_units(i * 2 + k, early_ref[i * 2 + k])

    @pl.loop(0, (experts - early) // 2)
    def _(i):
        for k in range(2):
            load(i * 2 + k, 0).wait()
        for k in range(2):
            hidden_units(early + i * 2 + k, wi[i * 2 + k])

    sends = []
    block = part.shape[-1]
    for c in range(width // block):
        lanes = slice(c * block, (c + 1) * block)

        def add_output(i, total, c=c, lanes=lanes):
            if c == 0:
                for k in range(4):
                    load(i * 4 + k, 1).wait()
            for k in range(4):
                total = total + dot_nn(ubuf[i * 4 + k], wo[i * 4 + k, :, lanes])
            return total
        sums = lax.fori_loop(0, experts // 4, add_output, jnp.zeros((total, block), F32))
        part[c] = sums.reshape(n, rows, block)
        sends += start_exchange(me, n, lambda p: part.at[c, p], ybuf.at[c, me], s5.at[c], r5.at[c])
        ybuf[c, me] = part[c, me]
    copies = sends

    my_rows = pl.ds(pl.multiple_of(me * rows, rows), rows)
    router = jnp.concatenate([rbuf[j] for j in range(n)], axis=0)
    logits = lax.dot_general(xbuf[my_rows, :].astype(F32), router, (((1,), (1,)), ((), ())),
                             precision=lax.Precision.HIGHEST, preferred_element_type=F32)
    probs = jnp.exp(logits - jnp.max(logits, axis=-1, keepdims=True))
    probs = probs / jnp.sum(probs, axis=-1, keepdims=True)
    chosen = lax.broadcasted_iota(jnp.int32, (rows, experts), 1) == mbuf[my_rows, :][:, 0:experts]
    gate = jnp.sum(jnp.where(chosen, probs, 0.0), axis=-1, keepdims=True)
    wait_all(copies)
    y = jnp.concatenate([sum(ybuf[c, j] for j in range(1, n)) + ybuf[c, 0] for c in range(width // block)], axis=1)
    out_ref[...] = (own[me].astype(F32) + y.astype(BF16).astype(F32) * gate).astype(BF16)


def call(body, out_shape, in_specs, out_specs, scratch, collective=None, flops=1_000_000, moved=1_000_000, vmem=VMEM_MAX):
    params = dict(vmem_limit_bytes=vmem)
    if collective is not None:
        params.update(collective_id=collective, has_side_effects=True)
    kernel = pl.pallas_call(
        body, out_shape=out_shape, in_specs=in_specs, out_specs=out_specs, scratch_shapes=scratch,
        compiler_params=pltpu.CompilerParams(**params),
        cost_estimate=pl.CostEstimate(flops=flops, bytes_accessed=moved, transcendentals=0))

    def run(*operands):
        return kernel(*[pltpu.with_memory_space_constraint(x, pltpu.HBM) if spec is HBM_SPEC else x
                        for x, spec in zip(operands, in_specs)])
    return run


def solution(mesh):
    n = mesh.shape['ws']
    row_axes = ('dp', 'ws')
    row_vec = P(row_axes)
    row_mat = P(row_axes, None)
    cache_spec = P(row_axes, None, None, None)
    col_split = P(None, 'ws')
    in_specs = (row_mat, cache_spec, cache_spec, cache_spec, cache_spec, row_vec, row_mat, P(None, None), row_vec,
                P(None), P(None), P(None), col_split, col_split, col_split, col_split, col_split, col_split,
                col_split, P(None, None, 'ws'), P(None, 'ws', None))
    out_specs = (row_mat, cache_spec, cache_spec)
    dma = pltpu.SemaphoreType.DMA

    def decoder_block(hidden, self_k, self_v, cross_k, cross_v, positions, enc_mask, rel_bias, expert_idx,
                      ln_self, ln_cross, ln_ffn, wq_self, wk_self, wv_self, wo_self, wq_cross, wo_cross,
                      w_router, w_in, w_out):
        rows, width = hidden.shape
        heads, length = rel_bias.shape
        head_dim = width // heads
        source = enc_mask.shape[1]
        cols = wq_self.shape[1]
        experts, _, units = w_in.shape
        total = n * rows
        sds = jax.ShapeDtypeStruct

        def flat(cache):
            return jnp.swapaxes(cache, 2, 3).reshape(rows, width, cache.shape[2])

        sems = [dma((n - 1,))]
        w_tile = pltpu.VMEM((cols, width), BF16)
        ln_tile = pltpu.VMEM((width,), F32)
        near, slots, early = NEAR, SLOTS, EARLY
        q, k, v, hall, brev, lens, wc_half, near_sk, near_sv = call(
            functools.partial(qkv_kernel, n),
            [sds((rows, width), BF16)] * 3 + [sds((total, width), BF16), sds((HEAD_PAD, length), F32), sds((rows, 128), jnp.int32),
               sds((cols // 2, width), BF16)]
            + [sds((rows, width, length), BF16)] * 2,
            [HBM_SPEC] * 10, [VMEM_SPEC] * 9,
            [pltpu.VMEM((rows, width), BF16), ln_tile, pltpu.VMEM((3, cols, width), BF16), pltpu.VMEM((heads, length), F32),
             pltpu.VMEM((rows, source), jnp.int32),
             pltpu.VMEM((n, rows, width), BF16), pltpu.VMEM((n, 3, rows, cols), BF16), pltpu.VMEM((n, 3, rows, cols), BF16)]
            + sems * 4 + [dma((8,)), dma((2, rows)), pltpu.VMEM((cols // 2, width), BF16), dma, dma],
            collective=0, vmem=8 << 20,
        )(hidden, ln_self, wq_self.T, wk_self.T, wv_self.T, rel_bias, enc_mask, wo_cross.T, flat(self_k), flat(self_v))

        def attention_scratch(size):
            return ([pltpu.VMEM((HEAD_PAD, size), F32)] * 4
                    + [pltpu.VMEM((rows, HEAD_PAD, width), BF16), pltpu.VMEM((rows, width), F32)])

        ctx, new_k, new_v = call(
            functools.partial(self_kernel, heads),
            [sds((rows, width), BF16)] + [sds((rows, width, length), BF16)] * 2,
            [HBM_SPEC] + [VMEM_SPEC] * 6, [VMEM_SPEC] + [HBM_SPEC] * 2,
            [pltpu.VMEM((rows, width, 128), BF16)] * 2 + [pltpu.VMEM((width, 128), F32)] * 2 + attention_scratch(length)
            + [pltpu.VMEM((rows, width), F32), pltpu.VMEM((rows, HEAD_PAD, 128), F32),
               dma((2, rows)), pltpu.SMEM((rows,), jnp.int32), dma],
            vmem=12 << 20,
        )(positions, q, k, v, brev, near_sk, near_sv)

        qc, h1, router, chosen, wc_full, near_ck, near_cv, early_w = call(
            functools.partial(mid_kernel, n),
            [sds((rows, width), BF16), sds((total, width), BF16), sds((n, experts // n, width), F32), sds((n, 1, rows), jnp.int32),
               sds((n, cols, width), BF16)]
            + [sds((rows, width, near), BF16)] * 2
            + [sds((early, width, units), BF16)],
            [VMEM_SPEC] * 2 + [HBM_SPEC] * 5 + [VMEM_SPEC] + [HBM_SPEC] * 4, [VMEM_SPEC] * 8,
            [pltpu.VMEM((experts // n, width), F32), pltpu.VMEM((1, rows), jnp.int32)] + sems * 4
            + [w_tile, dma((4,)), dma((4,)), w_tile, ln_tile, w_tile, dma((6,)), dma((2, rows)), dma((1, early)), pltpu.VMEM((n, rows, width), BF16), pltpu.VMEM((n, total, cols), BF16),
             pltpu.VMEM((n, rows, cols), BF16), pltpu.VMEM((n, rows, cols), BF16)] + sems * 6,
            collective=1, vmem=VM3 << 20,
        )(ctx, hall, wo_self.T, ln_cross, wq_cross.T, w_router.T, expert_idx[None, :], wc_half, wo_cross.T, flat(cross_k), flat(cross_v), w_in)

        ctx2 = call(
            functools.partial(cross_kernel, heads),
            sds((rows, width), BF16),
            [SMEM_SPEC] + [VMEM_SPEC] * 4 + [HBM_SPEC] * 2, VMEM_SPEC,
            [pltpu.VMEM((slots, width, source - near), BF16)] * 2 + attention_scratch(source) + [dma((2, slots))],
            vmem=VM4 << 20,
        )(lens, qc, enc_mask, near_ck, near_cv, flat(cross_k), flat(cross_v))

        parts = 3
        out = call(
            functools.partial(ffn_kernel, n),
            sds((rows, width), BF16),
            [VMEM_SPEC] * 3 + [HBM_SPEC] + [VMEM_SPEC] * 3 + [HBM_SPEC] * 2, VMEM_SPEC,
            [pltpu.VMEM((n, rows, width), BF16),
             pltpu.VMEM((total, width), BF16), pltpu.VMEM((total, 128), jnp.int32),
             pltpu.VMEM((experts - early, width, units), BF16), pltpu.VMEM((experts, units, width), BF16),
             pltpu.VMEM((experts, total, units), BF16),
             pltpu.VMEM((parts, n, rows, width // parts), F32), pltpu.VMEM((n, rows, width), BF16),
             pltpu.VMEM((parts, n, rows, width // parts), F32)]
            + sems * 2 + [dma((parts, n - 1))] * 2 + [dma((experts,)), dma((experts,))]
            + [ln_tile, dma((1,))],
            collective=2, vmem=VM5 << 20,
        )(ctx2, h1, wc_full, ln_ffn, router, chosen, early_w, w_in, w_out)

        def unflat(cache):
            return jnp.swapaxes(cache.reshape(rows, heads, head_dim, length), 2, 3)

        return out, unflat(new_k), unflat(new_v)

    return jax.shard_map(decoder_block, mesh=mesh, in_specs=in_specs, out_specs=out_specs, check_vma=False)
```

```python
import functools
import jax
import jax.numpy as jnp
from jax import lax
from jax.experimental import pallas as pl
from jax.experimental.pallas import tpu as pltpu
from jax.sharding import PartitionSpec as P

EPSILON = 1e-6
NEG_BIG = -1e30
F32 = jnp.float32
BF16 = jnp.bfloat16
MESH = pl.DeviceIdType.MESH
VMEM_SPEC = pl.BlockSpec(memory_space=pltpu.VMEM)
SMEM_SPEC = pl.BlockSpec(memory_space=pltpu.SMEM)
HBM_SPEC = pl.BlockSpec(memory_space=pltpu.HBM)
VMEM_MAX = 67_000_000
HEAD_PAD = 16
NEAR, SLOTS, EARLY = 512, 8, 4
VM3, VM4, VM5 = 8, 14, 39


def rms_norm(hidden, scale):
    hid = hidden.astype(F32)
    inv = lax.rsqrt(jnp.mean(hid * hid, axis=-1, keepdims=True) + EPSILON)
    return (hid * inv * scale).astype(BF16)


def dot_nn(a, b):
    return lax.dot_general(a, b, (((1,), (0,)), ((), ())), preferred_element_type=F32)


def dot_nt(a, b):
    return lax.dot_general(a, b, (((1,), (1,)), ((), ())), preferred_element_type=F32)


def greet(me, n, across=None):
    sem = pltpu.get_barrier_semaphore()
    for k in range(1, n):
        pl.semaphore_signal(sem, inc=1, device_id={"ws": lax.rem(me + k, n)}, device_id_type=MESH)
    if across is not None:
        pl.semaphore_signal(sem, inc=1, device_id=across, device_id_type=MESH)


def all_here(count):
    pl.semaphore_wait(pltpu.get_barrier_semaphore(), count)


def send(src, dst, send_sem, recv_sem, device):
    copy = pltpu.make_async_remote_copy(src_ref=src, dst_ref=dst, send_sem=send_sem, recv_sem=recv_sem,
                                        device_id=device, device_id_type=MESH)
    copy.start()
    return copy


def start_exchange(me, n, src_of, dst, send_sem, recv_sem):
    copies = []
    for k in range(1, n):
        peer = lax.rem(me + k, n)
        copy = pltpu.make_async_remote_copy(
            src_ref=src_of(peer), dst_ref=dst, send_sem=send_sem.at[k - 1], recv_sem=recv_sem.at[k - 1],
            device_id={"ws": peer}, device_id_type=MESH)
        copy.start()
        copies.append(copy)
    return copies


def wait_all(copies):
    for copy in copies:
        copy.wait()


def my_columns(full, me, n, width):
    picked = full[:, 0:width]
    for j in range(1, n):
        picked = jnp.where(me == j, full[:, j * width:(j + 1) * width], picked)
    return picked


def fetch(pairs, sem):
    copies = [pltpu.make_async_copy(src, dst, sem.at[i]) for i, (src, dst) in enumerate(pairs)]
    for copy in copies:
        copy.start()
    return copies


def read_rows(pairs, sem):
    def copy(i, r):
        return pltpu.make_async_copy(pairs[i][0].at[r], pairs[i][1].at[r], sem.at[i, r])
    rows = pairs[0][1].shape[0]

    def start():
        @pl.loop(0, rows)
        def _(r):
            for i in range(len(pairs)):
                copy(i, r).start()

    def wait():
        @pl.loop(0, rows)
        def _(r):
            for i in range(len(pairs)):
                copy(i, r).wait()
    return start, wait


def qkv_kernel(n, h_hbm, ln_hbm, wq_hbm, wk_hbm, wv_hbm, bias_hbm, mask_hbm, wc_hbm, sk_hbm, sv_hbm,
               q_ref, k_ref, v_ref, hall_ref, brev_ref, lens_ref, wc_half, sk_ref, sv_ref,
               h_ref, ln_ref, w_ref, bias_ref, mask_ref, hbuf, sendbuf, recvbuf, s1, r1, s2, r2, in_sem, row_sem,
               wc_own, swc, rwc):
    me = lax.axis_index("ws")
    rows, width = h_ref.shape
    cols = w_ref.shape[1]
    greet(me, n)
    half = cols // 2
    start = pl.multiple_of(lax.axis_index("dp") * half, 16)
    loads = fetch([(h_hbm, h_ref), (wc_hbm.at[pl.ds(start, half)], wc_own), (ln_hbm, ln_ref), (bias_hbm, bias_ref), (mask_hbm, mask_ref)]
                  + [(w, w_ref.at[i]) for i, w in enumerate((wq_hbm, wk_hbm, wv_hbm))], in_sem)
    start_rows, wait_rows = read_rows([(sk_hbm, sk_ref), (sv_hbm, sv_ref)], row_sem)
    start_rows()
    all_here(n - 1)
    loads[0].wait()
    copies = start_exchange(me, n, lambda p: h_ref, hbuf.at[me], s1, r1)
    hbuf[me] = h_ref[...]
    other = {"ws": lax.rem(me + n // 2, n)}
    loads[1].wait()
    bulk = [send(wc_own, wc_half, swc, rwc, other)]
    for load in loads[2:]:
        load.wait()
    lens_ref[...] = jnp.broadcast_to(jnp.sum(mask_ref[...], axis=1, keepdims=True), lens_ref.shape)
    heads, length = bias_ref.shape
    flip = (lax.broadcasted_iota(jnp.int32, (length, length), 0)
            + lax.broadcasted_iota(jnp.int32, (length, length), 1) == length - 1).astype(F32)
    brev_ref[...] = jnp.zeros_like(brev_ref)
    brev_ref[0:heads, :] = lax.dot_general(bias_ref[...], flip, (((1,), (0,)), ((), ())),
                                           precision=lax.Precision.HIGHEST, preferred_element_type=F32)
    wait_all(copies)
    hidden = hbuf[...].reshape(n * rows, width)
    hall_ref[...] = hidden
    x = rms_norm(hidden, ln_ref[...].reshape(1, width))
    for i in range(3):
        sendbuf[:, i] = dot_nt(x, w_ref[i]).astype(BF16).reshape(n, rows, cols)
    copies = start_exchange(me, n, lambda p: sendbuf.at[p], recvbuf.at[me], s2, r2)
    recvbuf[me] = sendbuf[me]
    wait_all(copies)
    for i, o in enumerate((q_ref, k_ref, v_ref)):
        o[...] = jnp.concatenate([recvbuf[j, i] for j in range(n)], axis=1)
    wait_rows()
    wait_all(bulk)


def head_mask(shape, head_dim):
    head = lax.broadcasted_iota(jnp.int32, shape, 0)
    return lax.broadcasted_iota(jnp.int32, shape, 1) // head_dim == head


def spread_heads(q_ref, qblk, head_dim):
    rows, width = q_ref.shape
    q = q_ref[...].astype(F32)
    keep = head_mask((HEAD_PAD, width), head_dim)
    for r in range(rows):
        qblk[r] = jnp.where(keep, jnp.broadcast_to(q[r:r + 1], (HEAD_PAD, width)), 0.0).astype(BF16)


def softmax_rows(scores):
    top = jnp.max(scores, axis=-1, keepdims=True)
    e = jnp.exp(scores - top)
    return (e / jnp.sum(e, axis=-1, keepdims=True)).astype(BF16).astype(F32)


def weighted_values(prob, value, heads, head_dim, length):
    parts = []
    for h in range(heads):
        total = None
        for t in range(length // 128):
            lanes = slice(t * 128, (t + 1) * 128)
            term = value(slice(h * head_dim, (h + 1) * head_dim), t).astype(F32) * prob[h:h + 1, lanes]
            total = term if total is None else total + term
        parts.append(total)
    return jnp.sum(jnp.transpose(jnp.concatenate(parts, axis=0)), axis=0, keepdims=True)


def self_kernel(heads, pos_hbm, q_ref, k_ref, v_ref, brev_ref, sk_ref, sv_ref,
                ctx_ref, nk_ref, nv_ref,
                ktile, vtile, kt, vt, s0, s1, p0, p1, qblk, cf, xf, snew, out_sem, pos_ref, pos_sem):
    rows, width, length = sk_ref.shape
    head_dim = width // heads
    tiles = length // 128
    scalars = pltpu.make_async_copy(pos_hbm, pos_ref, pos_sem)
    scalars.start()

    pad = jnp.zeros((128 - rows, width), F32)
    kt[...] = jnp.transpose(jnp.concatenate([k_ref[...].astype(F32), pad], axis=0))
    vt[...] = jnp.transpose(jnp.concatenate([v_ref[...].astype(F32), pad], axis=0))
    spread_heads(q_ref, qblk, head_dim)
    snew[...] = dot_nn(qblk[...].reshape(rows * HEAD_PAD, width), kt[...].astype(BF16)).reshape(snew.shape)
    sbufs, pbufs = (s0, s1), (p0, p1)
    scalars.wait()

    def insert(r, cache, tile_buf, cols):
        pos = pos_ref[r]
        tile = pos // 128
        at = pos - tile * 128
        new = jnp.broadcast_to(cols[:, r:r + 1], (width, 128))
        old = cache[r, :, pl.ds(pl.multiple_of(tile * 128, 128), 128)]
        hit = lax.broadcasted_iota(jnp.int32, (width, 128), 1) == at
        tile_buf[r] = jnp.where(hit, new, old.astype(F32)).astype(BF16)

    def save(r):
        tile = pos_ref[r] // 128
        for i, (cache, tile_buf, dst) in enumerate(((sk_ref, ktile, nk_ref), (sv_ref, vtile, nv_ref))):
            for t in range(tiles):
                lanes = slice(t * 128, (t + 1) * 128)

                @pl.when(tile == t)
                def _():
                    pltpu.make_async_copy(tile_buf.at[r], dst.at[r, :, lanes], out_sem.at[i, r]).start()

                @pl.when(tile != t)
                def _():
                    pltpu.make_async_copy(cache.at[r, :, lanes], dst.at[r, :, lanes], out_sem.at[i, r]).start()

    def softmax(r):
        pos = pos_ref[r]
        bias = pltpu.roll(brev_ref[...], lax.rem(pos + 1, length), 1)
        lane = lax.broadcasted_iota(jnp.int32, (HEAD_PAD, length), 1)
        pick = lax.broadcasted_iota(jnp.int32, (HEAD_PAD, 128), 1) == r
        fresh = jnp.sum(jnp.where(pick, snew[r], 0.0), axis=-1, keepdims=True)
        scores = jnp.where(lane == pos, fresh, sbufs[r % 2][...]) + bias
        prob = softmax_rows(jnp.where(lane <= pos, scores, NEG_BIG))
        pbufs[r % 2][...] = jnp.where(lane == pos, 0.0, prob)
        at_pos = jnp.sum(jnp.where(lane == pos, prob, 0.0), axis=-1, keepdims=True)
        spread = jnp.where(head_mask((HEAD_PAD, width), head_dim), jnp.broadcast_to(at_pos, (HEAD_PAD, width)), 0.0)
        xf[r:r + 1, :] = jnp.sum(spread, axis=0, keepdims=True) * v_ref[r:r + 1, :].astype(F32)

    for step in range(rows + 2):
        if step >= 2:
            done = step - 2
            cf[done:done + 1, :] = xf[done:done + 1, :] + weighted_values(
                pbufs[done % 2], lambda d, t: sv_ref[done, d, t * 128:(t + 1) * 128], heads, head_dim, length)
        if 1 <= step < rows + 1:
            softmax(step - 1)
            save(step - 1)
        if step < rows:
            sbufs[step % 2][...] = dot_nn(qblk[step], sk_ref[step])
            insert(step, sk_ref, ktile, kt)
            insert(step, sv_ref, vtile, vt)

    ctx_ref[...] = cf[...].astype(BF16)
    for r in range(rows):
        pltpu.make_async_copy(sk_ref.at[r], nk_ref.at[r], out_sem.at[0, r]).wait()
        pltpu.make_async_copy(sv_ref.at[r], nv_ref.at[r], out_sem.at[1, r]).wait()


def mid_kernel(n, ctx_ref, hall_ref, wo_hbm, ln_hbm, wq_hbm, wr_hbm, idx_hbm, wc_half, wc_hbm, ck_hbm, cv_hbm, win_hbm,
               q_ref, h1_ref, wr_ref, idx_ref, wc_ref, ck_ref, cv_ref, win_ref, wr_own, idx_own, sr, rr, si, ri, wc_own, sw, rw, wo_ref, ln_ref, wq_ref, in_sem, row_sem, win_sem, cbuf, hpart, sendbuf, recvbuf, s1, r1, s2, r2, s3, r3):
    me = lax.axis_index("ws")
    rows, width = ctx_ref.shape
    cols = wo_ref.shape[0]
    group = lax.axis_index("dp")
    across = {"dp": 1 - group, "ws": me}
    greet(me, n, across)
    loads = fetch([(wo_hbm, wo_ref), (ln_hbm, ln_ref), (wq_hbm, wq_ref), (wr_hbm, wr_own), (idx_hbm, idx_own), (wc_hbm, wc_own)], in_sem)
    near = ck_ref.shape[2]
    start_rows, wait_rows = read_rows([(ck_hbm.at[:, :, 0:near], ck_ref), (cv_hbm.at[:, :, 0:near], cv_ref)], row_sem)
    start_win, wait_win = read_rows([(win_hbm, win_ref)], win_sem)
    start_rows()
    start_win()
    facing, sibling = lax.rem(me + n // 2, n), me + 1 - 2 * lax.rem(me, 2)
    half = cols // 2
    mine_half = pl.ds(pl.multiple_of(group * half, 16), half)
    its_half = pl.ds(pl.multiple_of((1 - group) * half, 16), half)
    all_here(n)
    copies = start_exchange(me, n, lambda p: ctx_ref, cbuf.at[me], s1, r1)
    swap = send(wc_half, wc_ref.at[facing, mine_half], sw.at[0], rw.at[0], across)
    bulk = [send(wc_half, wc_ref.at[facing, mine_half], sw.at[1], rw.at[1], {"ws": sibling})]
    cbuf[me] = ctx_ref[...]
    mine = my_columns(hall_ref[...].astype(F32), me, n, cols)
    wait_all(loads)
    bulk += start_exchange(me, n, lambda p: wr_own, wr_ref.at[me], sr, rr)
    bulk += start_exchange(me, n, lambda p: idx_own, idx_ref.at[me], si, ri)
    bulk.append(send(wc_own, wc_ref.at[me], sw.at[2], rw.at[2], {"ws": sibling}))
    wc_ref[me] = wc_own[...]
    wc_ref[facing, mine_half] = wc_half[...]
    wait_all(copies)
    attn = dot_nt(cbuf[...].reshape(n * rows, width), wo_ref[...])
    hpart[me] = (mine + attn).astype(BF16)
    copies = start_exchange(me, n, lambda p: hpart.at[me], hpart.at[me], s2, r2)
    wait_all(copies)
    h1 = jnp.concatenate([hpart[j] for j in range(n)], axis=1)
    h1_ref[...] = h1
    x = rms_norm(h1, ln_ref[...].reshape(1, width))
    sendbuf[...] = dot_nt(x, wq_ref[...]).astype(BF16).reshape(n, rows, cols)
    copies = start_exchange(me, n, lambda p: sendbuf.at[p], recvbuf.at[me], s3, r3)
    recvbuf[me] = sendbuf[me]
    wr_ref[me] = wr_own[...]
    idx_ref[me] = idx_own[...]
    swap.wait()
    bulk.append(send(wc_ref.at[facing, its_half], wc_ref.at[facing, its_half], sw.at[3], rw.at[3], {"ws": sibling}))
    wait_all(copies)
    q_ref[...] = jnp.concatenate([recvbuf[j] for j in range(n)], axis=1)
    wait_rows()
    wait_all(bulk)
    wait_win()


def cross_kernel(heads, lens_ref, q_ref, mask_ref, kn_ref, vn_ref, ck_ref, cv_ref,
                 ctx_ref, kbuf, vbuf, s0, s1, p0, p1, qblk, cf, in_sem):
    rows, width, near = kn_ref.shape
    slots = kbuf.shape[0]
    length = near + kbuf.shape[2]
    head_dim = width // heads
    block = 256
    tiles, near_tiles = length // 128, near // 128

    def slot(r):
        return lax.rem(r, slots)

    def tile_count(r):
        return (lens_ref[r, 0] + 127) // 128

    def far_copies(r, body):
        count = tile_count(r)
        for t in range(near_tiles + 1, tiles + 1):
            @pl.when(count == t)
            def _(size=(t - near_tiles) * 128):
                body(lambda i: pltpu.make_async_copy(
                    (ck_ref, cv_ref)[i].at[r, :, near:near + size], (kbuf, vbuf)[i].at[slot(r), :, 0:size],
                    in_sem.at[i, slot(r)]))

    def far_start(r):
        far_copies(r, lambda copy: (copy(0).start(), copy(1).start()))
        for t in [t for t in range(1, tiles, 2) if t >= near_tiles]:
            @pl.when(tile_count(r) == t)
            def _(at=(t - near_tiles) * 128):
                vbuf[slot(r), :, at:at + 128] = jnp.zeros((width, 128), BF16)

    def per_block(r, body):
        blocks = (lens_ref[r, 0] + block - 1) // block
        for t in range(1, length // block + 1):
            @pl.when(blocks == t)
            def _(size=t * block):
                body(size)

    @pl.loop(0, slots)
    def _(r):
        far_start(r)

    spread_heads(q_ref, qblk, head_dim)

    def scores(r, size, out):
        first = min(size, near)
        out[:, 0:first] = dot_nn(qblk[r], kn_ref[r, :, 0:first])
        if size > near:
            out[:, near:size] = dot_nn(qblk[r], kbuf[slot(r), :, 0:size - near])

    def softmax(r, src, out):
        keep = jnp.broadcast_to(mask_ref[pl.ds(r, 1), :], (HEAD_PAD, length)) == 1
        out[...] = softmax_rows(jnp.where(keep, src[...], NEG_BIG))

    def values(r, size, prob):
        def tile(d, t):
            if t < near_tiles:
                return vn_ref[r, d, t * 128:(t + 1) * 128]
            return vbuf[slot(r), d, (t - near_tiles) * 128:(t - near_tiles + 1) * 128]
        cf[pl.ds(r, 1), :] = weighted_values(prob, tile, heads, head_dim, size)

    def arrived(r, i):
        far_copies(r, lambda copy: copy(i).wait())

    arrived(0, 0)
    per_block(0, lambda size: scores(0, size, s0))
    arrived(1, 0)

    def second(size):
        softmax(0, s0, p0)
        scores(1, size, s1)
    per_block(1, second)

    def step(r, sa, sb, pa, pb):
        arrived(r, 1)
        arrived(r + 2, 0)

        def outer(size_v):
            def inner(size_s):
                values(r, size_v, pa)
                softmax(r + 1, sb, pb)
                scores(r + 2, size_s, sa)
            per_block(r + 2, inner)
        per_block(r, outer)

        @pl.when(r + slots < rows)
        def _():
            far_start(r + slots)

    @pl.loop(0, (rows - 2) // 2)
    def _(i):
        step(2 * i, s0, s1, p0, p1)
        step(2 * i + 1, s1, s0, p1, p0)

    def last_but_one(size):
        values(rows - 2, size, p0)
        softmax(rows - 1, s1, p1)
    arrived(rows - 2, 1)
    per_block(rows - 2, last_but_one)
    arrived(rows - 1, 1)
    per_block(rows - 1, lambda size: values(rows - 1, size, p1))
    ctx_ref[...] = cf[...].astype(BF16)


def ffn_kernel(n, ctx_ref, h1_ref, wo_ref, ln_hbm, rbuf, ibuf, early_ref, win_ref, wout_ref,
               out_ref, cbuf, xbuf, mbuf, wi, wo, ubuf, part, own, ybuf,
               s1, r1, s5, r5, wi_sem, wo_sem, ln_ref, in_sem):
    me = lax.axis_index("ws")
    rows, width = ctx_ref.shape
    experts = win_ref.shape[0]
    total = n * rows
    capacity = (2 * total + experts - 1) // experts

    early = early_ref.shape[0]

    def load(e, i):
        if i == 0:
            return pltpu.make_async_copy(win_ref.at[e + early], wi.at[e], wi_sem.at[e])
        return pltpu.make_async_copy(wout_ref.at[e], wo.at[e], wo_sem.at[e])

    greet(me, n)
    loads = fetch([(ln_hbm, ln_ref)], in_sem)

    for i in range(2):
        @pl.loop(0, experts - early if i == 0 else experts)
        def _(e, i=i):
            load(e, i).start()

    all_here(n - 1)
    copies = start_exchange(me, n, lambda p: ctx_ref, cbuf.at[me], s1, r1)
    cbuf[me] = ctx_ref[...]

    idx_row = jnp.concatenate([ibuf[j] for j in range(n)], axis=1)
    grid_i = lax.broadcasted_iota(jnp.int32, (total, total), 0)
    grid_j = lax.broadcasted_iota(jnp.int32, (total, total), 1)
    row_b = jnp.broadcast_to(idx_row, (total, total))
    idx_col = jnp.sum(jnp.where(grid_i == grid_j, row_b, 0), axis=1, keepdims=True)
    earlier = (row_b == idx_col) & (grid_j < grid_i)
    slot = jnp.sum(earlier.astype(jnp.int32), axis=1, keepdims=True)
    target = jnp.where(slot < capacity, idx_col, -1)
    mbuf[...] = jnp.broadcast_to(target, mbuf.shape)

    wait_all(loads)
    wait_all(copies)
    attn = dot_nt(cbuf[...].reshape(total, width), wo_ref[...].reshape(width, width))
    h2 = (h1_ref[...].astype(F32) + attn).astype(BF16)
    x = rms_norm(h2, ln_ref[...].reshape(1, width))
    xbuf[...] = x
    own[...] = h2.reshape(n, rows, width)
    def hidden_units(e, weight):
        u = jnp.maximum(dot_nn(xbuf[...], weight), 0.0)
        hit = jnp.broadcast_to(mbuf[:, 0:1], u.shape) == e
        ubuf[e] = jnp.where(hit, u, 0.0).astype(BF16)

    @pl.loop(0, early // 2)
    def _(i):
        for k in range(2):
            hidden_units(i * 2 + k, early_ref[i * 2 + k])

    @pl.loop(0, (experts - early) // 2)
    def _(i):
        for k in range(2):
            load(i * 2 + k, 0).wait()
        for k in range(2):
            hidden_units(early + i * 2 + k, wi[i * 2 + k])

    sends = []
    block = part.shape[-1]
    for c in range(width // block):
        lanes = slice(c * block, (c + 1) * block)

        def add_output(i, total, c=c, lanes=lanes):
            if c == 0:
                for k in range(4):
                    load(i * 4 + k, 1).wait()
            for k in range(4):
                total = total + dot_nn(ubuf[i * 4 + k], wo[i * 4 + k, :, lanes])
            return total
        sums = lax.fori_loop(0, experts // 4, add_output, jnp.zeros((total, block), F32))
        part[c] = sums.reshape(n, rows, block)
        sends += start_exchange(me, n, lambda p: part.at[c, p], ybuf.at[c, me], s5.at[c], r5.at[c])
        ybuf[c, me] = part[c, me]
    copies = sends

    my_rows = pl.ds(pl.multiple_of(me * rows, rows), rows)
    router = jnp.concatenate([rbuf[j] for j in range(n)], axis=0)
    logits = lax.dot_general(xbuf[my_rows, :].astype(F32), router, (((1,), (1,)), ((), ())),
                             precision=lax.Precision.HIGHEST, preferred_element_type=F32)
    probs = jnp.exp(logits - jnp.max(logits, axis=-1, keepdims=True))
    probs = probs / jnp.sum(probs, axis=-1, keepdims=True)
    chosen = lax.broadcasted_iota(jnp.int32, (rows, experts), 1) == mbuf[my_rows, :][:, 0:experts]
    gate = jnp.sum(jnp.where(chosen, probs, 0.0), axis=-1, keepdims=True)
    wait_all(copies)
    y = jnp.concatenate([sum(ybuf[c, j] for j in range(1, n)) + ybuf[c, 0] for c in range(width // block)], axis=1)
    out_ref[...] = (own[me].astype(F32) + y.astype(BF16).astype(F32) * gate).astype(BF16)


def call(body, out_shape, in_specs, out_specs, scratch, collective=None, flops=1_000_000, moved=1_000_000, vmem=VMEM_MAX):
    params = dict(vmem_limit_bytes=vmem)
    if collective is not None:
        params.update(collective_id=collective, has_side_effects=True)
    kernel = pl.pallas_call(
        body, out_shape=out_shape, in_specs=in_specs, out_specs=out_specs, scratch_shapes=scratch,
        compiler_params=pltpu.CompilerParams(**params),
        cost_estimate=pl.CostEstimate(flops=flops, bytes_accessed=moved, transcendentals=0))

    def run(*operands):
        return kernel(*[pltpu.with_memory_space_constraint(x, pltpu.HBM) if spec is HBM_SPEC else x
                        for x, spec in zip(operands, in_specs)])
    return run


def solution(mesh):
    n = mesh.shape['ws']
    row_axes = ('dp', 'ws')
    row_vec = P(row_axes)
    row_mat = P(row_axes, None)
    cache_spec = P(row_axes, None, None, None)
    col_split = P(None, 'ws')
    in_specs = (row_mat, cache_spec, cache_spec, cache_spec, cache_spec, row_vec, row_mat, P(None, None), row_vec,
                P(None), P(None), P(None), col_split, col_split, col_split, col_split, col_split, col_split,
                col_split, P(None, None, 'ws'), P(None, 'ws', None))
    out_specs = (row_mat, cache_spec, cache_spec)
    dma = pltpu.SemaphoreType.DMA

    def decoder_block(hidden, self_k, self_v, cross_k, cross_v, positions, enc_mask, rel_bias, expert_idx,
                      ln_self, ln_cross, ln_ffn, wq_self, wk_self, wv_self, wo_self, wq_cross, wo_cross,
                      w_router, w_in, w_out):
        rows, width = hidden.shape
        heads, length = rel_bias.shape
        head_dim = width // heads
        source = enc_mask.shape[1]
        cols = wq_self.shape[1]
        experts, _, units = w_in.shape
        total = n * rows
        sds = jax.ShapeDtypeStruct

        def flat(cache):
            return jnp.swapaxes(cache, 2, 3).reshape(rows, width, cache.shape[2])

        sems = [dma((n - 1,))]
        w_tile = pltpu.VMEM((cols, width), BF16)
        ln_tile = pltpu.VMEM((width,), F32)
        near, slots, early = NEAR, SLOTS, EARLY
        q, k, v, hall, brev, lens, wc_half, near_sk, near_sv = call(
            functools.partial(qkv_kernel, n),
            [sds((rows, width), BF16)] * 3 + [sds((total, width), BF16), sds((HEAD_PAD, length), F32), sds((rows, 128), jnp.int32),
               sds((cols // 2, width), BF16)]
            + [sds((rows, width, length), BF16)] * 2,
            [HBM_SPEC] * 10, [VMEM_SPEC] * 9,
            [pltpu.VMEM((rows, width), BF16), ln_tile, pltpu.VMEM((3, cols, width), BF16), pltpu.VMEM((heads, length), F32),
             pltpu.VMEM((rows, source), jnp.int32),
             pltpu.VMEM((n, rows, width), BF16), pltpu.VMEM((n, 3, rows, cols), BF16), pltpu.VMEM((n, 3, rows, cols), BF16)]
            + sems * 4 + [dma((8,)), dma((2, rows)), pltpu.VMEM((cols // 2, width), BF16), dma, dma],
            collective=0, vmem=8 << 20,
        )(hidden, ln_self, wq_self.T, wk_self.T, wv_self.T, rel_bias, enc_mask, wo_cross.T, flat(self_k), flat(self_v))

        def attention_scratch(size):
            return ([pltpu.VMEM((HEAD_PAD, size), F32)] * 4
                    + [pltpu.VMEM((rows, HEAD_PAD, width), BF16), pltpu.VMEM((rows, width), F32)])

        ctx, new_k, new_v = call(
            functools.partial(self_kernel, heads),
            [sds((rows, width), BF16)] + [sds((rows, width, length), BF16)] * 2,
            [HBM_SPEC] + [VMEM_SPEC] * 6, [VMEM_SPEC] + [HBM_SPEC] * 2,
            [pltpu.VMEM((rows, width, 128), BF16)] * 2 + [pltpu.VMEM((width, 128), F32)] * 2 + attention_scratch(length)
            + [pltpu.VMEM((rows, width), F32), pltpu.VMEM((rows, HEAD_PAD, 128), F32),
               dma((2, rows)), pltpu.SMEM((rows,), jnp.int32), dma],
            vmem=12 << 20,
        )(positions, q, k, v, brev, near_sk, near_sv)

        qc, h1, router, chosen, wc_full, near_ck, near_cv, early_w = call(
            functools.partial(mid_kernel, n),
            [sds((rows, width), BF16), sds((total, width), BF16), sds((n, experts // n, width), F32), sds((n, 1, rows), jnp.int32),
               sds((n, cols, width), BF16)]
            + [sds((rows, width, near), BF16)] * 2
            + [sds((early, width, units), BF16)],
            [VMEM_SPEC] * 2 + [HBM_SPEC] * 5 + [VMEM_SPEC] + [HBM_SPEC] * 4, [VMEM_SPEC] * 8,
            [pltpu.VMEM((experts // n, width), F32), pltpu.VMEM((1, rows), jnp.int32)] + sems * 4
            + [w_tile, dma((4,)), dma((4,)), w_tile, ln_tile, w_tile, dma((6,)), dma((2, rows)), dma((1, early)), pltpu.VMEM((n, rows, width), BF16), pltpu.VMEM((n, total, cols), BF16),
             pltpu.VMEM((n, rows, cols), BF16), pltpu.VMEM((n, rows, cols), BF16)] + sems * 6,
            collective=1, vmem=VM3 << 20,
        )(ctx, hall, wo_self.T, ln_cross, wq_cross.T, w_router.T, expert_idx[None, :], wc_half, wo_cross.T, flat(cross_k), flat(cross_v), w_in)

        ctx2 = call(
            functools.partial(cross_kernel, heads),
            sds((rows, width), BF16),
            [SMEM_SPEC] + [VMEM_SPEC] * 4 + [HBM_SPEC] * 2, VMEM_SPEC,
            [pltpu.VMEM((slots, width, source - near), BF16)] * 2 + attention_scratch(source) + [dma((2, slots))],
            vmem=VM4 << 20,
        )(lens, qc, enc_mask, near_ck, near_cv, flat(cross_k), flat(cross_v))

        parts = 3
        out = call(
            functools.partial(ffn_kernel, n),
            sds((rows, width), BF16),
            [VMEM_SPEC] * 3 + [HBM_SPEC] + [VMEM_SPEC] * 3 + [HBM_SPEC] * 2, VMEM_SPEC,
            [pltpu.VMEM((n, rows, width), BF16),
             pltpu.VMEM((total, width), BF16), pltpu.VMEM((total, 128), jnp.int32),
             pltpu.VMEM((experts - early, width, units), BF16), pltpu.VMEM((experts, units, width), BF16),
             pltpu.VMEM((experts, total, units), BF16),
             pltpu.VMEM((parts, n, rows, width // parts), F32), pltpu.VMEM((n, rows, width), BF16),
             pltpu.VMEM((parts, n, rows, width // parts), F32)]
            + sems * 2 + [dma((parts, n - 1))] * 2 + [dma((experts,)), dma((experts,))]
            + [ln_tile, dma((1,))],
            collective=2, vmem=VM5 << 20,
        )(ctx2, h1, wc_full, ln_ffn, router, chosen, early_w, w_in, w_out)

        def unflat(cache):
            return jnp.swapaxes(cache.reshape(rows, heads, head_dim, length), 2, 3)

        return out, unflat(new_k), unflat(new_v)

    return jax.shard_map(decoder_block, mesh=mesh, in_specs=in_specs, out_specs=out_specs, check_vma=False)
```

```python
import functools
import jax
import jax.numpy as jnp
from jax import lax
from jax.experimental import pallas as pl
from jax.experimental.pallas import tpu as pltpu
from jax.sharding import PartitionSpec as P

EPSILON = 1e-6
NEG_BIG = -1e30
F32 = jnp.float32
BF16 = jnp.bfloat16
MESH = pl.DeviceIdType.MESH
VMEM_SPEC = pl.BlockSpec(memory_space=pltpu.VMEM)
SMEM_SPEC = pl.BlockSpec(memory_space=pltpu.SMEM)
HBM_SPEC = pl.BlockSpec(memory_space=pltpu.HBM)
VMEM_MAX = 67_000_000
HEAD_PAD = 16
NEAR, SLOTS, EARLY = 512, 8, 4
VM3, VM4, VM5 = 8, 14, 39


def rms_norm(hidden, scale):
    hid = hidden.astype(F32)
    inv = lax.rsqrt(jnp.mean(hid * hid, axis=-1, keepdims=True) + EPSILON)
    return (hid * inv * scale).astype(BF16)


def dot_nn(a, b):
    return lax.dot_general(a, b, (((1,), (0,)), ((), ())), preferred_element_type=F32)


def dot_nt(a, b):
    return lax.dot_general(a, b, (((1,), (1,)), ((), ())), preferred_element_type=F32)


def greet(me, n, across=None):
    sem = pltpu.get_barrier_semaphore()
    for k in range(1, n):
        pl.semaphore_signal(sem, inc=1, device_id={"ws": lax.rem(me + k, n)}, device_id_type=MESH)
    if across is not None:
        pl.semaphore_signal(sem, inc=1, device_id=across, device_id_type=MESH)


def all_here(count):
    pl.semaphore_wait(pltpu.get_barrier_semaphore(), count)


def send(src, dst, send_sem, recv_sem, device):
    copy = pltpu.make_async_remote_copy(src_ref=src, dst_ref=dst, send_sem=send_sem, recv_sem=recv_sem,
                                        device_id=device, device_id_type=MESH)
    copy.start()
    return copy


def start_exchange(me, n, src_of, dst, send_sem, recv_sem):
    copies = []
    for k in range(1, n):
        peer = lax.rem(me + k, n)
        copy = pltpu.make_async_remote_copy(
            src_ref=src_of(peer), dst_ref=dst, send_sem=send_sem.at[k - 1], recv_sem=recv_sem.at[k - 1],
            device_id={"ws": peer}, device_id_type=MESH)
        copy.start()
        copies.append(copy)
    return copies


def wait_all(copies):
    for copy in copies:
        copy.wait()


def my_columns(full, me, n, width):
    picked = full[:, 0:width]
    for j in range(1, n):
        picked = jnp.where(me == j, full[:, j * width:(j + 1) * width], picked)
    return picked


def fetch(pairs, sem):
    copies = [pltpu.make_async_copy(src, dst, sem.at[i]) for i, (src, dst) in enumerate(pairs)]
    for copy in copies:
        copy.start()
    return copies


def read_rows(pairs, sem):
    def copy(i, r):
        return pltpu.make_async_copy(pairs[i][0].at[r], pairs[i][1].at[r], sem.at[i, r])
    rows = pairs[0][1].shape[0]

    def start():
        @pl.loop(0, rows)
        def _(r):
            for i in range(len(pairs)):
                copy(i, r).start()

    def wait():
        @pl.loop(0, rows)
        def _(r):
            for i in range(len(pairs)):
                copy(i, r).wait()
    return start, wait


def qkv_kernel(n, h_hbm, ln_hbm, wq_hbm, wk_hbm, wv_hbm, bias_hbm, mask_hbm, wc_hbm, sk_hbm, sv_hbm,
               q_ref, k_ref, v_ref, hall_ref, brev_ref, lens_ref, wc_half, sk_ref, sv_ref,
               h_ref, ln_ref, w_ref, bias_ref, mask_ref, hbuf, sendbuf, recvbuf, s1, r1, s2, r2, in_sem, row_sem,
               wc_own, swc, rwc):
    me = lax.axis_index("ws")
    rows, width = h_ref.shape
    cols = w_ref.shape[1]
    greet(me, n)
    half = cols // 2
    start = pl.multiple_of(lax.axis_index("dp") * half, 16)
    loads = fetch([(h_hbm, h_ref), (wc_hbm.at[pl.ds(start, half)], wc_own), (ln_hbm, ln_ref), (bias_hbm, bias_ref), (mask_hbm, mask_ref)]
                  + [(w, w_ref.at[i]) for i, w in enumerate((wq_hbm, wk_hbm, wv_hbm))], in_sem)
    start_rows, wait_rows = read_rows([(sk_hbm, sk_ref), (sv_hbm, sv_ref)], row_sem)
    start_rows()
    all_here(n - 1)
    loads[0].wait()
    copies = start_exchange(me, n, lambda p: h_ref, hbuf.at[me], s1, r1)
    hbuf[me] = h_ref[...]
    other = {"ws": lax.rem(me + n // 2, n)}
    loads[1].wait()
    bulk = [send(wc_own, wc_half, swc, rwc, other)]
    for load in loads[2:]:
        load.wait()
    lens_ref[...] = jnp.broadcast_to(jnp.sum(mask_ref[...], axis=1, keepdims=True), lens_ref.shape)
    heads, length = bias_ref.shape
    flip = (lax.broadcasted_iota(jnp.int32, (length, length), 0)
            + lax.broadcasted_iota(jnp.int32, (length, length), 1) == length - 1).astype(F32)
    brev_ref[...] = jnp.zeros_like(brev_ref)
    brev_ref[0:heads, :] = lax.dot_general(bias_ref[...], flip, (((1,), (0,)), ((), ())),
                                           precision=lax.Precision.HIGHEST, preferred_element_type=F32)
    wait_all(copies)
    hidden = hbuf[...].reshape(n * rows, width)
    hall_ref[...] = hidden
    x = rms_norm(hidden, ln_ref[...].reshape(1, width))
    for i in range(3):
        sendbuf[:, i] = dot_nt(x, w_ref[i]).astype(BF16).reshape(n, rows, cols)
    copies = start_exchange(me, n, lambda p: sendbuf.at[p], recvbuf.at[me], s2, r2)
    recvbuf[me] = sendbuf[me]
    wait_all(copies)
    for i, o in enumerate((q_ref, k_ref, v_ref)):
        o[...] = jnp.concatenate([recvbuf[j, i] for j in range(n)], axis=1)
    wait_rows()
    wait_all(bulk)


def head_mask(shape, head_dim):
    head = lax.broadcasted_iota(jnp.int32, shape, 0)
    return lax.broadcasted_iota(jnp.int32, shape, 1) // head_dim == head


def spread_heads(q_ref, qblk, head_dim):
    rows, width = q_ref.shape
    q = q_ref[...].astype(F32)
    keep = head_mask((HEAD_PAD, width), head_dim)
    for r in range(rows):
        qblk[r] = jnp.where(keep, jnp.broadcast_to(q[r:r + 1], (HEAD_PAD, width)), 0.0).astype(BF16)


def softmax_rows(scores):
    top = jnp.max(scores, axis=-1, keepdims=True)
    e = jnp.exp(scores - top)
    return (e / jnp.sum(e, axis=-1, keepdims=True)).astype(BF16).astype(F32)


def weighted_values(prob, value, heads, head_dim, length):
    parts = []
    for h in range(heads):
        total = None
        for t in range(length // 128):
            lanes = slice(t * 128, (t + 1) * 128)
            term = value(slice(h * head_dim, (h + 1) * head_dim), t).astype(F32) * prob[h:h + 1, lanes]
            total = term if total is None else total + term
        parts.append(total)
    return jnp.sum(jnp.transpose(jnp.concatenate(parts, axis=0)), axis=0, keepdims=True)


def self_kernel(heads, pos_hbm, q_ref, k_ref, v_ref, brev_ref, sk_ref, sv_ref,
                ctx_ref, nk_ref, nv_ref,
                ktile, vtile, kt, vt, s0, s1, p0, p1, qblk, cf, xf, snew, out_sem, pos_ref, pos_sem):
    rows, width, length = sk_ref.shape
    head_dim = width // heads
    tiles = length // 128
    scalars = pltpu.make_async_copy(pos_hbm, pos_ref, pos_sem)
    scalars.start()

    pad = jnp.zeros((128 - rows, width), F32)
    kt[...] = jnp.transpose(jnp.concatenate([k_ref[...].astype(F32), pad], axis=0))
    vt[...] = jnp.transpose(jnp.concatenate([v_ref[...].astype(F32), pad], axis=0))
    spread_heads(q_ref, qblk, head_dim)
    snew[...] = dot_nn(qblk[...].reshape(rows * HEAD_PAD, width), kt[...].astype(BF16)).reshape(snew.shape)
    sbufs, pbufs = (s0, s1), (p0, p1)
    scalars.wait()

    def insert(r, cache, tile_buf, cols):
        pos = pos_ref[r]
        tile = pos // 128
        at = pos - tile * 128
        new = jnp.broadcast_to(cols[:, r:r + 1], (width, 128))
        old = cache[r, :, pl.ds(pl.multiple_of(tile * 128, 128), 128)]
        hit = lax.broadcasted_iota(jnp.int32, (width, 128), 1) == at
        tile_buf[r] = jnp.where(hit, new, old.astype(F32)).astype(BF16)

    def save(r):
        tile = pos_ref[r] // 128
        for i, (cache, tile_buf, dst) in enumerate(((sk_ref, ktile, nk_ref), (sv_ref, vtile, nv_ref))):
            for t in range(tiles):
                lanes = slice(t * 128, (t + 1) * 128)

                @pl.when(tile == t)
                def _():
                    pltpu.make_async_copy(tile_buf.at[r], dst.at[r, :, lanes], out_sem.at[i, r]).start()

                @pl.when(tile != t)
                def _():
                    pltpu.make_async_copy(cache.at[r, :, lanes], dst.at[r, :, lanes], out_sem.at[i, r]).start()

    def softmax(r):
        pos = pos_ref[r]
        bias = pltpu.roll(brev_ref[...], lax.rem(pos + 1, length), 1)
        lane = lax.broadcasted_iota(jnp.int32, (HEAD_PAD, length), 1)
        pick = lax.broadcasted_iota(jnp.int32, (HEAD_PAD, 128), 1) == r
        fresh = jnp.sum(jnp.where(pick, snew[r], 0.0), axis=-1, keepdims=True)
        scores = jnp.where(lane == pos, fresh, sbufs[r % 2][...]) + bias
        prob = softmax_rows(jnp.where(lane <= pos, scores, NEG_BIG))
        pbufs[r % 2][...] = jnp.where(lane == pos, 0.0, prob)
        at_pos = jnp.sum(jnp.where(lane == pos, prob, 0.0), axis=-1, keepdims=True)
        spread = jnp.where(head_mask((HEAD_PAD, width), head_dim), jnp.broadcast_to(at_pos, (HEAD_PAD, width)), 0.0)
        xf[r:r + 1, :] = jnp.sum(spread, axis=0, keepdims=True) * v_ref[r:r + 1, :].astype(F32)

    for step in range(rows + 2):
        if step >= 2:
            done = step - 2
            cf[done:done + 1, :] = xf[done:done + 1, :] + weighted_values(
                pbufs[done % 2], lambda d, t: sv_ref[done, d, t * 128:(t + 1) * 128], heads, head_dim, length)
        if 1 <= step < rows + 1:
            softmax(step - 1)
            save(step - 1)
        if step < rows:
            sbufs[step % 2][...] = dot_nn(qblk[step], sk_ref[step])
            insert(step, sk_ref, ktile, kt)
            insert(step, sv_ref, vtile, vt)

    ctx_ref[...] = cf[...].astype(BF16)
    for r in range(rows):
        pltpu.make_async_copy(sk_ref.at[r], nk_ref.at[r], out_sem.at[0, r]).wait()
        pltpu.make_async_copy(sv_ref.at[r], nv_ref.at[r], out_sem.at[1, r]).wait()


def mid_kernel(n, ctx_ref, hall_ref, wo_hbm, ln_hbm, wq_hbm, wr_hbm, idx_hbm, wc_half, wc_hbm, ck_hbm, cv_hbm, win_hbm,
               q_ref, h1_ref, wr_ref, idx_ref, wc_ref, ck_ref, cv_ref, win_ref, wr_own, idx_own, sr, rr, si, ri, wc_own, sw, rw, wo_ref, ln_ref, wq_ref, in_sem, row_sem, win_sem, cbuf, hpart, sendbuf, recvbuf, s1, r1, s2, r2, s3, r3):
    me = lax.axis_index("ws")
    rows, width = ctx_ref.shape
    cols = wo_ref.shape[0]
    group = lax.axis_index("dp")
    across = {"dp": 1 - group, "ws": me}
    greet(me, n, across)
    loads = fetch([(wo_hbm, wo_ref), (ln_hbm, ln_ref), (wq_hbm, wq_ref), (wr_hbm, wr_own), (idx_hbm, idx_own), (wc_hbm, wc_own)], in_sem)
    near = ck_ref.shape[2]
    start_rows, wait_rows = read_rows([(ck_hbm.at[:, :, 0:near], ck_ref), (cv_hbm.at[:, :, 0:near], cv_ref)], row_sem)
    start_win, wait_win = read_rows([(win_hbm, win_ref)], win_sem)
    start_rows()
    start_win()
    facing, sibling = lax.rem(me + n // 2, n), me + 1 - 2 * lax.rem(me, 2)
    half = cols // 2
    mine_half = pl.ds(pl.multiple_of(group * half, 16), half)
    its_half = pl.ds(pl.multiple_of((1 - group) * half, 16), half)
    all_here(n)
    copies = start_exchange(me, n, lambda p: ctx_ref, cbuf.at[me], s1, r1)
    swap = send(wc_half, wc_ref.at[facing, mine_half], sw.at[0], rw.at[0], across)
    bulk = [send(wc_half, wc_ref.at[facing, mine_half], sw.at[1], rw.at[1], {"ws": sibling})]
    cbuf[me] = ctx_ref[...]
    mine = my_columns(hall_ref[...].astype(F32), me, n, cols)
    wait_all(loads)
    bulk += start_exchange(me, n, lambda p: wr_own, wr_ref.at[me], sr, rr)
    bulk += start_exchange(me, n, lambda p: idx_own, idx_ref.at[me], si, ri)
    bulk.append(send(wc_own, wc_ref.at[me], sw.at[2], rw.at[2], {"ws": sibling}))
    wc_ref[me] = wc_own[...]
    wc_ref[facing, mine_half] = wc_half[...]
    wait_all(copies)
    attn = dot_nt(cbuf[...].reshape(n * rows, width), wo_ref[...])
    hpart[me] = (mine + attn).astype(BF16)
    copies = start_exchange(me, n, lambda p: hpart.at[me], hpart.at[me], s2, r2)
    wait_all(copies)
    h1 = jnp.concatenate([hpart[j] for j in range(n)], axis=1)
    h1_ref[...] = h1
    x = rms_norm(h1, ln_ref[...].reshape(1, width))
    sendbuf[...] = dot_nt(x, wq_ref[...]).astype(BF16).reshape(n, rows, cols)
    copies = start_exchange(me, n, lambda p: sendbuf.at[p], recvbuf.at[me], s3, r3)
    recvbuf[me] = sendbuf[me]
    wr_ref[me] = wr_own[...]
    idx_ref[me] = idx_own[...]
    swap.wait()
    bulk.append(send(wc_ref.at[facing, its_half], wc_ref.at[facing, its_half], sw.at[3], rw.at[3], {"ws": sibling}))
    wait_all(copies)
    q_ref[...] = jnp.concatenate([recvbuf[j] for j in range(n)], axis=1)
    wait_rows()
    wait_all(bulk)
    wait_win()


def cross_kernel(heads, lens_ref, q_ref, mask_ref, kn_ref, vn_ref, ck_ref, cv_ref,
                 ctx_ref, kbuf, vbuf, s0, s1, p0, p1, qblk, cf, in_sem):
    rows, width, near = kn_ref.shape
    slots = kbuf.shape[0]
    length = near + kbuf.shape[2]
    head_dim = width // heads
    block = 256
    tiles, near_tiles = length // 128, near // 128

    def slot(r):
        return lax.rem(r, slots)

    def tile_count(r):
        return (lens_ref[r, 0] + 127) // 128

    def far_copies(r, body):
        count = tile_count(r)
        for t in range(near_tiles + 1, tiles + 1):
            @pl.when(count == t)
            def _(size=(t - near_tiles) * 128):
                body(lambda i: pltpu.make_async_copy(
                    (ck_ref, cv_ref)[i].at[r, :, near:near + size], (kbuf, vbuf)[i].at[slot(r), :, 0:size],
                    in_sem.at[i, slot(r)]))

    def far_start(r):
        far_copies(r, lambda copy: (copy(0).start(), copy(1).start()))
        for t in [t for t in range(1, tiles, 2) if t >= near_tiles]:
            @pl.when(tile_count(r) == t)
            def _(at=(t - near_tiles) * 128):
                vbuf[slot(r), :, at:at + 128] = jnp.zeros((width, 128), BF16)

    def per_block(r, body):
        blocks = (lens_ref[r, 0] + block - 1) // block
        for t in range(1, length // block + 1):
            @pl.when(blocks == t)
            def _(size=t * block):
                body(size)

    @pl.loop(0, slots)
    def _(r):
        far_start(r)

    spread_heads(q_ref, qblk, head_dim)

    def scores(r, size, out):
        first = min(size, near)
        out[:, 0:first] = dot_nn(qblk[r], kn_ref[r, :, 0:first])
        if size > near:
            out[:, near:size] = dot_nn(qblk[r], kbuf[slot(r), :, 0:size - near])

    def softmax(r, src, out):
        keep = jnp.broadcast_to(mask_ref[pl.ds(r, 1), :], (HEAD_PAD, length)) == 1
        out[...] = softmax_rows(jnp.where(keep, src[...], NEG_BIG))

    def values(r, size, prob):
        def tile(d, t):
            if t < near_tiles:
                return vn_ref[r, d, t * 128:(t + 1) * 128]
            return vbuf[slot(r), d, (t - near_tiles) * 128:(t - near_tiles + 1) * 128]
        cf[pl.ds(r, 1), :] = weighted_values(prob, tile, heads, head_dim, size)

    def arrived(r, i):
        far_copies(r, lambda copy: copy(i).wait())

    arrived(0, 0)
    per_block(0, lambda size: scores(0, size, s0))
    arrived(1, 0)

    def second(size):
        softmax(0, s0, p0)
        scores(1, size, s1)
    per_block(1, second)

    def step(r, sa, sb, pa, pb):
        arrived(r, 1)
        arrived(r + 2, 0)

        def outer(size_v):
            def inner(size_s):
                values(r, size_v, pa)
                softmax(r + 1, sb, pb)
                scores(r + 2, size_s, sa)
            per_block(r + 2, inner)
        per_block(r, outer)

        @pl.when(r + slots < rows)
        def _():
            far_start(r + slots)

    @pl.loop(0, (rows - 2) // 2)
    def _(i):
        step(2 * i, s0, s1, p0, p1)
        step(2 * i + 1, s1, s0, p1, p0)

    def last_but_one(size):
        values(rows - 2, size, p0)
        softmax(rows - 1, s1, p1)
    arrived(rows - 2, 1)
    per_block(rows - 2, last_but_one)
    arrived(rows - 1, 1)
    per_block(rows - 1, lambda size: values(rows - 1, size, p1))
    ctx_ref[...] = cf[...].astype(BF16)


def ffn_kernel(n, ctx_ref, h1_ref, wo_ref, ln_hbm, rbuf, ibuf, early_ref, win_ref, wout_ref,
               out_ref, cbuf, xbuf, mbuf, wi, wo, ubuf, part, own, ybuf,
               s1, r1, s5, r5, wi_sem, wo_sem, ln_ref, in_sem):
    me = lax.axis_index("ws")
    rows, width = ctx_ref.shape
    experts = win_ref.shape[0]
    total = n * rows
    capacity = (2 * total + experts - 1) // experts

    early = early_ref.shape[0]

    def load(e, i):
        if i == 0:
            return pltpu.make_async_copy(win_ref.at[e + early], wi.at[e], wi_sem.at[e])
        return pltpu.make_async_copy(wout_ref.at[e], wo.at[e], wo_sem.at[e])

    greet(me, n)
    loads = fetch([(ln_hbm, ln_ref)], in_sem)

    @pl.loop(0, experts - early)
    def _(e):
        load(e, 0).start()

    all_here(n - 1)
    copies = start_exchange(me, n, lambda p: ctx_ref, cbuf.at[me], s1, r1)

    @pl.loop(0, experts)
    def _(e):
        load(e, 1).start()

    cbuf[me] = ctx_ref[...]

    idx_row = jnp.concatenate([ibuf[j] for j in range(n)], axis=1)
    grid_i = lax.broadcasted_iota(jnp.int32, (total, total), 0)
    grid_j = lax.broadcasted_iota(jnp.int32, (total, total), 1)
    row_b = jnp.broadcast_to(idx_row, (total, total))
    idx_col = jnp.sum(jnp.where(grid_i == grid_j, row_b, 0), axis=1, keepdims=True)
    earlier = (row_b == idx_col) & (grid_j < grid_i)
    slot = jnp.sum(earlier.astype(jnp.int32), axis=1, keepdims=True)
    target = jnp.where(slot < capacity, idx_col, -1)
    mbuf[...] = jnp.broadcast_to(target, mbuf.shape)

    wait_all(loads)
    wait_all(copies)
    attn = dot_nt(cbuf[...].reshape(total, width), wo_ref[...].reshape(width, width))
    h2 = (h1_ref[...].astype(F32) + attn).astype(BF16)
    x = rms_norm(h2, ln_ref[...].reshape(1, width))
    xbuf[...] = x
    own[...] = h2.reshape(n, rows, width)
    def hidden_units(e, weight):
        u = jnp.maximum(dot_nn(xbuf[...], weight), 0.0)
        hit = jnp.broadcast_to(mbuf[:, 0:1], u.shape) == e
        ubuf[e] = jnp.where(hit, u, 0.0).astype(BF16)

    @pl.loop(0, early // 2)
    def _(i):
        for k in range(2):
            hidden_units(i * 2 + k, early_ref[i * 2 + k])

    @pl.loop(0, (experts - early) // 2)
    def _(i):
        for k in range(2):
            load(i * 2 + k, 0).wait()
        for k in range(2):
            hidden_units(early + i * 2 + k, wi[i * 2 + k])

    sends = []
    block = part.shape[-1]
    for c in range(width // block):
        lanes = slice(c * block, (c + 1) * block)

        def add_output(i, total, c=c, lanes=lanes):
            if c == 0:
                for k in range(4):
                    load(i * 4 + k, 1).wait()
            for k in range(4):
                total = total + dot_nn(ubuf[i * 4 + k], wo[i * 4 + k, :, lanes])
            return total
        sums = lax.fori_loop(0, experts // 4, add_output, jnp.zeros((total, block), F32))
        part[c] = sums.reshape(n, rows, block)
        sends += start_exchange(me, n, lambda p: part.at[c, p], ybuf.at[c, me], s5.at[c], r5.at[c])
        ybuf[c, me] = part[c, me]
    copies = sends

    my_rows = pl.ds(pl.multiple_of(me * rows, rows), rows)
    router = jnp.concatenate([rbuf[j] for j in range(n)], axis=0)
    logits = lax.dot_general(xbuf[my_rows, :].astype(F32), router, (((1,), (1,)), ((), ())),
                             precision=lax.Precision.HIGHEST, preferred_element_type=F32)
    probs = jnp.exp(logits - jnp.max(logits, axis=-1, keepdims=True))
    probs = probs / jnp.sum(probs, axis=-1, keepdims=True)
    chosen = lax.broadcasted_iota(jnp.int32, (rows, experts), 1) == mbuf[my_rows, :][:, 0:experts]
    gate = jnp.sum(jnp.where(chosen, probs, 0.0), axis=-1, keepdims=True)
    wait_all(copies)
    y = jnp.concatenate([sum(ybuf[c, j] for j in range(1, n)) + ybuf[c, 0] for c in range(width // block)], axis=1)
    out_ref[...] = (own[me].astype(F32) + y.astype(BF16).astype(F32) * gate).astype(BF16)


def call(body, out_shape, in_specs, out_specs, scratch, collective=None, flops=1_000_000, moved=1_000_000, vmem=VMEM_MAX):
    params = dict(vmem_limit_bytes=vmem)
    if collective is not None:
        params.update(collective_id=collective, has_side_effects=True)
    kernel = pl.pallas_call(
        body, out_shape=out_shape, in_specs=in_specs, out_specs=out_specs, scratch_shapes=scratch,
        compiler_params=pltpu.CompilerParams(**params),
        cost_estimate=pl.CostEstimate(flops=flops, bytes_accessed=moved, transcendentals=0))

    def run(*operands):
        return kernel(*[pltpu.with_memory_space_constraint(x, pltpu.HBM) if spec is HBM_SPEC else x
                        for x, spec in zip(operands, in_specs)])
    return run


def solution(mesh):
    n = mesh.shape['ws']
    row_axes = ('dp', 'ws')
    row_vec = P(row_axes)
    row_mat = P(row_axes, None)
    cache_spec = P(row_axes, None, None, None)
    col_split = P(None, 'ws')
    in_specs = (row_mat, cache_spec, cache_spec, cache_spec, cache_spec, row_vec, row_mat, P(None, None), row_vec,
                P(None), P(None), P(None), col_split, col_split, col_split, col_split, col_split, col_split,
                col_split, P(None, None, 'ws'), P(None, 'ws', None))
    out_specs = (row_mat, cache_spec, cache_spec)
    dma = pltpu.SemaphoreType.DMA

    def decoder_block(hidden, self_k, self_v, cross_k, cross_v, positions, enc_mask, rel_bias, expert_idx,
                      ln_self, ln_cross, ln_ffn, wq_self, wk_self, wv_self, wo_self, wq_cross, wo_cross,
                      w_router, w_in, w_out):
        rows, width = hidden.shape
        heads, length = rel_bias.shape
        head_dim = width // heads
        source = enc_mask.shape[1]
        cols = wq_self.shape[1]
        experts, _, units = w_in.shape
        total = n * rows
        sds = jax.ShapeDtypeStruct

        def flat(cache):
            return jnp.swapaxes(cache, 2, 3).reshape(rows, width, cache.shape[2])

        sems = [dma((n - 1,))]
        w_tile = pltpu.VMEM((cols, width), BF16)
        ln_tile = pltpu.VMEM((width,), F32)
        near, slots, early = NEAR, SLOTS, EARLY
        q, k, v, hall, brev, lens, wc_half, near_sk, near_sv = call(
            functools.partial(qkv_kernel, n),
            [sds((rows, width), BF16)] * 3 + [sds((total, width), BF16), sds((HEAD_PAD, length), F32), sds((rows, 128), jnp.int32),
               sds((cols // 2, width), BF16)]
            + [sds((rows, width, length), BF16)] * 2,
            [HBM_SPEC] * 10, [VMEM_SPEC] * 9,
            [pltpu.VMEM((rows, width), BF16), ln_tile, pltpu.VMEM((3, cols, width), BF16), pltpu.VMEM((heads, length), F32),
             pltpu.VMEM((rows, source), jnp.int32),
             pltpu.VMEM((n, rows, width), BF16), pltpu.VMEM((n, 3, rows, cols), BF16), pltpu.VMEM((n, 3, rows, cols), BF16)]
            + sems * 4 + [dma((8,)), dma((2, rows)), pltpu.VMEM((cols // 2, width), BF16), dma, dma],
            collective=0, vmem=8 << 20,
        )(hidden, ln_self, wq_self.T, wk_self.T, wv_self.T, rel_bias, enc_mask, wo_cross.T, flat(self_k), flat(self_v))

        def attention_scratch(size):
            return ([pltpu.VMEM((HEAD_PAD, size), F32)] * 4
                    + [pltpu.VMEM((rows, HEAD_PAD, width), BF16), pltpu.VMEM((rows, width), F32)])

        ctx, new_k, new_v = call(
            functools.partial(self_kernel, heads),
            [sds((rows, width), BF16)] + [sds((rows, width, length), BF16)] * 2,
            [HBM_SPEC] + [VMEM_SPEC] * 6, [VMEM_SPEC] + [HBM_SPEC] * 2,
            [pltpu.VMEM((rows, width, 128), BF16)] * 2 + [pltpu.VMEM((width, 128), F32)] * 2 + attention_scratch(length)
            + [pltpu.VMEM((rows, width), F32), pltpu.VMEM((rows, HEAD_PAD, 128), F32),
               dma((2, rows)), pltpu.SMEM((rows,), jnp.int32), dma],
            vmem=12 << 20,
        )(positions, q, k, v, brev, near_sk, near_sv)

        qc, h1, router, chosen, wc_full, near_ck, near_cv, early_w = call(
            functools.partial(mid_kernel, n),
            [sds((rows, width), BF16), sds((total, width), BF16), sds((n, experts // n, width), F32), sds((n, 1, rows), jnp.int32),
               sds((n, cols, width), BF16)]
            + [sds((rows, width, near), BF16)] * 2
            + [sds((early, width, units), BF16)],
            [VMEM_SPEC] * 2 + [HBM_SPEC] * 5 + [VMEM_SPEC] + [HBM_SPEC] * 4, [VMEM_SPEC] * 8,
            [pltpu.VMEM((experts // n, width), F32), pltpu.VMEM((1, rows), jnp.int32)] + sems * 4
            + [w_tile, dma((4,)), dma((4,)), w_tile, ln_tile, w_tile, dma((6,)), dma((2, rows)), dma((1, early)), pltpu.VMEM((n, rows, width), BF16), pltpu.VMEM((n, total, cols), BF16),
             pltpu.VMEM((n, rows, cols), BF16), pltpu.VMEM((n, rows, cols), BF16)] + sems * 6,
            collective=1, vmem=VM3 << 20,
        )(ctx, hall, wo_self.T, ln_cross, wq_cross.T, w_router.T, expert_idx[None, :], wc_half, wo_cross.T, flat(cross_k), flat(cross_v), w_in)

        ctx2 = call(
            functools.partial(cross_kernel, heads),
            sds((rows, width), BF16),
            [SMEM_SPEC] + [VMEM_SPEC] * 4 + [HBM_SPEC] * 2, VMEM_SPEC,
            [pltpu.VMEM((slots, width, source - near), BF16)] * 2 + attention_scratch(source) + [dma((2, slots))],
            vmem=VM4 << 20,
        )(lens, qc, enc_mask, near_ck, near_cv, flat(cross_k), flat(cross_v))

        parts = 3
        out = call(
            functools.partial(ffn_kernel, n),
            sds((rows, width), BF16),
            [VMEM_SPEC] * 3 + [HBM_SPEC] + [VMEM_SPEC] * 3 + [HBM_SPEC] * 2, VMEM_SPEC,
            [pltpu.VMEM((n, rows, width), BF16),
             pltpu.VMEM((total, width), BF16), pltpu.VMEM((total, 128), jnp.int32),
             pltpu.VMEM((experts - early, width, units), BF16), pltpu.VMEM((experts, units, width), BF16),
             pltpu.VMEM((experts, total, units), BF16),
             pltpu.VMEM((parts, n, rows, width // parts), F32), pltpu.VMEM((n, rows, width), BF16),
             pltpu.VMEM((parts, n, rows, width // parts), F32)]
            + sems * 2 + [dma((parts, n - 1))] * 2 + [dma((experts,)), dma((experts,))]
            + [ln_tile, dma((1,))],
            collective=2, vmem=VM5 << 20,
        )(ctx2, h1, wc_full, ln_ffn, router, chosen, early_w, w_in, w_out)

        def unflat(cache):
            return jnp.swapaxes(cache.reshape(rows, heads, head_dim, length), 2, 3)

        return out, unflat(new_k), unflat(new_v)

    return jax.shard_map(decoder_block, mesh=mesh, in_specs=in_specs, out_specs=out_specs, check_vma=False)
```
